512 devices in a mesh: cuts: 32 (over z, core), row: 16 (over y, x).
Axes of the slice: x: 4, y: 4, z: 16, core: 2. Of those that a mesh axis runs over, the one named last changes fastest.
Arguments:
- field: float32 [2, 256, 256, 256], P(None, 'cuts', 'row'), may hold values from -6 to 6
- row_prop: float32 [2, 256, 256], replicated, may hold values from -0.25 to 0.25
- col_prop: float32 [2, 256, 256], replicated, may hold values from -0.25 to 0.25
- phase: float32 [256, 8192], P('cuts', 'row'), may hold values from -3.140625 to 3.140625
- energy: float32 [256, 8192], P('cuts', 'row'), may hold values from -6 to 6
- cells: int32 [256, 8192], P('cuts', 'row'), may hold values from 0 to 65535, as said below
- shifts: int32 [4], replicated, may hold values from 1 to 2, as said below
Outputs:
- field_out: float32 [2, 256, 256, 256], P(None, 'cuts', 'row')
- phase_out: float32 [256, 8192], P('cuts', 'row')
- energy_out: float32 [256, 8192], P('cuts', 'row')
- bunching: float32 [4, 2, 256], P(None, None, 'cuts')
The draws below stay inside these ranges and needn't reach their ends.
Inputs may be any that keep to these rules, and one draw needn't show every extreme that they name: `cells`: electron j of a slice sits in a grid row from b * 16 to (b + 1) * 16 - 1, where b = j // 512. `shifts`: 2 slices slip in at least one period.
All inputs are finite; a program needn't handle non-finite values.
Results may differ from the reference program's by a relative error of at most 0.00021.
Values sent between devices are 32-bit elements; how exact they have to be, the bound alone decides.
A program may use at most 64 MiB of HBM per device.

```python
import jax
import jax.numpy as jnp
from jax import lax

NR = 256
NC = 256
ELEC = 8192
PERIODS = 4
KMAX = 2
SLICES = 256
N_ROW = 16


def draw_cells(key, part):
    rows_dev = NR // N_ROW
    row_block = jnp.arange(ELEC, dtype=jnp.int32) // (ELEC // N_ROW)
    offset = jax.random.randint(jax.random.fold_in(key, 11), (SLICES, ELEC), 0, rows_dev * NC, dtype=jnp.int32)
    return (row_block[None, :] * (rows_dev * NC) + offset).astype(jnp.int32)


def draw_shifts(key, part):
    chosen = jax.random.randint(jax.random.fold_in(key, 21), (PERIODS,), 1, KMAX + 1, dtype=jnp.int32)
    marked = jax.random.randint(jax.random.fold_in(key, 22), (), 0, PERIODS, dtype=jnp.int32)
    return jnp.where(jnp.arange(PERIODS, dtype=jnp.int32) == marked, KMAX, chosen).astype(jnp.int32)


def steps_of(key, dims, cuts, low, top_value):
    loudness = 1.0
    for dim, parts in cuts:
        steps = jax.random.uniform(jax.random.fold_in(jax.random.fold_in(key, 6), dim), (parts,), jnp.float32, low / len(cuts), top_value / len(cuts))
        loudness = loudness * jnp.repeat(jnp.exp(steps), dims[dim] // parts).reshape((-1,) + (1,) * (len(dims) - 1 - dim))
    return loudness


def noise(stream_key, extent, spread, most, cuts=(), held_as=jnp.bfloat16):
    gain = steps_of(stream_key, extent, cuts, -0.22, 0.18) if cuts else 1.0
    array = jax.random.normal(stream_key, extent, jnp.float32) * spread * gain
    return jnp.minimum(jnp.maximum(array, -most), most).astype(held_as)


def setup_inputs(seed: int = 0) -> dict:
    splits = jax.random.split(jax.random.key(seed), 8)
    field = noise(splits[0], (2, SLICES, NR, NC), 1.0, 6.0, ((1, 32), (2, 16)), jnp.float32)
    row_prop = noise(splits[1], (2, NR, NR), (2 * NR) ** -0.5, 0.25, (), jnp.float32)
    col_prop = noise(splits[2], (2, NC, NC), (2 * NC) ** -0.5, 0.25, (), jnp.float32)
    phase = jnp.clip(jax.random.uniform(splits[3], (SLICES, ELEC), jnp.float32, -3.140625, 3.140625), -3.140625, 3.140625)
    energy = noise(splits[4], (SLICES, ELEC), 1.0, 6.0, ((0, 32), (1, 16)), jnp.float32)
    cells = draw_cells(jax.random.fold_in(splits[7], 71), 0)
    shifts = draw_shifts(jax.random.fold_in(splits[7], 71), 0)
    return {"field": field, "row_prop": row_prop, "col_prop": col_prop, "phase": phase, "energy": energy, "cells": cells, "shifts": shifts}


kick_rate = 0.5
source_gain = 0.5


def sweep_columns(prop, real_part, imag_part):
    def product(matrix, values):
        return jnp.einsum('ck,srk->src', matrix, values, precision=lax.Precision.HIGHEST)
    return (product(prop[0], real_part) - product(prop[1], imag_part),
            product(prop[0], imag_part) + product(prop[1], real_part))


def sweep_rows(prop, real_part, imag_part):
    def product(matrix, values):
        return jnp.einsum('rk,skc->src', matrix, values, precision=lax.Precision.HIGHEST)
    return (product(prop[0], real_part) - product(prop[1], imag_part),
            product(prop[0], imag_part) + product(prop[1], real_part))


def reference(field, row_prop, col_prop, phase, energy, cells, shifts):
    real_part = field[0]
    imag_part = field[1]
    count = real_part.shape[0]
    slice_index = jnp.arange(count, dtype=jnp.int32)[:, None]
    partials = []
    for period in range(PERIODS):
        start = (KMAX - shifts[period]).astype(jnp.int32)
        padding = jnp.zeros((KMAX, NR, NC), dtype=real_part.dtype)
        real_part = lax.dynamic_slice_in_dim(jnp.concatenate([padding, real_part], 0), start, count, 0)
        imag_part = lax.dynamic_slice_in_dim(jnp.concatenate([padding, imag_part], 0), start, count, 0)
        sample_real = jnp.take_along_axis(real_part.reshape(count, NR * NC), cells, axis=1)
        sample_imag = jnp.take_along_axis(imag_part.reshape(count, NR * NC), cells, axis=1)
        energy = energy - kick_rate * (sample_real * jnp.cos(phase) - sample_imag * jnp.sin(phase))
        phase = phase + energy
        emit_real = jnp.cos(phase)
        emit_imag = -jnp.sin(phase)
        partials.append(jnp.stack([jnp.sum(emit_real, 1), jnp.sum(emit_imag, 1)]))
        deposit_real = jnp.zeros((count, NR * NC), dtype=real_part.dtype).at[slice_index, cells].add(emit_real)
        deposit_imag = jnp.zeros((count, NR * NC), dtype=real_part.dtype).at[slice_index, cells].add(emit_imag)
        real_part = real_part + source_gain * deposit_real.reshape(count, NR, NC)
        imag_part = imag_part + source_gain * deposit_imag.reshape(count, NR, NC)
        real_part, imag_part = sweep_columns(col_prop, real_part, imag_part)
        real_part, imag_part = sweep_rows(row_prop, real_part, imag_part)
    bunching = jnp.stack(partials) * (ELEC ** -0.5)
    return jnp.stack([real_part, imag_part]), phase, energy, bunching
```

```python
import jax
import jax.numpy as jnp
from jax import lax
from jax.experimental import pallas as pl
from jax.experimental.pallas import tpu as pltpu
from jax.sharding import PartitionSpec as P

F32 = jnp.float32
BF16 = jnp.bfloat16
MESH = pl.DeviceIdType.MESH
ELEC = 8192
PLANES = 16
CUTS = 32
SLOTS = 256
kick_rate = 0.5
source_gain = 0.5


def split(x):
    high = x.astype(BF16)
    return high, (x - high.astype(F32)).astype(BF16)


def kernel(shifts, field_in, row_in, col_in, phase_in, energy_in, cells_in,
           field_out, phase_out, energy_out, sums_out,
           own, halo, rowp, colp, ph_in, en_in, ce_in,
           mh, ml, ah, al,
           cell_f, row_i, col_i, onehot, fld, gx, gown, goth,
           samp, emit, state, xst, xce, rxst, rxce, rst, rce, efin, fin, rfld, rel, rsum,
           lsem, s_halo, r_halo, s_a2a, r_a2a, s_fwd, r_fwd, s_ex, r_ex,
           s_xst, r_xst, s_xce, r_xce, s_st, r_st, s_ce, r_ce,
           s_fld, r_fld, s_el, r_el, s_sum, r_sum):
    c = lax.axis_index("cuts")
    b = lax.axis_index("row")
    z = c // 2
    h = c % 2
    slot = z * 16 + b
    half = b // 8
    place = b % 8
    sends = []

    def coords(j, core):
        return (j // 16) * 2 + core, j % 16

    def remote(src, dst, ss, rs, dc, db):
        return pltpu.make_async_remote_copy(
            src_ref=src, dst_ref=dst, send_sem=ss, recv_sem=rs,
            device_id=(dc, db), device_id_type=MESH)

    def send(src, dst, ss, rs, dc, db, extra=None):
        here = (dc == c) & (db == b)
        there = jnp.logical_not(here)
        if extra is not None:
            here = here & extra
            there = there & extra

        @pl.when(there)
        def _():
            remote(src, dst, ss, rs, dc, db).start()

        @pl.when(here)
        def _():
            dst[...] = src[...]

        sends.append((there, src, dst, ss, rs))

    def sure_send(src, dst, ss, rs, dc, db):
        remote(src, dst, ss, rs, dc, db).start()
        sends.append((None, src, dst, ss, rs))

    def await_from(dst, ss, rs, dc, db):
        @pl.when(jnp.logical_not((dc == c) & (db == b)))
        def _():
            remote(dst, dst, ss, rs, dc, db).wait_recv()

    def sure_await(dst, ss, rs):
        remote(dst, dst, ss, rs, c, b).wait_recv()

    loads = [(field_in, own), (phase_in, ph_in), (energy_in, en_in), (cells_in, ce_in),
             (col_in, colp), (row_in, rowp)]
    loads = [pltpu.make_async_copy(src, dst, lsem.at[n]) for n, (src, dst) in enumerate(loads)]
    for copy in loads:
        copy.start()

    barrier = pltpu.get_barrier_semaphore()
    mine = 32 + h * 16 + b

    def greet(off, carry):
        peer = (mine + off) % 96
        dc = (z * 2 - 2 + peer // 16 + CUTS) % CUTS
        pl.semaphore_signal(barrier, inc=1, device_id=(dc, peer % 16), device_id_type=MESH)
        return carry

    lax.fori_loop(1, 96, greet, 0)

    for n in (1, 2, 3):
        loads[n].wait()
    for u in range(8):
        for i in range(4):
            lanes = slice(128 * i, 128 * i + 128)
            at = 4 * u + i
            cell = ce_in[u:u + 1, lanes]
            xce[u, i:i + 1, :] = cell.astype(F32)
            row_i[at:at + 1, :] = (cell // 256) & 15
            col_i[at:at + 1, :] = cell & 255
            state[at:at + 1, :] = ph_in[u:u + 1, lanes]
            state[32 + at:33 + at, :] = en_in[u:u + 1, lanes]
        xce[u, 4:8, :] = jnp.zeros((4, 128), F32)

    def build_onehot():
        iota = lax.broadcasted_iota(jnp.int32, (256, 128), 0)
        for u in range(8):
            for i in range(4):
                at = 4 * u + i
                hot = jnp.where(iota == col_i[at:at + 1, :], 1.0, 0.0)
                onehot[u, :, 128 * i:128 * i + 128] = hot.astype(BF16)

    build_onehot()
    loads[0].wait()
    pl.semaphore_wait(barrier, 95)

    nc = (c + 1) % CUTS
    sure_send(own.at[:, 6:8], halo, s_halo, r_halo, nc, b)
    for u in range(8):
        for k in (1, 2):
            j = (8 * c + u - k + SLOTS) % SLOTS
            dc, db = coords(j, half)
            send(xce.at[u], rxce.at[k - 1, place], s_xce.at[k - 1, u], r_xce.at[k - 1, place], dc, db)

    loads[4].wait()
    loads[5].wait()
    for part in range(2):
        ct = jnp.transpose(colp[part])
        if part == 0:
            places = ((0, 0, 1.0), (1, 1, 1.0))
        else:
            places = ((1, 0, -1.0), (0, 1, 1.0))
        hi, lo = split(ct)
        for kk, nn, sign in places:
            at = (slice(256 * kk, 256 * kk + 256), slice(256 * nn, 256 * nn + 256))
            mh[at] = hi if sign > 0 else -hi
            ml[at] = lo if sign > 0 else -lo
    rows = pl.ds(pl.multiple_of(h * 128, 128), 128)
    for side in range(2):
        cols = pl.ds(pl.multiple_of((h + side - 2 * h * side) * 128, 128), 128)
        rr = split(rowp[0, rows, cols])
        ri = split(rowp[1, rows, cols])
        for n, ref in ((0, ah), (1, al)):
            ref[side, 0:128, 0:128] = rr[n]
            ref[side, 0:128, 128:256] = -ri[n]
            ref[side, 128:256, 0:128] = ri[n]
            ref[side, 128:256, 128:256] = rr[n]

    def sample():
        for u in range(8):
            fu = fld[:, u].reshape(32, 256)
            hi, lo = split(fu)
            got = jnp.dot(jnp.concatenate([hi, lo], axis=0), onehot[u], preferred_element_type=F32)
            got = got[0:32] + got[32:64]
            iota = lax.broadcasted_iota(jnp.int32, (16, 128), 0)
            for i in range(4):
                at = 4 * u + i
                lanes = slice(128 * i, 128 * i + 128)
                mask = iota == row_i[at:at + 1, :]
                for part in range(2):
                    picked = jnp.where(mask, got[16 * part:16 * part + 16, lanes], 0.0)
                    samp[part, at:at + 1, :] = jnp.sum(picked, axis=0, keepdims=True)

    def deposit():
        for u in range(8):
            iota = lax.broadcasted_iota(jnp.int32, (16, 128), 0)
            pieces = []
            for i in range(4):
                at = 4 * u + i
                mask = iota == row_i[at:at + 1, :]
                pieces.append(jnp.concatenate(
                    [jnp.where(mask, emit[n, at:at + 1, :], 0.0).astype(BF16) for n in range(4)], axis=0))
            weights = jnp.concatenate(pieces, axis=1)
            add = lax.dot_general(weights, onehot[u], (((1,), (1,)), ((), ())), preferred_element_type=F32)
            fld[:, u] = fld[:, u] + (add[0:32] + add[32:64]).reshape(2, 16, 256)

    def kick(cosine, sine):
        energy = state[32:64, :] - kick_rate * (samp[0] * cosine - samp[1] * sine)
        phase = state[0:32, :] + energy
        state[0:32, :] = phase
        state[32:64, :] = energy
        cosine, sine = jnp.cos(phase), jnp.sin(phase)
        for n, value in ((0, source_gain * cosine), (1, -source_gain * sine)):
            high = value.astype(BF16).astype(F32)
            emit[n] = high
            emit[2 + n] = value - high
        return cosine, sine

    def add_sums(period, cosine, sine):
        line = lax.broadcasted_iota(jnp.int32, (8, 128), 0)
        total = state[64:72, :]
        total = total + jnp.where(line == 2 * period, jnp.sum(cosine, axis=0, keepdims=True), 0.0)
        total = total + jnp.where(line == 2 * period + 1, -jnp.sum(sine, axis=0, keepdims=True), 0.0)
        state[64:72, :] = total

    def sweep_cols(target, after):
        f = fld[...].reshape(2, 128, 256)
        parts = [split(f[0]), split(f[1])]
        lh = jnp.concatenate([parts[0][0], parts[1][0]], axis=1)
        ll = jnp.concatenate([parts[0][1], parts[1][1]], axis=1)
        for part in range(2):
            lanes = slice(256 * part, 256 * part + 256)
            g = jnp.dot(lh, mh[:, lanes], preferred_element_type=F32)
            g = g + jnp.dot(lh, ml[:, lanes], preferred_element_type=F32)
            g = g + jnp.dot(ll, mh[:, lanes], preferred_element_type=F32)
            target[part] = g.reshape(8, 16, 256)
            after(part)

    def rows_of(side, g):
        hi, lo = split(g)
        out = jnp.dot(ah[side], hi, preferred_element_type=F32)
        out = out + jnp.dot(al[side], hi, preferred_element_type=F32)
        return out + jnp.dot(ah[side], lo, preferred_element_type=F32)

    sure_await(halo, s_halo, r_halo)
    one = shifts[0] == 1
    for u in range(8):
        if u == 0:
            near, far = halo[:, 1], halo[:, 0]
            near = jnp.where(c > 0, near, 0.0)
            far = jnp.where(c > 0, far, 0.0)
        elif u == 1:
            near, far = own[:, 0], jnp.where(c > 0, halo[:, 1], 0.0)
        else:
            near, far = own[:, u - 1], own[:, u - 2]
        fld[:, u] = jnp.where(one, near, far)
    sample()
    kick(jnp.cos(state[0:32, :]), jnp.sin(state[0:32, :]))
    for u in range(8):
        xst[u, 0:4, :] = state[4 * u:4 * u + 4, :]
        xst[u, 4:8, :] = state[32 + 4 * u:36 + 4 * u, :]
    for u in range(8):
        for k in (1, 2):
            j = (8 * c + u - k + SLOTS) % SLOTS
            dc, db = coords(j, half)
            send(xst.at[u], rxst.at[k - 1, place], s_xst.at[k - 1, u], r_xst.at[k - 1, place], dc, db)
    deposit()
    sweep_cols(gx, lambda part: None)
    for u in range(8):
        send(gx.at[:, u], gown.at[0, :, place], s_a2a.at[u], r_a2a.at[place], z * 2 + half, 8 * h + u)

    partner = c + 1 - 2 * h
    for v in range(8):
        await_from(gown.at[0, :, v], s_a2a.at[v], r_a2a.at[v], z * 2 + half, 8 * h + v)
        sure_send(gown.at[0, :, v], goth.at[0, :, v], s_fwd.at[v], r_fwd.at[v], partner, b)
    acc = rows_of(0, gown[0].reshape(256, 256))
    for v in range(8):
        sure_await(goth.at[0, :, v], s_fwd.at[v], r_fwd.at[v])
    acc = acc + rows_of(1, goth[0].reshape(256, 256))

    moved = 0
    for period in range(1, 4):
        one = shifts[period] == 1
        moved = moved + shifts[period]
        fresh = ((slot + moved) & 255) < shifts[period]
        fld[...] = jnp.where(fresh, 0.0, acc).reshape(2, 8, 16, 256)
        if period == 1:
            for k in (1, 2):
                for v in range(8):
                    j = (slot + k) % SLOTS
                    dc, db = j // 8, 8 * h + v
                    await_from(rxce.at[k - 1, v], s_xce.at[k - 1, v], r_xce.at[k - 1, v], dc, db)
                    await_from(rxst.at[k - 1, v], s_xst.at[k - 1, v], r_xst.at[k - 1, v], dc, db)
            for v in range(8):
                tile = jnp.where(one, rxst[0, v], rxst[1, v])
                state[4 * v:4 * v + 4, :] = tile[0:4]
                state[32 + 4 * v:36 + 4 * v, :] = tile[4:8]
                cell_f[0, 4 * v:4 * v + 4, :] = jnp.where(one, rxce[0, v], rxce[1, v])[0:4]
            state[64:72, :] = jnp.zeros((8, 128), F32)
        else:
            for k in (1, 2):
                sure_await(rce.at[period - 2, k - 1], s_ce.at[period - 2, k - 1], r_ce.at[period - 2, k - 1])
                sure_await(rst.at[period - 2, k - 1], s_st.at[period - 2, k - 1], r_st.at[period - 2, k - 1])
            state[...] = jnp.where(one, rst[period - 2, 0], rst[period - 2, 1])
            cell_f[period - 1] = jnp.where(one, rce[period - 2, 0], rce[period - 2, 1])
        if period < 3:
            for k in (1, 2):
                dc, db = coords((slot - k + SLOTS) % SLOTS, h)
                sure_send(cell_f.at[period - 1], rce.at[period - 1, k - 1],
                          s_ce.at[period - 1, k - 1], r_ce.at[period - 1, k - 1], dc, db)
        cell = cell_f[period - 1].astype(jnp.int32)
        row_i[...] = (cell // 256) & 15
        col_i[...] = cell & 255
        build_onehot()
        sample()
        cosine, sine = jnp.cos(state[0:32, :]), jnp.sin(state[0:32, :])
        add_sums(period - 1, cosine, sine)
        cosine, sine = kick(cosine, sine)
        if period < 3:
            efin_at = period - 1
            efin[efin_at] = state[...]
            for k in (1, 2):
                dc, db = coords((slot - k + SLOTS) % SLOTS, h)
                sure_send(efin.at[efin_at], rst.at[period - 1, k - 1],
                          s_st.at[period - 1, k - 1], r_st.at[period - 1, k - 1], dc, db)
        else:
            add_sums(3, cosine, sine)
            efin[2] = state[...]
            for v in range(8):
                xst2 = jnp.concatenate([state[4 * v:4 * v + 4, :], state[32 + 4 * v:36 + 4 * v, :]], axis=0)
                efin[3, 8 * v:8 * v + 8, :] = xst2
            c1, c2 = (slot + 3) // 8, (slot + 6) // 8
            for n, cc in ((0, c1), (1, c2)):
                extra = None if n == 0 else c1 != c2
                w = slot - 8 * cc + 6
                dc = cc % CUTS
                for v in range(8):
                    send(efin.at[3, 8 * v:8 * v + 8], rel.at[w], s_el.at[n, v], r_el.at[w], dc, 8 * h + v, extra)
                for v in range(16):
                    send(efin.at[2, 64:72], rsum.at[w, h], s_sum.at[n, v], r_sum.at[w, h], dc, v, extra)
        deposit()

        def exchange(part, period=period):
            sure_send(gown.at[period, part], goth.at[period, part],
                      s_ex.at[period - 1, part], r_ex.at[period - 1, part], partner, b)

        sweep_cols(gown.at[period], exchange)
        acc = rows_of(0, gown[period].reshape(256, 256))
        for part in range(2):
            sure_await(goth.at[period, part], s_ex.at[period - 1, part], r_ex.at[period - 1, part])
        acc = acc + rows_of(1, goth[period].reshape(256, 256))

    fin[...] = acc.reshape(2, 8, 16, 256)
    c1, c2 = (slot + 3) // 8, (slot + 6) // 8
    for n, cc in ((0, c1), (1, c2)):
        extra = None if n == 0 else c1 != c2
        w = slot - 8 * cc + 6
        dc = cc % CUTS
        for v in range(8):
            send(fin.at[:, v], rfld.at[w], s_fld.at[n, v], r_fld.at[w], dc, 8 * h + v, extra)

    for w in range(11):
        j = (8 * c - 6 + w + SLOTS) % SLOTS
        for core in range(2):
            dc, db = coords(j, core)
            await_from(rsum.at[w, core], s_sum.at[0, 0], r_sum.at[w, core], dc, db)
        dc, db = coords(j, half)
        await_from(rel.at[w], s_el.at[0, 0], r_el.at[w], dc, db)
    base = jnp.clip(6 - moved, 0, 3)
    lane = lax.broadcasted_iota(jnp.int32, (8, 8), 1)
    sums = jnp.zeros((8, 8), F32)
    for u in range(8):
        tile = rel[base + u]
        for i in range(4):
            lanes = slice(128 * i, 128 * i + 128)
            phase_out[u:u + 1, lanes] = tile[i:i + 1]
            energy_out[u:u + 1, lanes] = tile[4 + i:5 + i]
        pair = rsum[base + u]
        total = jnp.sum(pair[0] + pair[1], axis=1, keepdims=True)
        sums = jnp.where(lane == u, total, sums)
    sums_out[...] = sums * ELEC ** (-0.5)
    for w in range(11):
        j = (8 * c - 6 + w + SLOTS) % SLOTS
        dc, db = coords(j, half)
        await_from(rfld.at[w], s_fld.at[0, 0], r_fld.at[w], dc, db)
    for u in range(8):
        field_out[:, u] = rfld[base + u]

    for there, src, dst, ss, rs in sends:
        copy = remote(src, dst, ss, rs, c, b)
        if there is None:
            copy.wait_send()
        else:
            @pl.when(there)
            def _():
                copy.wait_send()


def shards(field, row_prop, col_prop, phase, energy, cells, shifts):
    V = pltpu.VMEM
    D = pltpu.SemaphoreType.DMA
    blocks = (2, 8, 16, 256)
    scratch = [
        V(blocks, F32), V((2, 2, 16, 256), F32), V((2, 256, 256), F32), V((2, 256, 256), F32),
        V((8, 512), F32), V((8, 512), F32), V((8, 512), jnp.int32),
        V((512, 512), BF16), V((512, 512), BF16), V((2, 256, 256), BF16), V((2, 256, 256), BF16),
        V((3, 32, 128), F32), V((32, 128), jnp.int32), V((32, 128), jnp.int32),
        V((8, 256, 512), BF16), V(blocks, F32), V(blocks, F32), V((4, *blocks), F32), V((4, *blocks), F32),
        V((2, 32, 128), F32), V((4, 32, 128), F32), V((72, 128), F32),
        V((8, 8, 128), F32), V((8, 8, 128), F32), V((2, 8, 8, 128), F32), V((2, 8, 8, 128), F32),
        V((2, 2, 72, 128), F32), V((2, 2, 32, 128), F32), V((4, 72, 128), F32),
        V(blocks, F32), V((11, 2, 16, 256), F32), V((11, 8, 128), F32), V((11, 2, 8, 128), F32),
        D((6,)), D, D, D((8,)), D((8,)), D((8,)), D((8,)), D((3, 2)), D((3, 2)),
        D((2, 8)), D((2, 8)), D((2, 8)), D((2, 8)), D((2, 2)), D((2, 2)), D((2, 2)), D((2, 2)),
        D((2, 8)), D((11,)), D((2, 8)), D((11,)), D((2, 16)), D((11, 2)),
    ]
    hbm = pl.BlockSpec(memory_space=pl.ANY)
    vmem = pl.BlockSpec(memory_space=pltpu.VMEM)
    out = pl.pallas_call(
        kernel,
        out_shape=(jax.ShapeDtypeStruct(blocks, F32), jax.ShapeDtypeStruct((8, 512), F32),
                   jax.ShapeDtypeStruct((8, 512), F32), jax.ShapeDtypeStruct((8, 8), F32)),
        in_specs=[pl.BlockSpec(memory_space=pltpu.SMEM)] + [hbm] * 6,
        out_specs=(vmem, vmem, vmem, vmem),
        scratch_shapes=scratch,
        compiler_params=pltpu.CompilerParams(
            collective_id=0, has_side_effects=True, vmem_limit_bytes=48 << 20),
    )(shifts, field, row_prop, col_prop, phase, energy, cells)
    return out[0], out[1], out[2], out[3].reshape(4, 2, 8)


def solution(mesh):
    return jax.shard_map(
        shards,
        mesh=mesh,
        in_specs=(
            P(None, "cuts", "row", None),
            P(),
            P(),
            P("cuts", "row"),
            P("cuts", "row"),
            P("cuts", "row"),
            P(),
        ),
        out_specs=(
            P(None, "cuts", "row", None),
            P("cuts", "row"),
            P("cuts", "row"),
            P(None, None, "cuts"),
        ),
        check_vma=False,
    )
```

```python
import jax
import jax.numpy as jnp
from jax import lax
from jax.experimental import pallas as pl
from jax.experimental.pallas import tpu as pltpu
from jax.sharding import PartitionSpec as P

F32 = jnp.float32
BF16 = jnp.bfloat16
MESH = pl.DeviceIdType.MESH
ELEC = 8192
CUTS = 32
SLOTS = 256
VMEM_LIMIT = 67_000_000
kick_rate = 0.5
source_gain = 0.5


def split(x):
    high = x.astype(BF16)
    return high, (x - high.astype(F32)).astype(BF16)


PATH = (0, 1, 5, 6, 10, 11, 15, 12, 8, 4, 7, 3, 2, 14, 13, 9)


def lookup(table, i):
    low = sum(n << (3 * (q % 8)) for q, n in enumerate(t % 8 for t in table[:8]))
    high = sum(n << (3 * (q % 8)) for q, n in enumerate(t % 8 for t in table[8:]))
    tops = sum((t // 8) << q for q, t in enumerate(table))
    word = jnp.where(i < 8, low, high)
    return ((word >> (3 * (i % 8))) & 7) + 8 * ((tops >> i) & 1)


def chip_of(j):
    z, at = j // 16, lookup(PATH, j % 16)
    return z, (at % 4 + z) % 4 + 4 * ((at // 4 + 2 * z) % 4)


def slot_of(z, b):
    at = (b % 4 + 3 * z) % 4 + 4 * ((b // 4 + 2 * z) % 4)
    return z * 16 + lookup(tuple(PATH.index(q) for q in range(16)), at)


def kernel(shifts_in, field_in, row_in, col_in, phase_in, energy_in, cells_in,
           field_out, phase_out, energy_out, sums_out,
           own, rowp, colp, ph_in, en_in, ce_in, mh, ml, ah, al,
           key_i, col_f, onehot, fld, arr, gown, goth, samp, emit, state, cell_f,
           shifts, out_sums, out_ph, out_en, out_fld, xel, rxel, sst, rst, rce, psum, psum_in, efin, fin, rfld, rel,
           lsem, s_a2a, r_a2a, s_xel, r_xel, s_ex, r_ex, s_st, r_st, s_ce, r_ce,
           s_ps, r_ps, s_fld, r_fld, s_el, r_el):
    c = lax.axis_index("cuts")
    b = lax.axis_index("row")
    z = c // 2
    h = c % 2
    half = b // 8
    place = b % 8
    slot = slot_of(z, b)
    group = (slot // 8) % 2
    base_cut = slot // 8
    partner = c + 1 - 2 * h
    sends = []
    scope = []

    def mark(name):
        if scope:
            scope.pop().__exit__(None, None, None)
        if name:
            scope.append(jax.named_scope(name))
            scope[0].__enter__()

    def remote(src, dst, ss, rs, dc, db):
        return pltpu.make_async_remote_copy(
            src_ref=src, dst_ref=dst, send_sem=ss, recv_sem=rs,
            device_id=(dc, db), device_id_type=MESH)

    def send(src, dst, ss, rs, dc, db, extra=None):
        here = (dc == c) & (db == b)
        there = jnp.logical_not(here)
        if extra is not None:
            here = here & extra
            there = there & extra

        @pl.when(there)
        def _():
            remote(src, dst, ss, rs, dc, db).start()

        @pl.when(here)
        def _():
            dst[...] = src[...]

        sends.append((there, src, dst, ss, rs))

    def sure_send(src, dst, ss, rs, dc, db):
        remote(src, dst, ss, rs, dc, db).start()
        sends.append((None, src, dst, ss, rs))

    def await_from(dst, ss, rs, dc, db):
        @pl.when(jnp.logical_not((dc == c) & (db == b)))
        def _():
            remote(dst, dst, ss, rs, dc, db).wait_recv()

    def sure_await(dst, ss, rs):
        remote(dst, dst, ss, rs, c, b).wait_recv()

    mark("start")
    loads = [(phase_in, ph_in), (energy_in, en_in), (cells_in, ce_in), (field_in, own),
             (col_in, colp), (row_in, rowp), (shifts_in, shifts)]
    loads = [pltpu.make_async_copy(src, dst, lsem.at[n]) for n, (src, dst) in enumerate(loads)]
    for copy in loads:
        copy.start()

    barrier = pltpu.get_barrier_semaphore()
    below = (base_cut + 1) % CUTS
    itself = (half == h) & ((base_cut == c) | ((below == c) & (slot % 8 >= 6)))
    def greet(dc, extra=None):
        for v in range(8):
            ok = jnp.logical_not((dc == c) & (8 * h + v == b))

            @pl.when(ok if extra is None else ok & extra)
            def _():
                pl.semaphore_signal(barrier, inc=1, device_id=(dc, 8 * h + v), device_id_type=MESH)

    greet(base_cut)
    greet(below, slot % 8 >= 6)
    for k in (1, 2):
        pz, pb = chip_of((slot + k) % SLOTS)
        pl.semaphore_signal(barrier, inc=1, device_id=(pz * 2 + h, pb), device_id_type=MESH)
    pl.semaphore_signal(barrier, inc=1, device_id=(partner, b), device_id_type=MESH)
    pl.semaphore_signal(barrier, inc=1, device_id=((c + CUTS - 1) % CUTS, b), device_id_type=MESH)

    mark("unpack")
    for n in (0, 1, 2):
        loads[n].wait()
    for u in range(8):
        for i in range(4):
            lanes = slice(128 * i, 128 * i + 128)
            xel[u, i:i + 1, :] = ph_in[u:u + 1, lanes]
            xel[u, 4 + i:5 + i, :] = en_in[u:u + 1, lanes]
            xel[u, 8 + i:9 + i, :] = ce_in[u:u + 1, lanes].astype(F32)
        xel[u, 12:16, :] = jnp.zeros((4, 128), F32)

    mark("w_barrier")
    loads[3].wait()
    pl.semaphore_wait(barrier, 14 - jnp.where(itself, 1, 0))

    mark("send0")
    for i in range(8):
        u = (place + i) % 8
        for k in (1, 2):
            pz, pb = chip_of((8 * c + u - k + SLOTS) % SLOTS)
            send(xel.at[u], rxel.at[k - 1, place], s_xel.at[k - 1, u], r_xel.at[k - 1, place], pz * 2 + half, pb)
    for i in range(8):
        u = (place + i) % 8
        _, db = chip_of(8 * c + u)
        send(own.at[:, u], arr.at[:, place], s_a2a.at[u], r_a2a.at[place], z * 2 + half, db)

    mark("prep")
    loads[4].wait()
    loads[5].wait()
    for part in range(2):
        hi, lo = split(jnp.transpose(colp[part]))
        places = ((0, 0, 1), (1, 1, 1)) if part == 0 else ((1, 0, -1), (0, 1, 1))
        for kk, nn, sign in places:
            at = (slice(256 * kk, 256 * kk + 256), slice(256 * nn, 256 * nn + 256))
            mh[at] = hi if sign > 0 else -hi
            ml[at] = lo if sign > 0 else -lo
    rows = pl.ds(pl.multiple_of(h * 128, 128), 128)
    for side in range(2):
        cols = pl.ds(pl.multiple_of((h + side - 2 * h * side) * 128, 128), 128)
        rr = split(rowp[0, rows, cols])
        ri = split(rowp[1, rows, cols])
        for n, ref in ((0, ah), (1, al)):
            ref[side, 0:128, 0:128] = rr[n]
            ref[side, 0:128, 128:256] = -ri[n]
            ref[side, 128:256, 0:128] = ri[n]
            ref[side, 128:256, 128:256] = rr[n]

    def build_onehot(period):
        if period < 3:
            relay(cell_f.at[period], rce, s_ce, r_ce, period)
        cell = cell_f[period].astype(jnp.int32)
        key_i[...] = ((cell >> 8) & 15) + ((cell >> 7) & 1) * 16
        col_f[...] = (cell & 127).astype(F32)
        iota = lax.broadcasted_iota(jnp.int32, (128, 128), 0).astype(F32).astype(BF16)
        for u in range(8):
            for i in range(4):
                at = 4 * u + i
                col = jnp.broadcast_to(col_f[at:at + 1, :], (128, 128)).astype(BF16)
                onehot[u, :, 128 * i:128 * i + 128] = jnp.where(iota == col, 1.0, 0.0).astype(BF16)

    def relay(src, dst, ss, rs, period):
        for k in (1, 2):
            pz, pb = chip_of((slot - k + SLOTS) % SLOTS)
            sure_send(src, dst.at[period, k - 1], ss.at[period, k - 1], rs.at[period, k - 1], pz * 2 + h, pb)

    def sample():
        iota = lax.broadcasted_iota(jnp.int32, (32, 128), 0)
        for u in range(8):
            fu = jnp.concatenate([fld[p, u, :, 128 * q:128 * q + 128] for p in range(2) for q in range(2)], axis=0)
            hi, lo = split(fu)
            got = jnp.dot(jnp.concatenate([hi, lo], axis=0), onehot[u], preferred_element_type=F32)
            got = got[0:64] + got[64:128]
            for i in range(4):
                at = 4 * u + i
                lanes = slice(128 * i, 128 * i + 128)
                mask = iota == key_i[at:at + 1, :]
                for part in range(2):
                    picked = jnp.where(mask, got[32 * part:32 * part + 32, lanes], 0.0)
                    samp[part, at:at + 1, :] = jnp.sum(picked, axis=0, keepdims=True)

    def deposit():
        iota = lax.broadcasted_iota(jnp.int32, (32, 128), 0)
        for u in range(8):
            pieces = []
            for i in range(4):
                at = 4 * u + i
                mask = iota == key_i[at:at + 1, :]
                pieces.append(jnp.concatenate(
                    [jnp.where(mask, emit[n, at:at + 1, :], 0.0).astype(BF16) for n in range(4)], axis=0))
            weights = jnp.concatenate(pieces, axis=1)
            add = lax.dot_general(weights, onehot[u], (((1,), (1,)), ((), ())), preferred_element_type=F32)
            add = add[0:64] + add[64:128]
            for p in range(2):
                for q in range(2):
                    lanes = slice(128 * q, 128 * q + 128)
                    rows = slice(32 * p + 16 * q, 32 * p + 16 * q + 16)
                    fld[p, u, :, lanes] = fld[p, u, :, lanes] + add[rows]

    def kick(period):
        cosine, sine = jnp.cos(state[0:32, :]), jnp.sin(state[0:32, :])
        energy = state[32:64, :] - kick_rate * (samp[0] * cosine - samp[1] * sine)
        phase = state[0:32, :] + energy
        cosine, sine = jnp.cos(phase), jnp.sin(phase)
        line = lax.broadcasted_iota(jnp.int32, (8, 128), 0)
        total = state[64:72, :]
        total = total + jnp.where(line == 2 * period, jnp.sum(cosine, axis=0, keepdims=True), 0.0)
        total = total + jnp.where(line == 2 * period + 1, -jnp.sum(sine, axis=0, keepdims=True), 0.0)
        for n, value in ((0, source_gain * cosine), (1, -source_gain * sine)):
            high = value.astype(BF16).astype(F32)
            emit[n] = high
            emit[2 + n] = value - high
        return phase, energy, total

    def sweep_cols(target):
        f = fld[...].reshape(2, 128, 256)
        parts = [split(f[0]), split(f[1])]
        lh = jnp.concatenate([parts[0][0], parts[1][0]], axis=1)
        ll = jnp.concatenate([parts[0][1], parts[1][1]], axis=1)
        for part in range(2):
            lanes = slice(256 * part, 256 * part + 256)
            g = jnp.dot(lh, mh[:, lanes], preferred_element_type=F32)
            g = g + jnp.dot(lh, ml[:, lanes], preferred_element_type=F32)
            g = g + jnp.dot(ll, mh[:, lanes], preferred_element_type=F32)
            target[part] = g.reshape(8, 16, 256)

    def rows_of(side, g):
        hi, lo = split(g)
        out = jnp.dot(ah[side], hi, preferred_element_type=F32)
        out = out + jnp.dot(al[side], hi, preferred_element_type=F32)
        return out + jnp.dot(ah[side], lo, preferred_element_type=F32)

    def to_rows(source, dst, ss, rs):
        c1, c2 = (slot + 5) // 8, (slot + 8) // 8
        for i in range(8):
            v = (place + i) % 8
            for n, cc in ((0, c1), (1, c2)):
                extra = None if n == 0 else c1 != c2
                w = slot - 8 * cc + 8
                send(source(v), dst.at[w], ss.at[n, v], rs.at[w], cc % CUTS, 8 * h + v, extra)

    def cells_for(period):
        mark("w_ce")
        for k in (1, 2):
            sure_await(rce.at[period - 1, k - 1], s_ce.at[period - 1, k - 1], r_ce.at[period - 1, k - 1])
        mark("hot")
        cell_f[period] = jnp.where(shifts[period] == 1, rce[period - 1, 0], rce[period - 1, 1])
        build_onehot(period)

    mark("w_xel")
    for k in (1, 2):
        for v in range(8):
            await_from(rxel.at[k - 1, v], s_xel.at[k - 1, v], r_xel.at[k - 1, v],
                       ((slot + k) % SLOTS) // 8, 8 * h + v)
    loads[6].wait()
    mark("first")
    one = shifts[0] == 1
    for v in range(8):
        tile = jnp.where(one, rxel[0, v], rxel[1, v])
        state[4 * v:4 * v + 4, :] = tile[0:4]
        state[32 + 4 * v:36 + 4 * v, :] = tile[4:8]
        cell_f[0, 4 * v:4 * v + 4, :] = tile[8:12]
    state[64:72, :] = jnp.zeros((8, 128), F32)
    build_onehot(0)
    moved = 0
    acc = None
    for period in range(4):
        one = shifts[period] == 1
        moved = moved + shifts[period]
        fresh = ((slot + moved) & 255) < shifts[period]
        if period > 0:
            mark("w_st")
            for k in (1, 2):
                sure_await(rst.at[period - 1, k - 1], s_st.at[period - 1, k - 1], r_st.at[period - 1, k - 1])
            state[...] = jnp.where(one, rst[period - 1, 0], rst[period - 1, 1])
        if period == 0:
            mark("w_a2a")
            for v in range(8):
                await_from(arr.at[:, v], s_a2a.at[v], r_a2a.at[v], z * 2 + group, 8 * h + v)
            fld[...] = jnp.where(fresh, 0.0, arr[...])
        else:
            fld[...] = jnp.where(fresh, 0.0, acc).reshape(2, 8, 16, 256)
        mark("samp")
        sample()
        mark("kick")
        phase, energy, total = kick(period)
        if period < 3:
            sst[period, 0:32, :] = phase
            sst[period, 32:64, :] = energy
            sst[period, 64:72, :] = total
            relay(sst.at[period], rst, s_st, r_st, period)
        else:
            state[0:32, :] = phase
            state[32:64, :] = energy
            psum[...] = total
            sure_send(psum, psum_in, s_ps, r_ps, partner, b)
        mark("dep")
        deposit()

        mark("col")
        sweep_cols(gown.at[period])
        for part in range(2):
            sure_send(gown.at[period, part], goth.at[period, part],
                      s_ex.at[period, part], r_ex.at[period, part], partner, b)
        mark("rowown")
        acc = rows_of(0, gown[period].reshape(256, 256))
        if period < 3:
            cells_for(period + 1)
        else:
            mark("elsend")
            sure_await(psum_in, s_ps, r_ps)
            total = psum[...] + psum_in[...]
            for v in range(8):
                efin[v, 0:4, :] = state[4 * v:4 * v + 4, :]
                efin[v, 4:8, :] = state[32 + 4 * v:36 + 4 * v, :]
                efin[v, 8:16, :] = total
            to_rows(lambda v: efin.at[v], rel, s_el, r_el)
        mark("w_ex")
        for part in range(2):
            sure_await(goth.at[period, part], s_ex.at[period, part], r_ex.at[period, part])
        mark("rowoth")
        acc = acc + rows_of(1, goth[period].reshape(256, 256))

    mark("fsend")
    fin[...] = acc.reshape(2, 8, 16, 256)
    to_rows(lambda v: fin.at[:, v], rfld, s_fld, r_fld)

    mark("w_small")
    for w in range(11):
        j = (8 * c - 8 + w + SLOTS) % SLOTS
        pz, pb = chip_of(j)
        await_from(rel.at[w], s_el.at[0, 0], r_el.at[w], pz * 2 + half, pb)
    mark("smallout")
    base = jnp.clip(8 - moved, 0, 3)
    lane = lax.broadcasted_iota(jnp.int32, (8, 8), 1)
    sums = jnp.zeros((8, 8), F32)
    for u in range(8):
        tile = rel[base + u]
        for i in range(4):
            lanes = slice(128 * i, 128 * i + 128)
            out_ph[u:u + 1, lanes] = tile[i:i + 1]
            out_en[u:u + 1, lanes] = tile[4 + i:5 + i]
        sums = jnp.where(lane == u, jnp.sum(tile[8:16], axis=1, keepdims=True), sums)
    out_sums[...] = sums * ELEC ** (-0.5)
    stores = [(out_ph, phase_out), (out_en, energy_out), (out_sums, sums_out), (out_fld, field_out)]
    stores = [pltpu.make_async_copy(src, dst, lsem.at[7 + n]) for n, (src, dst) in enumerate(stores)]
    for copy in stores[:3]:
        copy.start()
    mark("w_fld")
    for w in range(11):
        j = (8 * c - 8 + w + SLOTS) % SLOTS
        pz, pb = chip_of(j)
        await_from(rfld.at[w], s_fld.at[0, 0], r_fld.at[w], pz * 2 + half, pb)
    mark("fout")
    for u in range(8):
        out_fld[:, u] = rfld[base + u]
    stores[3].start()

    mark("drain")
    for there, src, dst, ss, rs in sends:
        copy = remote(src, dst, ss, rs, c, b)
        if there is None:
            copy.wait_send()
        else:
            @pl.when(there)
            def _():
                copy.wait_send()
    for copy in stores:
        copy.wait()
    mark(None)


def hand_over(field, phase, energy, sums, field_out, phase_out, energy_out, bunching_out,
              a, p, e, q, out, sem):
    ins = [(field, a), (phase, p), (energy, e), (sums, q)]
    outs = [(a, field_out), (p, phase_out), (e, energy_out), (out, bunching_out)]
    ins = [pltpu.make_async_copy(src, dst, sem.at[n]) for n, (src, dst) in enumerate(ins)]
    outs = [pltpu.make_async_copy(src, dst, sem.at[4 + n]) for n, (src, dst) in enumerate(outs)]
    for copy in ins:
        copy.start()
    for n in (3, 1, 2, 0):
        ins[n].wait()
        if n == 3:
            for period in range(4):
                out[period] = q[2 * period:2 * period + 2]
        outs[n].start()
    for copy in outs:
        copy.wait()


def shards(field, row_prop, col_prop, phase, energy, cells, shifts):
    V = pltpu.VMEM
    D = pltpu.SemaphoreType.DMA
    blocks = (2, 8, 16, 256)
    square = (2, 256, 256)
    scratch = [
        V(blocks, F32), V(square, F32), V(square, F32),
        V((8, 512), F32), V((8, 512), F32), V((8, 512), jnp.int32),
        V((512, 512), BF16), V((512, 512), BF16), V(square, BF16), V(square, BF16),
        V((32, 128), jnp.int32), V((32, 128), F32), V((8, 128, 512), BF16),
        V(blocks, F32), V(blocks, F32), V((4, *blocks), F32), V((4, *blocks), F32),
        V((2, 32, 128), F32), V((4, 32, 128), F32), V((72, 128), F32), V((4, 32, 128), F32),
        pltpu.SMEM((4,), jnp.int32), V((8, 8), F32), V((8, 512), F32), V((8, 512), F32), V(blocks, F32),
        V((8, 16, 128), F32), V((2, 8, 16, 128), F32), V((3, 72, 128), F32),
        V((3, 2, 72, 128), F32), V((3, 2, 32, 128), F32), V((8, 128), F32), V((8, 128), F32),
        V((8, 16, 128), F32), V(blocks, F32), V((11, 2, 16, 256), F32), V((11, 16, 128), F32),
        D((11,)), D((8,)), D((8,)), D((2, 8)), D((2, 8)), D((4, 2)), D((4, 2)),
        D((3, 2)), D((3, 2)), D((3, 2)), D((3, 2)), D, D,
        D((2, 8)), D((11,)), D((2, 8)), D((11,)),
    ]
    hbm = pl.BlockSpec(memory_space=pl.ANY)
    results = (jax.ShapeDtypeStruct(blocks, F32), jax.ShapeDtypeStruct((8, 512), F32),
               jax.ShapeDtypeStruct((8, 512), F32))
    out = pl.pallas_call(
        kernel,
        out_shape=(*results, jax.ShapeDtypeStruct((8, 8), F32)),
        in_specs=[hbm] * 7,
        out_specs=[hbm] * 4,
        scratch_shapes=scratch,
        compiler_params=pltpu.CompilerParams(
            collective_id=0, has_side_effects=True, vmem_limit_bytes=VMEM_LIMIT),
    )(shifts, field, row_prop, col_prop, phase, energy, cells)
    return pl.pallas_call(
        hand_over,
        out_shape=(*results, jax.ShapeDtypeStruct((4, 2, 8), F32)),
        in_specs=[hbm] * 4,
        out_specs=[hbm] * 4,
        scratch_shapes=[V(blocks, F32), V((8, 512), F32), V((8, 512), F32), V((8, 8), F32),
                        V((4, 2, 8), F32), D((8,))],
        compiler_params=pltpu.CompilerParams(vmem_limit_bytes=VMEM_LIMIT),
    )(*out)


def solution(mesh):
    return jax.shard_map(
        shards,
        mesh=mesh,
        in_specs=(
            P(None, "cuts", "row", None),
            P(),
            P(),
            P("cuts", "row"),
            P("cuts", "row"),
            P("cuts", "row"),
            P(),
        ),
        out_specs=(
            P(None, "cuts", "row", None),
            P("cuts", "row"),
            P("cuts", "row"),
            P(None, None, "cuts"),
        ),
        check_vma=False,
    )
```

```python
import jax
import jax.numpy as jnp
from jax import lax
from jax.experimental import pallas as pl
from jax.experimental.pallas import tpu as pltpu
from jax.sharding import PartitionSpec as P

F32 = jnp.float32
BF16 = jnp.bfloat16
MESH = pl.DeviceIdType.MESH
ELEC = 8192
CUTS = 32
SLOTS = 256
VMEM_LIMIT = 67_000_000
kick_rate = 0.5
source_gain = 0.5


def split(x):
    high = x.astype(BF16)
    return high, (x - high.astype(F32)).astype(BF16)


PATH = (0, 1, 5, 6, 10, 11, 15, 12, 8, 4, 7, 3, 2, 14, 13, 9)


def lookup(table, i):
    low = sum(n << (3 * (q % 8)) for q, n in enumerate(t % 8 for t in table[:8]))
    high = sum(n << (3 * (q % 8)) for q, n in enumerate(t % 8 for t in table[8:]))
    tops = sum((t // 8) << q for q, t in enumerate(table))
    word = jnp.where(i < 8, low, high)
    return ((word >> (3 * (i % 8))) & 7) + 8 * ((tops >> i) & 1)


def chip_of(j):
    z, at = j // 16, lookup(PATH, j % 16)
    return z, (at % 4 + z) % 4 + 4 * ((at // 4 + 2 * z) % 4)


def slot_of(z, b):
    at = (b % 4 + 3 * z) % 4 + 4 * ((b // 4 + 2 * z) % 4)
    return z * 16 + lookup(tuple(PATH.index(q) for q in range(16)), at)


def kernel(shifts_in, field_in, row_in, col_in, phase_in, energy_in, cells_in,
           field_out, phase_out, energy_out, sums_out,
           own, rowp, colp, ph_in, en_in, ce_in, mh, ml, ah, al,
           key_i, col_f, onehot, fld, arr, gown, goth, samp, emit, state, cell_f,
           shifts, out_sums, out_ph, out_en, out_fld, xel, rxel, sst, rst, rce, psum, psum_in, efin, fin, rfld, rel,
           lsem, s_a2a, r_a2a, s_xel, r_xel, s_ex, r_ex, s_st, r_st, s_ce, r_ce,
           s_ps, r_ps, s_fld, r_fld, s_el, r_el):
    c = lax.axis_index("cuts")
    b = lax.axis_index("row")
    z = c // 2
    h = c % 2
    half = b // 8
    place = b % 8
    slot = slot_of(z, b)
    group = (slot // 8) % 2
    base_cut = slot // 8
    partner = c + 1 - 2 * h
    sends = []
    scope = []

    def mark(name):
        if scope:
            scope.pop().__exit__(None, None, None)
        if name:
            scope.append(jax.named_scope(name))
            scope[0].__enter__()

    def remote(src, dst, ss, rs, dc, db):
        return pltpu.make_async_remote_copy(
            src_ref=src, dst_ref=dst, send_sem=ss, recv_sem=rs,
            device_id=(dc, db), device_id_type=MESH)

    def send(src, dst, ss, rs, dc, db, extra=None):
        here = (dc == c) & (db == b)
        there = jnp.logical_not(here)
        if extra is not None:
            here = here & extra
            there = there & extra

        @pl.when(there)
        def _():
            remote(src, dst, ss, rs, dc, db).start()

        @pl.when(here)
        def _():
            dst[...] = src[...]

        sends.append((there, src, dst, ss, rs))

    def sure_send(src, dst, ss, rs, dc, db):
        remote(src, dst, ss, rs, dc, db).start()
        sends.append((None, src, dst, ss, rs))

    def await_from(dst, ss, rs, dc, db):
        @pl.when(jnp.logical_not((dc == c) & (db == b)))
        def _():
            remote(dst, dst, ss, rs, dc, db).wait_recv()

    def sure_await(dst, ss, rs):
        remote(dst, dst, ss, rs, c, b).wait_recv()

    mark("start")
    barrier = pltpu.get_barrier_semaphore()
    below = (base_cut + 1) % CUTS
    itself = (half == h) & ((base_cut == c) | ((below == c) & (slot % 8 >= 6)))
    def greet(dc, extra=None):
        for v in range(8):
            ok = jnp.logical_not((dc == c) & (8 * h + v == b))

            @pl.when(ok if extra is None else ok & extra)
            def _():
                pl.semaphore_signal(barrier, inc=1, device_id=(dc, 8 * h + v), device_id_type=MESH)

    greet(base_cut)
    greet(below, slot % 8 >= 6)
    for k in (1, 2):
        pz, pb = chip_of((slot + k) % SLOTS)
        pl.semaphore_signal(barrier, inc=1, device_id=(pz * 2 + h, pb), device_id_type=MESH)
    pl.semaphore_signal(barrier, inc=1, device_id=(partner, b), device_id_type=MESH)
    pl.semaphore_signal(barrier, inc=1, device_id=((c + CUTS - 1) % CUTS, b), device_id_type=MESH)

    loads = [(phase_in, ph_in), (energy_in, en_in), (cells_in, ce_in), (field_in, own),
             (col_in, colp), (row_in, rowp), (shifts_in, shifts)]
    loads = [pltpu.make_async_copy(src, dst, lsem.at[n]) for n, (src, dst) in enumerate(loads)]
    for copy in loads:
        copy.start()

    mark("unpack")
    for n in (0, 1, 2):
        loads[n].wait()
    for u in range(8):
        for i in range(4):
            lanes = slice(128 * i, 128 * i + 128)
            xel[u, 0, i:i + 1, :] = ph_in[u:u + 1, lanes]
            xel[u, 1, i:i + 1, :] = en_in[u:u + 1, lanes]
            xel[u, 2, i:i + 1, :] = ce_in[u:u + 1, lanes].astype(F32)

    mark("w_barrier")
    loads[3].wait()
    pl.semaphore_wait(barrier, 14 - jnp.where(itself, 1, 0))

    mark("send0")
    for i in range(8):
        u = (place + i) % 8
        for k in (1, 2):
            pz, pb = chip_of((8 * c + u - k + SLOTS) % SLOTS)
            send(xel.at[u], rxel.at[k - 1, place], s_xel.at[k - 1, u], r_xel.at[k - 1, place], pz * 2 + half, pb)
    for i in range(8):
        u = (place + i) % 8
        _, db = chip_of(8 * c + u)
        send(own.at[:, u], arr.at[:, place], s_a2a.at[u], r_a2a.at[place], z * 2 + half, db)

    mark("prep")
    loads[4].wait()
    loads[5].wait()
    for part in range(2):
        hi, lo = split(jnp.transpose(colp[part]))
        places = ((0, 0, 1), (1, 1, 1)) if part == 0 else ((1, 0, -1), (0, 1, 1))
        for kk, nn, sign in places:
            at = (slice(256 * kk, 256 * kk + 256), slice(256 * nn, 256 * nn + 256))
            mh[at] = hi if sign > 0 else -hi
            ml[at] = lo if sign > 0 else -lo
    rows = pl.ds(pl.multiple_of(h * 128, 128), 128)
    for side in range(2):
        cols = pl.ds(pl.multiple_of((h + side - 2 * h * side) * 128, 128), 128)
        rr = split(rowp[0, rows, cols])
        ri = split(rowp[1, rows, cols])
        for n, ref in ((0, ah), (1, al)):
            ref[side, 0:128, 0:128] = rr[n]
            ref[side, 0:128, 128:256] = -ri[n]
            ref[side, 128:256, 0:128] = ri[n]
            ref[side, 128:256, 128:256] = rr[n]

    def build_onehot(period):
        if period < 3:
            relay(cell_f.at[period], rce, s_ce, r_ce, period)
        cell = cell_f[period].astype(jnp.int32)
        key_i[...] = ((cell >> 8) & 15) + ((cell >> 7) & 1) * 16
        col_f[...] = (cell & 127).astype(F32)
        iota = lax.broadcasted_iota(jnp.int32, (128, 128), 0).astype(F32).astype(BF16)
        for u in range(8):
            for i in range(4):
                at = 4 * u + i
                col = jnp.broadcast_to(col_f[at:at + 1, :], (128, 128)).astype(BF16)
                onehot[u, :, 128 * i:128 * i + 128] = jnp.where(iota == col, 1.0, 0.0).astype(BF16)

    def relay(src, dst, ss, rs, period):
        for k in (1, 2):
            pz, pb = chip_of((slot - k + SLOTS) % SLOTS)
            sure_send(src, dst.at[period, k - 1], ss.at[period, k - 1], rs.at[period, k - 1], pz * 2 + h, pb)

    def sample():
        iota = lax.broadcasted_iota(jnp.int32, (32, 128), 0)
        for u in range(8):
            fu = jnp.concatenate([fld[p, u, :, 128 * q:128 * q + 128] for p in range(2) for q in range(2)], axis=0)
            hi, lo = split(fu)
            got = jnp.dot(jnp.concatenate([hi, lo], axis=0), onehot[u], preferred_element_type=F32)
            got = got[0:64] + got[64:128]
            for i in range(4):
                at = 4 * u + i
                lanes = slice(128 * i, 128 * i + 128)
                mask = iota == key_i[at:at + 1, :]
                for part in range(2):
                    picked = jnp.where(mask, got[32 * part:32 * part + 32, lanes], 0.0)
                    samp[part, at:at + 1, :] = jnp.sum(picked, axis=0, keepdims=True)

    def deposit():
        iota = lax.broadcasted_iota(jnp.int32, (32, 128), 0)
        for u in range(8):
            pieces = []
            for i in range(4):
                at = 4 * u + i
                mask = iota == key_i[at:at + 1, :]
                pieces.append(jnp.concatenate(
                    [jnp.where(mask, emit[n, at:at + 1, :], 0.0).astype(BF16) for n in range(4)], axis=0))
            weights = jnp.concatenate(pieces, axis=1)
            add = lax.dot_general(weights, onehot[u], (((1,), (1,)), ((), ())), preferred_element_type=F32)
            add = add[0:64] + add[64:128]
            for p in range(2):
                for q in range(2):
                    lanes = slice(128 * q, 128 * q + 128)
                    rows = slice(32 * p + 16 * q, 32 * p + 16 * q + 16)
                    fld[p, u, :, lanes] = fld[p, u, :, lanes] + add[rows]

    def kick(period):
        cosine, sine = jnp.cos(state[0:32, :]), jnp.sin(state[0:32, :])
        energy = state[32:64, :] - kick_rate * (samp[0] * cosine - samp[1] * sine)
        phase = state[0:32, :] + energy
        cosine, sine = jnp.cos(phase), jnp.sin(phase)
        line = lax.broadcasted_iota(jnp.int32, (8, 128), 0)
        total = state[64:72, :]
        total = total + jnp.where(line == 2 * period, jnp.sum(cosine, axis=0, keepdims=True), 0.0)
        total = total + jnp.where(line == 2 * period + 1, -jnp.sum(sine, axis=0, keepdims=True), 0.0)
        for n, value in ((0, source_gain * cosine), (1, -source_gain * sine)):
            high = value.astype(BF16).astype(F32)
            emit[n] = high
            emit[2 + n] = value - high
        return phase, energy, total

    def sweep_cols(target):
        f = fld[...].reshape(2, 128, 256)
        parts = [split(f[0]), split(f[1])]
        lh = jnp.concatenate([parts[0][0], parts[1][0]], axis=1)
        ll = jnp.concatenate([parts[0][1], parts[1][1]], axis=1)
        for part in range(2):
            lanes = slice(256 * part, 256 * part + 256)
            g = jnp.dot(lh, mh[:, lanes], preferred_element_type=F32)
            g = g + jnp.dot(lh, ml[:, lanes], preferred_element_type=F32)
            g = g + jnp.dot(ll, mh[:, lanes], preferred_element_type=F32)
            target[part] = g.reshape(8, 16, 256)

    def rows_of(side, g):
        hi, lo = split(g)
        out = jnp.dot(ah[side], hi, preferred_element_type=F32)
        out = out + jnp.dot(al[side], hi, preferred_element_type=F32)
        return out + jnp.dot(ah[side], lo, preferred_element_type=F32)

    def to_rows(source, dst, ss, rs):
        c1, c2 = (slot + 5) // 8, (slot + 8) // 8
        for q in (2, 6, 3, 7, 1, 5, 0, 4):
            v = place ^ q
            for n, cc in ((0, c1), (1, c2)):
                extra = None if n == 0 else c1 != c2
                w = slot - 8 * cc + 8
                send(source(v), dst.at[w], ss.at[n, v], rs.at[w], cc % CUTS, 8 * h + v, extra)

    def cells_for(period):
        mark("w_ce")
        for k in (1, 2):
            sure_await(rce.at[period - 1, k - 1], s_ce.at[period - 1, k - 1], r_ce.at[period - 1, k - 1])
        mark("hot")
        cell_f[period] = jnp.where(shifts[period] == 1, rce[period - 1, 0], rce[period - 1, 1])
        build_onehot(period)

    mark("w_xel")
    for k in (1, 2):
        for v in range(8):
            await_from(rxel.at[k - 1, v], s_xel.at[k - 1, v], r_xel.at[k - 1, v],
                       ((slot + k) % SLOTS) // 8, 8 * h + v)
    loads[6].wait()
    mark("first")
    one = shifts[0] == 1
    for v in range(8):
        state[4 * v:4 * v + 4, :] = jnp.where(one, rxel[0, v, 0], rxel[1, v, 0])
        state[32 + 4 * v:36 + 4 * v, :] = jnp.where(one, rxel[0, v, 1], rxel[1, v, 1])
        cell_f[0, 4 * v:4 * v + 4, :] = jnp.where(one, rxel[0, v, 2], rxel[1, v, 2])
    state[64:72, :] = jnp.zeros((8, 128), F32)
    build_onehot(0)
    moved = shifts[0]
    mark("w_a2a")
    for v in range(8):
        await_from(arr.at[:, v], s_a2a.at[v], r_a2a.at[v], z * 2 + group, 8 * h + v)
    fld[...] = jnp.where(((slot + moved) & 255) < shifts[0], 0.0, arr[...])
    for period in range(4):
        mark("samp")
        sample()
        if period > 0:
            mark("w_st")
            for k in (1, 2):
                sure_await(rst.at[period - 1, k - 1], s_st.at[period - 1, k - 1], r_st.at[period - 1, k - 1])
            state[...] = jnp.where(shifts[period] == 1, rst[period - 1, 0], rst[period - 1, 1])
        mark("kick")
        phase, energy, total = kick(period)
        if period < 3:
            sst[period, 0:32, :] = phase
            sst[period, 32:64, :] = energy
            sst[period, 64:72, :] = total
            relay(sst.at[period], rst, s_st, r_st, period)
        else:
            state[0:32, :] = phase
            state[32:64, :] = energy
            psum[...] = total
            sure_send(psum, psum_in, s_ps, r_ps, partner, b)
        mark("dep")
        deposit()

        mark("col")
        sweep_cols(gown.at[period])
        for part in range(2):
            sure_send(gown.at[period, part], goth.at[period, part],
                      s_ex.at[period, part], r_ex.at[period, part], partner, b)
        mark("rowown")
        acc = rows_of(0, gown[period].reshape(256, 256))
        if period < 3:
            cells_for(period + 1)
        else:
            mark("elsend")
            sure_await(psum_in, s_ps, r_ps)
            total = psum[...] + psum_in[...]
            for v in range(8):
                efin[v, 0:4, :] = state[4 * v:4 * v + 4, :]
                efin[v, 4:8, :] = state[32 + 4 * v:36 + 4 * v, :]
                efin[v, 8:16, :] = total
            to_rows(lambda v: efin.at[v], rel, s_el, r_el)
        mark("w_ex")
        for part in range(2):
            sure_await(goth.at[period, part], s_ex.at[period, part], r_ex.at[period, part])
        mark("rowoth")
        acc = (acc + rows_of(1, goth[period].reshape(256, 256))).reshape(2, 8, 16, 256)
        if period < 3:
            moved = moved + shifts[period + 1]
            fld[...] = jnp.where(((slot + moved) & 255) < shifts[period + 1], 0.0, acc)

    mark("fsend")
    fin[...] = acc
    to_rows(lambda v: fin.at[:, v], rfld, s_fld, r_fld)

    mark("w_small")
    for w in range(11):
        j = (8 * c - 8 + w + SLOTS) % SLOTS
        pz, pb = chip_of(j)
        await_from(rel.at[w], s_el.at[0, 0], r_el.at[w], pz * 2 + half, pb)
    mark("smallout")
    base = jnp.clip(8 - moved, 0, 3)
    lane = lax.broadcasted_iota(jnp.int32, (8, 8), 1)
    sums = jnp.zeros((8, 8), F32)
    for u in range(8):
        tile = rel[base + u]
        for i in range(4):
            lanes = slice(128 * i, 128 * i + 128)
            out_ph[u:u + 1, lanes] = tile[i:i + 1]
            out_en[u:u + 1, lanes] = tile[4 + i:5 + i]
        sums = jnp.where(lane == u, jnp.sum(tile[8:16], axis=1, keepdims=True), sums)
    out_sums[...] = sums * ELEC ** (-0.5)
    stores = [(out_ph, phase_out), (out_en, energy_out), (out_sums, sums_out), (out_fld, field_out)]
    stores = [pltpu.make_async_copy(src, dst, lsem.at[7 + n]) for n, (src, dst) in enumerate(stores)]
    for copy in stores[:3]:
        copy.start()
    mark("w_fld")
    for w in range(11):
        j = (8 * c - 8 + w + SLOTS) % SLOTS
        pz, pb = chip_of(j)
        await_from(rfld.at[w], s_fld.at[0, 0], r_fld.at[w], pz * 2 + half, pb)
    mark("fout")
    for u in range(8):
        out_fld[:, u] = rfld[base + u]
    stores[3].start()

    mark("drain")
    for there, src, dst, ss, rs in sends:
        copy = remote(src, dst, ss, rs, c, b)
        if there is None:
            copy.wait_send()
        else:
            @pl.when(there)
            def _():
                copy.wait_send()
    for copy in stores:
        copy.wait()
    mark(None)


def hand_over(field, phase, energy, sums, field_out, phase_out, energy_out, bunching_out,
              a, p, e, q, out, sem):
    ins = [(field, a), (phase, p), (energy, e), (sums, q)]
    outs = [(a, field_out), (p, phase_out), (e, energy_out), (out, bunching_out)]
    ins = [pltpu.make_async_copy(src, dst, sem.at[n]) for n, (src, dst) in enumerate(ins)]
    outs = [pltpu.make_async_copy(src, dst, sem.at[4 + n]) for n, (src, dst) in enumerate(outs)]
    for copy in ins:
        copy.start()
    for n in (3, 1, 2, 0):
        ins[n].wait()
        if n == 3:
            for period in range(4):
                out[period] = q[2 * period:2 * period + 2]
        outs[n].start()
    for copy in outs:
        copy.wait()


def shards(field, row_prop, col_prop, phase, energy, cells, shifts):
    V = pltpu.VMEM
    D = pltpu.SemaphoreType.DMA
    blocks = (2, 8, 16, 256)
    square = (2, 256, 256)
    scratch = [
        V(blocks, F32), V(square, F32), V(square, F32),
        V((8, 512), F32), V((8, 512), F32), V((8, 512), jnp.int32),
        V((512, 512), BF16), V((512, 512), BF16), V(square, BF16), V(square, BF16),
        V((32, 128), jnp.int32), V((32, 128), F32), V((8, 128, 512), BF16),
        V(blocks, F32), V(blocks, F32), V((4, *blocks), F32), V((4, *blocks), F32),
        V((2, 32, 128), F32), V((4, 32, 128), F32), V((72, 128), F32), V((4, 32, 128), F32),
        pltpu.SMEM((4,), jnp.int32), V((8, 8), F32), V((8, 512), F32), V((8, 512), F32), V(blocks, F32),
        V((8, 3, 4, 128), F32), V((2, 8, 3, 4, 128), F32), V((3, 72, 128), F32),
        V((3, 2, 72, 128), F32), V((3, 2, 32, 128), F32), V((8, 128), F32), V((8, 128), F32),
        V((8, 16, 128), F32), V(blocks, F32), V((11, 2, 16, 256), F32), V((11, 16, 128), F32),
        D((11,)), D((8,)), D((8,)), D((2, 8)), D((2, 8)), D((4, 2)), D((4, 2)),
        D((3, 2)), D((3, 2)), D((3, 2)), D((3, 2)), D, D,
        D((2, 8)), D((11,)), D((2, 8)), D((11,)),
    ]
    hbm = pl.BlockSpec(memory_space=pl.ANY)
    results = (jax.ShapeDtypeStruct(blocks, F32), jax.ShapeDtypeStruct((8, 512), F32),
               jax.ShapeDtypeStruct((8, 512), F32))
    out = pl.pallas_call(
        kernel,
        out_shape=(*results, jax.ShapeDtypeStruct((8, 8), F32)),
        in_specs=[hbm] * 7,
        out_specs=[hbm] * 4,
        scratch_shapes=scratch,
        compiler_params=pltpu.CompilerParams(
            collective_id=0, has_side_effects=True, vmem_limit_bytes=VMEM_LIMIT),
    )(shifts, field, row_prop, col_prop, phase, energy, cells)
    return pl.pallas_call(
        hand_over,
        out_shape=(*results, jax.ShapeDtypeStruct((4, 2, 8), F32)),
        in_specs=[hbm] * 4,
        out_specs=[hbm] * 4,
        scratch_shapes=[V(blocks, F32), V((8, 512), F32), V((8, 512), F32), V((8, 8), F32),
                        V((4, 2, 8), F32), D((8,))],
        compiler_params=pltpu.CompilerParams(vmem_limit_bytes=VMEM_LIMIT),
    )(*out)


def solution(mesh):
    return jax.shard_map(
        shards,
        mesh=mesh,
        in_specs=(
            P(None, "cuts", "row", None),
            P(),
            P(),
            P("cuts", "row"),
            P("cuts", "row"),
            P("cuts", "row"),
            P(),
        ),
        out_specs=(
            P(None, "cuts", "row", None),
            P("cuts", "row"),
            P("cuts", "row"),
            P(None, None, "cuts"),
        ),
        check_vma=False,
    )
```

```python
import jax
import jax.numpy as jnp
from jax import lax
from jax.experimental import pallas as pl
from jax.experimental.pallas import tpu as pltpu
from jax.sharding import PartitionSpec as P

F32 = jnp.float32
BF16 = jnp.bfloat16
MESH = pl.DeviceIdType.MESH
ELEC = 8192
CUTS = 32
SLOTS = 256
VMEM_LIMIT = 67_000_000
kick_rate = 0.5
source_gain = 0.5


def split(x):
    high = x.astype(BF16)
    return high, (x - high.astype(F32)).astype(BF16)


PATH = (0, 1, 5, 6, 10, 11, 15, 12, 8, 4, 7, 3, 2, 14, 13, 9)


def lookup(table, i):
    low = sum(n << (3 * (q % 8)) for q, n in enumerate(t % 8 for t in table[:8]))
    high = sum(n << (3 * (q % 8)) for q, n in enumerate(t % 8 for t in table[8:]))
    tops = sum((t // 8) << q for q, t in enumerate(table))
    word = jnp.where(i < 8, low, high)
    return ((word >> (3 * (i % 8))) & 7) + 8 * ((tops >> i) & 1)


def chip_of(j):
    z, at = j // 16, lookup(PATH, j % 16)
    return z, (at % 4 + z) % 4 + 4 * ((at // 4 + 2 * z) % 4)


def slot_of(z, b):
    at = (b % 4 + 3 * z) % 4 + 4 * ((b // 4 + 2 * z) % 4)
    return z * 16 + lookup(tuple(PATH.index(q) for q in range(16)), at)


def kernel(shifts_in, field_in, row_in, col_in, phase_in, energy_in, cells_in,
           field_out, phase_out, energy_out, sums_out,
           own, rowp, colp, ph_in, en_in, ce_in, mh, ml, ah, al,
           key_i, col_f, onehot, fld, arr, gown, goth, samp, emit, state, cell_f,
           shifts, out_sums, out_ph, out_en, out_fld, xel, rxel, sst, rst, rce, psum, psum_in, efin, fin, rfld, rel,
           lsem, s_a2a, r_a2a, s_xel, r_xel, s_ex, r_ex, s_st, r_st, s_ce, r_ce,
           s_ps, r_ps, s_fld, r_fld, s_el, r_el, go_first, go_relay):
    c = lax.axis_index("cuts")
    b = lax.axis_index("row")
    z = c // 2
    h = c % 2
    half = b // 8
    place = b % 8
    slot = slot_of(z, b)
    group = (slot // 8) % 2
    base_cut = slot // 8
    partner = c + 1 - 2 * h
    sends = []
    scope = []

    def mark(name):
        if scope:
            scope.pop().__exit__(None, None, None)
        if name:
            scope.append(jax.named_scope(name))
            scope[0].__enter__()

    def remote(src, dst, ss, rs, dc, db):
        return pltpu.make_async_remote_copy(
            src_ref=src, dst_ref=dst, send_sem=ss, recv_sem=rs,
            device_id=(dc, db), device_id_type=MESH)

    def send(src, dst, ss, rs, dc, db, extra=None):
        here = (dc == c) & (db == b)
        there = jnp.logical_not(here)
        if extra is not None:
            here = here & extra
            there = there & extra

        @pl.when(there)
        def _():
            remote(src, dst, ss, rs, dc, db).start()

        @pl.when(here)
        def _():
            dst[...] = src[...]

        sends.append((there, src, dst, ss, rs))

    def sure_send(src, dst, ss, rs, dc, db):
        remote(src, dst, ss, rs, dc, db).start()
        sends.append((None, src, dst, ss, rs))

    def await_from(dst, ss, rs, dc, db):
        @pl.when(jnp.logical_not((dc == c) & (db == b)))
        def _():
            remote(dst, dst, ss, rs, dc, db).wait_recv()

    def sure_await(dst, ss, rs):
        remote(dst, dst, ss, rs, c, b).wait_recv()

    mark("start")
    barrier = pltpu.get_barrier_semaphore()
    below = (base_cut + 1) % CUTS
    itself = (half == h) & ((base_cut == c) | ((below == c) & (slot % 8 >= 6)))
    def greet(dc, extra=None):
        for v in range(8):
            ok = jnp.logical_not((dc == c) & (8 * h + v == b))

            @pl.when(ok if extra is None else ok & extra)
            def _():
                pl.semaphore_signal(barrier, inc=1, device_id=(dc, 8 * h + v), device_id_type=MESH)

    greet(base_cut)
    greet(below, (slot % 8 >= 6) & (slot < SLOTS - 2))
    for k in (1, 2):
        pz, pb = chip_of((slot + k) % SLOTS)

        @pl.when(slot + k < SLOTS)
        def _():
            pl.semaphore_signal(barrier, inc=1, device_id=(pz * 2 + h, pb), device_id_type=MESH)

    for k in (1, 2):
        pz, pb = chip_of(SLOTS - k)

        @pl.when(c == 0)
        def _():
            pl.semaphore_signal(barrier, inc=1, device_id=(pz * 2 + half, pb), device_id_type=MESH)

        for first in range(k):
            qz, qb = chip_of(SLOTS + first - k)

            @pl.when(slot == first)
            def _():
                pl.semaphore_signal(barrier, inc=1, device_id=(qz * 2 + h, qb), device_id_type=MESH)

    pl.semaphore_signal(barrier, inc=1, device_id=(partner, b), device_id_type=MESH)
    pl.semaphore_signal(barrier, inc=1, device_id=((c + CUTS - 1) % CUTS, b), device_id_type=MESH)

    loads = [(phase_in, ph_in), (energy_in, en_in), (cells_in, ce_in), (field_in, own),
             (col_in, colp), (row_in, rowp), (shifts_in, shifts)]
    loads = [pltpu.make_async_copy(src, dst, lsem.at[n]) for n, (src, dst) in enumerate(loads)]
    for copy in loads:
        copy.start()

    mark("unpack")
    for n in (0, 1, 2):
        loads[n].wait()
    for u in range(8):
        for i in range(4):
            lanes = slice(128 * i, 128 * i + 128)
            xel[u, 0, i:i + 1, :] = ph_in[u:u + 1, lanes]
            xel[u, 1, i:i + 1, :] = en_in[u:u + 1, lanes]
            xel[u, 2, i:i + 1, :] = ce_in[u:u + 1, lanes].astype(F32)

    mark("w_barrier")
    loads[3].wait()
    closing = jnp.where(slot == SLOTS - 1, 10, 0) + jnp.where(slot == SLOTS - 2, 9, 0)
    opening = jnp.where(slot == 0, 2, 0) + jnp.where(slot == 1, 1, 0) + jnp.where(c == 0, 2, 0)
    pl.semaphore_wait(barrier, 14 - jnp.where(itself, 1, 0) + closing - opening)

    @pl.when(slot >= SLOTS - 2)
    def _():
        for v in range(8):
            pl.semaphore_signal(go_first, inc=1, device_id=(0, 8 * h + v), device_id_type=MESH)
        qz, qb = chip_of(0)
        pl.semaphore_signal(go_relay, inc=1, device_id=(qz * 2 + h, qb), device_id_type=MESH)

    @pl.when(slot == SLOTS - 1)
    def _():
        qz, qb = chip_of(1)
        pl.semaphore_signal(go_relay, inc=1, device_id=(qz * 2 + h, qb), device_id_type=MESH)


    mark("send0")
    for i in range(8):
        u = (place + i) % 8
        for k in (1, 2):
            pz, pb = chip_of((8 * c + u - k + SLOTS) % SLOTS)
            send(xel.at[u], rxel.at[k - 1, place], s_xel.at[k - 1, u], r_xel.at[k - 1, place], pz * 2 + half, pb,
                 jnp.logical_not((c == 0) & (u < k)))
    for i in range(8):
        u = (place + i) % 8
        _, db = chip_of(8 * c + u)
        send(own.at[:, u], arr.at[:, place], s_a2a.at[u], r_a2a.at[place], z * 2 + half, db)

    mark("prep")
    loads[4].wait()
    loads[5].wait()
    for part in range(2):
        hi, lo = split(jnp.transpose(colp[part]))
        places = ((0, 0, 1), (1, 1, 1)) if part == 0 else ((1, 0, -1), (0, 1, 1))
        for kk, nn, sign in places:
            at = (slice(256 * kk, 256 * kk + 256), slice(256 * nn, 256 * nn + 256))
            mh[at] = hi if sign > 0 else -hi
            ml[at] = lo if sign > 0 else -lo
    rows = pl.ds(pl.multiple_of(h * 128, 128), 128)
    for side in range(2):
        cols = pl.ds(pl.multiple_of((h + side - 2 * h * side) * 128, 128), 128)
        rr = split(rowp[0, rows, cols])
        ri = split(rowp[1, rows, cols])
        for n, ref in ((0, ah), (1, al)):
            ref[side, 0:128, 0:128] = rr[n]
            ref[side, 0:128, 128:256] = -ri[n]
            ref[side, 128:256, 0:128] = ri[n]
            ref[side, 128:256, 128:256] = rr[n]

    def build_onehot(period):
        if period < 3:
            relay(cell_f.at[period], rce, s_ce, r_ce, period, "inner" if period == 0 else None)
        cell = cell_f[period].astype(jnp.int32)
        key_i[...] = ((cell >> 8) & 15) + ((cell >> 7) & 1) * 16
        col_f[...] = (cell & 127).astype(F32)
        iota = lax.broadcasted_iota(jnp.int32, (128, 128), 0).astype(F32).astype(BF16)
        for u in range(8):
            for i in range(4):
                at = 4 * u + i
                col = jnp.broadcast_to(col_f[at:at + 1, :], (128, 128)).astype(BF16)
                onehot[u, :, 128 * i:128 * i + 128] = jnp.where(iota == col, 1.0, 0.0).astype(BF16)

    def relay(src, dst, ss, rs, period, when=None):
        for k in (1, 2):
            pz, pb = chip_of((slot - k + SLOTS) % SLOTS)
            if when is not None:
                send(src, dst.at[period, k - 1], ss.at[period, k - 1], rs.at[period, k - 1], pz * 2 + h, pb,
                     (slot < k) if when == "closing" else (slot >= k))
                continue
            sure_send(src, dst.at[period, k - 1], ss.at[period, k - 1], rs.at[period, k - 1], pz * 2 + h, pb)

    def sample():
        iota = lax.broadcasted_iota(jnp.int32, (32, 128), 0)
        for u in range(8):
            fu = jnp.concatenate([fld[p, u, :, 128 * q:128 * q + 128] for p in range(2) for q in range(2)], axis=0)
            hi, lo = split(fu)
            got = jnp.dot(jnp.concatenate([hi, lo], axis=0), onehot[u], preferred_element_type=F32)
            got = got[0:64] + got[64:128]
            for i in range(4):
                at = 4 * u + i
                lanes = slice(128 * i, 128 * i + 128)
                mask = iota == key_i[at:at + 1, :]
                for part in range(2):
                    picked = jnp.where(mask, got[32 * part:32 * part + 32, lanes], 0.0)
                    samp[part, at:at + 1, :] = jnp.sum(picked, axis=0, keepdims=True)

    def deposit():
        iota = lax.broadcasted_iota(jnp.int32, (32, 128), 0)
        for u in range(8):
            pieces = []
            for i in range(4):
                at = 4 * u + i
                mask = iota == key_i[at:at + 1, :]
                pieces.append(jnp.concatenate(
                    [jnp.where(mask, emit[n, at:at + 1, :], 0.0).astype(BF16) for n in range(4)], axis=0))
            weights = jnp.concatenate(pieces, axis=1)
            add = lax.dot_general(weights, onehot[u], (((1,), (1,)), ((), ())), preferred_element_type=F32)
            add = add[0:64] + add[64:128]
            for p in range(2):
                for q in range(2):
                    lanes = slice(128 * q, 128 * q + 128)
                    rows = slice(32 * p + 16 * q, 32 * p + 16 * q + 16)
                    fld[p, u, :, lanes] = fld[p, u, :, lanes] + add[rows]

    def kick(period):
        cosine, sine = jnp.cos(state[0:32, :]), jnp.sin(state[0:32, :])
        energy = state[32:64, :] - kick_rate * (samp[0] * cosine - samp[1] * sine)
        phase = state[0:32, :] + energy
        cosine, sine = jnp.cos(phase), jnp.sin(phase)
        line = lax.broadcasted_iota(jnp.int32, (8, 128), 0)
        total = state[64:72, :]
        total = total + jnp.where(line == 2 * period, jnp.sum(cosine, axis=0, keepdims=True), 0.0)
        total = total + jnp.where(line == 2 * period + 1, -jnp.sum(sine, axis=0, keepdims=True), 0.0)
        for n, value in ((0, source_gain * cosine), (1, -source_gain * sine)):
            high = value.astype(BF16).astype(F32)
            emit[n] = high
            emit[2 + n] = value - high
        return phase, energy, total

    def sweep_cols(target):
        f = fld[...].reshape(2, 128, 256)
        parts = [split(f[0]), split(f[1])]
        lh = jnp.concatenate([parts[0][0], parts[1][0]], axis=1)
        ll = jnp.concatenate([parts[0][1], parts[1][1]], axis=1)
        for part in range(2):
            lanes = slice(256 * part, 256 * part + 256)
            g = jnp.dot(lh, mh[:, lanes], preferred_element_type=F32)
            g = g + jnp.dot(lh, ml[:, lanes], preferred_element_type=F32)
            g = g + jnp.dot(ll, mh[:, lanes], preferred_element_type=F32)
            target[part] = g.reshape(8, 16, 256)

    def rows_of(side, g):
        hi, lo = split(g)
        out = jnp.dot(ah[side], hi, preferred_element_type=F32)
        out = out + jnp.dot(al[side], hi, preferred_element_type=F32)
        return out + jnp.dot(ah[side], lo, preferred_element_type=F32)

    def to_rows(source, dst, ss, rs):
        c1, c2 = (slot + 5) // 8, (slot + 8) // 8
        for q in (2, 6, 3, 7, 1, 5, 0, 4):
            v = place ^ q
            for n, cc in ((0, c1), (1, c2)):
                extra = None if n == 0 else c1 != c2
                w = slot - 8 * cc + 8
                send(source(v), dst.at[w], ss.at[n, v], rs.at[w], cc % CUTS, 8 * h + v, extra)

    def cells_for(period):
        mark("w_ce")
        for k in (1, 2):
            sure_await(rce.at[period - 1, k - 1], s_ce.at[period - 1, k - 1], r_ce.at[period - 1, k - 1])
        mark("hot")
        cell_f[period] = jnp.where(shifts[period] == 1, rce[period - 1, 0], rce[period - 1, 1])
        build_onehot(period)

    mark("w_xel")
    for k in (1, 2):
        for v in range(8):
            await_from(rxel.at[k - 1, v], s_xel.at[k - 1, v], r_xel.at[k - 1, v],
                       ((slot + k) % SLOTS) // 8, 8 * h + v)
    loads[6].wait()
    mark("first")
    one = shifts[0] == 1
    for v in range(8):
        state[4 * v:4 * v + 4, :] = jnp.where(one, rxel[0, v, 0], rxel[1, v, 0])
        state[32 + 4 * v:36 + 4 * v, :] = jnp.where(one, rxel[0, v, 1], rxel[1, v, 1])
        cell_f[0, 4 * v:4 * v + 4, :] = jnp.where(one, rxel[0, v, 2], rxel[1, v, 2])
    state[64:72, :] = jnp.zeros((8, 128), F32)
    build_onehot(0)
    mark("wrap")

    @pl.when(c == 0)
    def _():
        pl.semaphore_wait(go_first, 2)

    for u, k in ((0, 1), (0, 2), (1, 2)):
        pz, pb = chip_of(SLOTS + u - k)
        send(xel.at[u], rxel.at[k - 1, place], s_xel.at[k - 1, u], r_xel.at[k - 1, place], pz * 2 + half, pb, c == 0)

    moved = shifts[0]
    mark("w_a2a")
    for v in range(8):
        await_from(arr.at[:, v], s_a2a.at[v], r_a2a.at[v], z * 2 + group, 8 * h + v)
    fld[...] = jnp.where(((slot + moved) & 255) < shifts[0], 0.0, arr[...])
    for period in range(4):
        mark("samp")
        sample()
        if period > 0:
            mark("w_st")
            for k in (1, 2):
                sure_await(rst.at[period - 1, k - 1], s_st.at[period - 1, k - 1], r_st.at[period - 1, k - 1])
            state[...] = jnp.where(shifts[period] == 1, rst[period - 1, 0], rst[period - 1, 1])
        mark("kick")
        phase, energy, total = kick(period)
        if period == 0:
            for first in range(2):
                @pl.when(slot == first)
                def _():
                    pl.semaphore_wait(go_relay, 2 - first)

            relay(cell_f.at[0], rce, s_ce, r_ce, 0, "closing")
        if period < 3:
            sst[period, 0:32, :] = phase
            sst[period, 32:64, :] = energy
            sst[period, 64:72, :] = total
            relay(sst.at[period], rst, s_st, r_st, period)
        else:
            state[0:32, :] = phase
            state[32:64, :] = energy
            psum[...] = total
            sure_send(psum, psum_in, s_ps, r_ps, partner, b)
        mark("dep")
        deposit()

        mark("col")
        sweep_cols(gown.at[period])
        for part in range(2):
            sure_send(gown.at[period, part], goth.at[period, part],
                      s_ex.at[period, part], r_ex.at[period, part], partner, b)
        mark("rowown")
        acc = rows_of(0, gown[period].reshape(256, 256))
        if period < 3:
            cells_for(period + 1)
        else:
            mark("elsend")
            sure_await(psum_in, s_ps, r_ps)
            total = psum[...] + psum_in[...]
            for v in range(8):
                efin[v, 0:4, :] = state[4 * v:4 * v + 4, :]
                efin[v, 4:8, :] = state[32 + 4 * v:36 + 4 * v, :]
                efin[v, 8:16, :] = total
            to_rows(lambda v: efin.at[v], rel, s_el, r_el)
        mark("w_ex")
        for part in range(2):
            sure_await(goth.at[period, part], s_ex.at[period, part], r_ex.at[period, part])
        mark("rowoth")
        acc = (acc + rows_of(1, goth[period].reshape(256, 256))).reshape(2, 8, 16, 256)
        if period < 3:
            moved = moved + shifts[period + 1]
            fld[...] = jnp.where(((slot + moved) & 255) < shifts[period + 1], 0.0, acc)

    mark("fsend")
    fin[...] = acc
    to_rows(lambda v: fin.at[:, v], rfld, s_fld, r_fld)

    mark("w_small")
    for w in range(11):
        j = (8 * c - 8 + w + SLOTS) % SLOTS
        pz, pb = chip_of(j)
        await_from(rel.at[w], s_el.at[0, 0], r_el.at[w], pz * 2 + half, pb)
    mark("smallout")
    base = jnp.clip(8 - moved, 0, 3)
    lane = lax.broadcasted_iota(jnp.int32, (8, 8), 1)
    sums = jnp.zeros((8, 8), F32)
    for u in range(8):
        tile = rel[base + u]
        for i in range(4):
            lanes = slice(128 * i, 128 * i + 128)
            out_ph[u:u + 1, lanes] = tile[i:i + 1]
            out_en[u:u + 1, lanes] = tile[4 + i:5 + i]
        sums = jnp.where(lane == u, jnp.sum(tile[8:16], axis=1, keepdims=True), sums)
    out_sums[...] = sums * ELEC ** (-0.5)
    stores = [(out_ph, phase_out), (out_en, energy_out), (out_sums, sums_out), (out_fld, field_out)]
    stores = [pltpu.make_async_copy(src, dst, lsem.at[7 + n]) for n, (src, dst) in enumerate(stores)]
    for copy in stores[:3]:
        copy.start()
    mark("w_fld")
    for w in range(11):
        j = (8 * c - 8 + w + SLOTS) % SLOTS
        pz, pb = chip_of(j)
        await_from(rfld.at[w], s_fld.at[0, 0], r_fld.at[w], pz * 2 + half, pb)
    mark("fout")
    for u in range(8):
        out_fld[:, u] = rfld[base + u]
    stores[3].start()

    mark("drain")
    for there, src, dst, ss, rs in sends:
        copy = remote(src, dst, ss, rs, c, b)
        if there is None:
            copy.wait_send()
        else:
            @pl.when(there)
            def _():
                copy.wait_send()
    for copy in stores:
        copy.wait()
    mark(None)


def hand_over(field, phase, energy, sums, field_out, phase_out, energy_out, bunching_out,
              a, p, e, q, out, sem):
    ins = [(field, a), (phase, p), (energy, e), (sums, q)]
    outs = [(a, field_out), (p, phase_out), (e, energy_out), (out, bunching_out)]
    ins = [pltpu.make_async_copy(src, dst, sem.at[n]) for n, (src, dst) in enumerate(ins)]
    outs = [pltpu.make_async_copy(src, dst, sem.at[4 + n]) for n, (src, dst) in enumerate(outs)]
    for copy in ins:
        copy.start()
    for n in (3, 1, 2, 0):
        ins[n].wait()
        if n == 3:
            for period in range(4):
                out[period] = q[2 * period:2 * period + 2]
        outs[n].start()
    for copy in outs:
        copy.wait()


def shards(field, row_prop, col_prop, phase, energy, cells, shifts):
    V = pltpu.VMEM
    D = pltpu.SemaphoreType.DMA
    blocks = (2, 8, 16, 256)
    square = (2, 256, 256)
    scratch = [
        V(blocks, F32), V(square, F32), V(square, F32),
        V((8, 512), F32), V((8, 512), F32), V((8, 512), jnp.int32),
        V((512, 512), BF16), V((512, 512), BF16), V(square, BF16), V(square, BF16),
        V((32, 128), jnp.int32), V((32, 128), F32), V((8, 128, 512), BF16),
        V(blocks, F32), V(blocks, F32), V((4, *blocks), F32), V((4, *blocks), F32),
        V((2, 32, 128), F32), V((4, 32, 128), F32), V((72, 128), F32), V((4, 32, 128), F32),
        pltpu.SMEM((4,), jnp.int32), V((8, 8), F32), V((8, 512), F32), V((8, 512), F32), V(blocks, F32),
        V((8, 3, 4, 128), F32), V((2, 8, 3, 4, 128), F32), V((3, 72, 128), F32),
        V((3, 2, 72, 128), F32), V((3, 2, 32, 128), F32), V((8, 128), F32), V((8, 128), F32),
        V((8, 16, 128), F32), V(blocks, F32), V((11, 2, 16, 256), F32), V((11, 16, 128), F32),
        D((11,)), D((8,)), D((8,)), D((2, 8)), D((2, 8)), D((4, 2)), D((4, 2)),
        D((3, 2)), D((3, 2)), D((3, 2)), D((3, 2)), D, D,
        D((2, 8)), D((11,)), D((2, 8)), D((11,)),
        pltpu.SemaphoreType.REGULAR, pltpu.SemaphoreType.REGULAR,
    ]
    hbm = pl.BlockSpec(memory_space=pl.ANY)
    results = (jax.ShapeDtypeStruct(blocks, F32), jax.ShapeDtypeStruct((8, 512), F32),
               jax.ShapeDtypeStruct((8, 512), F32))
    out = pl.pallas_call(
        kernel,
        out_shape=(*results, jax.ShapeDtypeStruct((8, 8), F32)),
        in_specs=[hbm] * 7,
        out_specs=[hbm] * 4,
        scratch_shapes=scratch,
        compiler_params=pltpu.CompilerParams(
            collective_id=0, has_side_effects=True, vmem_limit_bytes=VMEM_LIMIT),
    )(shifts, field, row_prop, col_prop, phase, energy, cells)
    return pl.pallas_call(
        hand_over,
        out_shape=(*results, jax.ShapeDtypeStruct((4, 2, 8), F32)),
        in_specs=[hbm] * 4,
        out_specs=[hbm] * 4,
        scratch_shapes=[V(blocks, F32), V((8, 512), F32), V((8, 512), F32), V((8, 8), F32),
                        V((4, 2, 8), F32), D((8,))],
        compiler_params=pltpu.CompilerParams(vmem_limit_bytes=VMEM_LIMIT),
    )(*out)


def solution(mesh):
    return jax.shard_map(
        shards,
        mesh=mesh,
        in_specs=(
            P(None, "cuts", "row", None),
            P(),
            P(),
            P("cuts", "row"),
            P("cuts", "row"),
            P("cuts", "row"),
            P(),
        ),
        out_specs=(
            P(None, "cuts", "row", None),
            P("cuts", "row"),
            P("cuts", "row"),
            P(None, None, "cuts"),
        ),
        check_vma=False,
    )
```

```python
import jax
import jax.numpy as jnp
from jax import lax
from jax.experimental import pallas as pl
from jax.experimental.pallas import tpu as pltpu
from jax.sharding import PartitionSpec as P

F32 = jnp.float32
BF16 = jnp.bfloat16
MESH = pl.DeviceIdType.MESH
ELEC = 8192
CUTS = 32
SLOTS = 256
VMEM_LIMIT = 67_000_000
kick_rate = 0.5
source_gain = 0.5


def split(x):
    high = x.astype(BF16)
    return high, (x - high.astype(F32)).astype(BF16)


PATH = (0, 1, 5, 6, 10, 11, 15, 12, 8, 4, 7, 3, 2, 14, 13, 9)


def lookup(table, i):
    low = sum(n << (3 * (q % 8)) for q, n in enumerate(t % 8 for t in table[:8]))
    high = sum(n << (3 * (q % 8)) for q, n in enumerate(t % 8 for t in table[8:]))
    tops = sum((t // 8) << q for q, t in enumerate(table))
    word = jnp.where(i < 8, low, high)
    return ((word >> (3 * (i % 8))) & 7) + 8 * ((tops >> i) & 1)


def chip_of(j):
    z, at = j // 16, lookup(PATH, j % 16)
    return z, (at % 4 + z) % 4 + 4 * ((at // 4 + 2 * z) % 4)


def slot_of(z, b):
    at = (b % 4 + 3 * z) % 4 + 4 * ((b // 4 + 2 * z) % 4)
    return z * 16 + lookup(tuple(PATH.index(q) for q in range(16)), at)


def kernel(shifts_in, field_in, row_in, col_in, phase_in, energy_in, cells_in,
           field_out, phase_out, energy_out, sums_out,
           own, rowp, colp, ph_in, en_in, ce_in, mh, ml, ah, al,
           key_i, col_f, onehot, fld, arr, gown, goth, samp, emit, state, cell_f,
           shifts, out_sums, out_ph, out_en, out_fld, xel, rxel, sst, rst, rce, psum, psum_in, efin, fin, rfld, rel,
           lsem, s_a2a, r_a2a, s_xel, r_xel, s_ex, r_ex, s_st, r_st, s_ce, r_ce,
           s_ps, r_ps, s_fld, r_fld, s_el, r_el):
    c = lax.axis_index("cuts")
    b = lax.axis_index("row")
    z = c // 2
    h = c % 2
    half = b // 8
    place = b % 8
    slot = slot_of(z, b)
    group = (slot // 8) % 2
    base_cut = slot // 8
    partner = c + 1 - 2 * h
    sends = []
    scope = []

    def mark(name):
        if scope:
            scope.pop().__exit__(None, None, None)
        if name:
            scope.append(jax.named_scope(name))
            scope[0].__enter__()

    def remote(src, dst, ss, rs, dc, db):
        return pltpu.make_async_remote_copy(
            src_ref=src, dst_ref=dst, send_sem=ss, recv_sem=rs,
            device_id=(dc, db), device_id_type=MESH)

    def send(src, dst, ss, rs, dc, db, extra=None):
        here = (dc == c) & (db == b)
        there = jnp.logical_not(here)
        if extra is not None:
            here = here & extra
            there = there & extra

        @pl.when(there)
        def _():
            remote(src, dst, ss, rs, dc, db).start()

        @pl.when(here)
        def _():
            dst[...] = src[...]

        sends.append((there, src, dst, ss, rs))

    def sure_send(src, dst, ss, rs, dc, db):
        remote(src, dst, ss, rs, dc, db).start()
        sends.append((None, src, dst, ss, rs))

    def await_from(dst, ss, rs, dc, db):
        @pl.when(jnp.logical_not((dc == c) & (db == b)))
        def _():
            remote(dst, dst, ss, rs, dc, db).wait_recv()

    def sure_await(dst, ss, rs):
        remote(dst, dst, ss, rs, c, b).wait_recv()

    mark("start")
    barrier = pltpu.get_barrier_semaphore()
    below = (base_cut + 1) % CUTS
    itself = (half == h) & ((base_cut == c) | ((below == c) & (slot % 8 >= 6)))
    def greet(dc, extra=None):
        for v in range(8):
            ok = jnp.logical_not((dc == c) & (8 * h + v == b))

            @pl.when(ok if extra is None else ok & extra)
            def _():
                pl.semaphore_signal(barrier, inc=1, device_id=(dc, 8 * h + v), device_id_type=MESH)

    greet(base_cut)
    greet(below, slot % 8 >= 6)
    for k in (1, 2):
        pz, pb = chip_of((slot + k) % SLOTS)
        pl.semaphore_signal(barrier, inc=1, device_id=(pz * 2 + h, pb), device_id_type=MESH)
    pl.semaphore_signal(barrier, inc=1, device_id=(partner, b), device_id_type=MESH)

    loads = [(phase_in, ph_in), (energy_in, en_in), (cells_in, ce_in), (field_in, own),
             (col_in, colp), (row_in, rowp), (shifts_in, shifts)]
    loads = [pltpu.make_async_copy(src, dst, lsem.at[n]) for n, (src, dst) in enumerate(loads)]
    for copy in loads:
        copy.start()

    mark("unpack")
    for n in (0, 1, 2):
        loads[n].wait()
    for u in range(8):
        for i in range(4):
            lanes = slice(128 * i, 128 * i + 128)
            xel[u, 0, i:i + 1, :] = ph_in[u:u + 1, lanes]
            xel[u, 1, i:i + 1, :] = en_in[u:u + 1, lanes]
            xel[u, 2, i:i + 1, :] = ce_in[u:u + 1, lanes].astype(F32)

    mark("w_barrier")
    loads[3].wait()
    pl.semaphore_wait(barrier, 13 - jnp.where(itself, 1, 0))

    mark("send0")
    for i in range(8):
        u = (place + i) % 8
        for k in (1, 2):
            pz, pb = chip_of((8 * c + u - k + SLOTS) % SLOTS)
            send(xel.at[u], rxel.at[k - 1, place], s_xel.at[k - 1, u], r_xel.at[k - 1, place], pz * 2 + half, pb)
    for i in range(8):
        u = (place + i) % 8
        _, db = chip_of(8 * c + u)
        send(own.at[:, u], arr.at[:, place], s_a2a.at[u], r_a2a.at[place], z * 2 + half, db)

    mark("prep")
    loads[4].wait()
    loads[5].wait()
    for part in range(2):
        hi, lo = split(jnp.transpose(colp[part]))
        places = ((0, 0, 1), (1, 1, 1)) if part == 0 else ((1, 0, -1), (0, 1, 1))
        for kk, nn, sign in places:
            at = (slice(256 * kk, 256 * kk + 256), slice(256 * nn, 256 * nn + 256))
            mh[at] = hi if sign > 0 else -hi
            ml[at] = lo if sign > 0 else -lo
    rows = pl.ds(pl.multiple_of(h * 128, 128), 128)
    for side in range(2):
        cols = pl.ds(pl.multiple_of((h + side - 2 * h * side) * 128, 128), 128)
        rr = split(rowp[0, rows, cols])
        ri = split(rowp[1, rows, cols])
        for n, ref in ((0, ah), (1, al)):
            ref[side, 0:128, 0:128] = rr[n]
            ref[side, 0:128, 128:256] = -ri[n]
            ref[side, 128:256, 0:128] = ri[n]
            ref[side, 128:256, 128:256] = rr[n]

    def build_onehot(period):
        if period < 3:
            relay(cell_f.at[period], rce, s_ce, r_ce, period)
        cell = cell_f[period].astype(jnp.int32)
        key_i[...] = ((cell >> 8) & 15) + ((cell >> 7) & 1) * 16
        col_f[...] = (cell & 127).astype(F32)
        iota = lax.broadcasted_iota(jnp.int32, (128, 128), 0).astype(F32).astype(BF16)
        for u in range(8):
            for i in range(4):
                at = 4 * u + i
                col = jnp.broadcast_to(col_f[at:at + 1, :], (128, 128)).astype(BF16)
                onehot[u, :, 128 * i:128 * i + 128] = jnp.where(iota == col, 1.0, 0.0).astype(BF16)

    def relay(src, dst, ss, rs, period):
        for k in (1, 2):
            pz, pb = chip_of((slot - k + SLOTS) % SLOTS)
            sure_send(src, dst.at[period, k - 1], ss.at[period, k - 1], rs.at[period, k - 1], pz * 2 + h, pb)

    def sample():
        iota = lax.broadcasted_iota(jnp.int32, (32, 128), 0)
        for u in range(8):
            fu = jnp.concatenate([fld[p, u, :, 128 * q:128 * q + 128] for p in range(2) for q in range(2)], axis=0)
            hi, lo = split(fu)
            got = jnp.dot(jnp.concatenate([hi, lo], axis=0), onehot[u], preferred_element_type=F32)
            got = got[0:64] + got[64:128]
            for i in range(4):
                at = 4 * u + i
                lanes = slice(128 * i, 128 * i + 128)
                mask = iota == key_i[at:at + 1, :]
                for part in range(2):
                    picked = jnp.where(mask, got[32 * part:32 * part + 32, lanes], 0.0)
                    samp[part, at:at + 1, :] = jnp.sum(picked, axis=0, keepdims=True)

    def deposit():
        iota = lax.broadcasted_iota(jnp.int32, (32, 128), 0)
        for u in range(8):
            pieces = []
            for i in range(4):
                at = 4 * u + i
                mask = iota == key_i[at:at + 1, :]
                pieces.append(jnp.concatenate(
                    [jnp.where(mask, emit[n, at:at + 1, :], 0.0).astype(BF16) for n in range(4)], axis=0))
            weights = jnp.concatenate(pieces, axis=1)
            add = lax.dot_general(weights, onehot[u], (((1,), (1,)), ((), ())), preferred_element_type=F32)
            add = add[0:64] + add[64:128]
            for p in range(2):
                for q in range(2):
                    lanes = slice(128 * q, 128 * q + 128)
                    rows = slice(32 * p + 16 * q, 32 * p + 16 * q + 16)
                    fld[p, u, :, lanes] = fld[p, u, :, lanes] + add[rows]

    def kick(period):
        cosine, sine = jnp.cos(state[0:32, :]), jnp.sin(state[0:32, :])
        energy = state[32:64, :] - kick_rate * (samp[0] * cosine - samp[1] * sine)
        phase = state[0:32, :] + energy
        cosine, sine = jnp.cos(phase), jnp.sin(phase)
        line = lax.broadcasted_iota(jnp.int32, (8, 128), 0)
        total = state[64:72, :]
        total = total + jnp.where(line == 2 * period, jnp.sum(cosine, axis=0, keepdims=True), 0.0)
        total = total + jnp.where(line == 2 * period + 1, -jnp.sum(sine, axis=0, keepdims=True), 0.0)
        for n, value in ((0, source_gain * cosine), (1, -source_gain * sine)):
            high = value.astype(BF16).astype(F32)
            emit[n] = high
            emit[2 + n] = value - high
        return phase, energy, total

    def sweep_cols(target):
        f = fld[...].reshape(2, 128, 256)
        parts = [split(f[0]), split(f[1])]
        lh = jnp.concatenate([parts[0][0], parts[1][0]], axis=1)
        ll = jnp.concatenate([parts[0][1], parts[1][1]], axis=1)
        for part in range(2):
            lanes = slice(256 * part, 256 * part + 256)
            g = jnp.dot(lh, mh[:, lanes], preferred_element_type=F32)
            g = g + jnp.dot(lh, ml[:, lanes], preferred_element_type=F32)
            g = g + jnp.dot(ll, mh[:, lanes], preferred_element_type=F32)
            target[part] = g.reshape(8, 16, 256)

    def rows_of(side, g):
        hi, lo = split(g)
        out = jnp.dot(ah[side], hi, preferred_element_type=F32)
        out = out + jnp.dot(al[side], hi, preferred_element_type=F32)
        return out + jnp.dot(ah[side], lo, preferred_element_type=F32)

    def to_rows(source, dst, ss, rs):
        c1, c2 = (slot + 5) // 8, (slot + 8) // 8
        for q in (2, 6, 3, 7, 1, 5, 0, 4):
            v = place ^ q
            for n, cc in ((0, c1), (1, c2)):
                extra = None if n == 0 else c1 != c2
                w = slot - 8 * cc + 8
                send(source(v), dst.at[w], ss.at[n, v], rs.at[w], cc % CUTS, 8 * h + v, extra)

    def cells_for(period):
        mark("w_ce")
        for k in (1, 2):
            sure_await(rce.at[period - 1, k - 1], s_ce.at[period - 1, k - 1], r_ce.at[period - 1, k - 1])
        mark("hot")
        cell_f[period] = jnp.where(shifts[period] == 1, rce[period - 1, 0], rce[period - 1, 1])
        build_onehot(period)

    mark("w_xel")
    for k in (1, 2):
        for v in range(8):
            await_from(rxel.at[k - 1, v], s_xel.at[k - 1, v], r_xel.at[k - 1, v],
                       ((slot + k) % SLOTS) // 8, 8 * h + v)
    loads[6].wait()
    mark("first")
    one = shifts[0] == 1
    for v in range(8):
        state[4 * v:4 * v + 4, :] = jnp.where(one, rxel[0, v, 0], rxel[1, v, 0])
        state[32 + 4 * v:36 + 4 * v, :] = jnp.where(one, rxel[0, v, 1], rxel[1, v, 1])
        cell_f[0, 4 * v:4 * v + 4, :] = jnp.where(one, rxel[0, v, 2], rxel[1, v, 2])
    state[64:72, :] = jnp.zeros((8, 128), F32)
    build_onehot(0)
    moved = shifts[0]
    mark("w_a2a")
    for v in range(8):
        await_from(arr.at[:, v], s_a2a.at[v], r_a2a.at[v], z * 2 + group, 8 * h + v)
    fld[...] = jnp.where(((slot + moved) & 255) < shifts[0], 0.0, arr[...])
    for period in range(4):
        mark("samp")
        sample()
        if period > 0:
            mark("w_st")
            for k in (1, 2):
                sure_await(rst.at[period - 1, k - 1], s_st.at[period - 1, k - 1], r_st.at[period - 1, k - 1])
            state[...] = jnp.where(shifts[period] == 1, rst[period - 1, 0], rst[period - 1, 1])
        mark("kick")
        phase, energy, total = kick(period)
        if period < 3:
            sst[period, 0:32, :] = phase
            sst[period, 32:64, :] = energy
            sst[period, 64:72, :] = total
            relay(sst.at[period], rst, s_st, r_st, period)
        else:
            state[0:32, :] = phase
            state[32:64, :] = energy
            psum[...] = total
            sure_send(psum, psum_in, s_ps, r_ps, partner, b)
        mark("dep")
        deposit()

        mark("col")
        sweep_cols(gown.at[period])
        for part in range(2):
            sure_send(gown.at[period, part], goth.at[period, part],
                      s_ex.at[period, part], r_ex.at[period, part], partner, b)
        mark("rowown")
        acc = rows_of(0, gown[period].reshape(256, 256))
        if period < 3:
            cells_for(period + 1)
        else:
            mark("elsend")
            sure_await(psum_in, s_ps, r_ps)
            diagonal = (lax.broadcasted_iota(jnp.int32, (8, 128), 0)
                        == lax.broadcasted_iota(jnp.int32, (8, 128), 1))
            total = jnp.sum(psum[...] + psum_in[...], axis=1, keepdims=True)
            total = jnp.sum(jnp.where(diagonal, total, 0.0), axis=0, keepdims=True)
            for v in range(8):
                efin[v, 0:4, :] = state[4 * v:4 * v + 4, :]
                efin[v, 4:8, :] = state[32 + 4 * v:36 + 4 * v, :]
                efin[v, 8:9, :] = total
            to_rows(lambda v: efin.at[v], rel, s_el, r_el)
        mark("w_ex")
        for part in range(2):
            sure_await(goth.at[period, part], s_ex.at[period, part], r_ex.at[period, part])
        mark("rowoth")
        acc = (acc + rows_of(1, goth[period].reshape(256, 256))).reshape(2, 8, 16, 256)
        if period < 3:
            moved = moved + shifts[period + 1]
            fld[...] = jnp.where(((slot + moved) & 255) < shifts[period + 1], 0.0, acc)

    mark("fsend")
    fin[...] = acc
    to_rows(lambda v: fin.at[:, v], rfld, s_fld, r_fld)

    mark("w_small")
    for w in range(11):
        j = (8 * c - 8 + w + SLOTS) % SLOTS
        pz, pb = chip_of(j)
        await_from(rel.at[w], s_el.at[0, 0], r_el.at[w], pz * 2 + half, pb)
    mark("smallout")
    base = jnp.clip(8 - moved, 0, 3)
    lane = lax.broadcasted_iota(jnp.int32, (8, 8), 1)
    sums = jnp.zeros((8, 8), F32)
    for u in range(8):
        tile = rel[base + u]
        for i in range(4):
            lanes = slice(128 * i, 128 * i + 128)
            out_ph[u:u + 1, lanes] = tile[i:i + 1]
            out_en[u:u + 1, lanes] = tile[4 + i:5 + i]
        total = jnp.sum(jnp.where(diagonal, tile[8:9], 0.0), axis=1, keepdims=True)
        sums = jnp.where(lane == u, total, sums)
    out_sums[...] = sums * ELEC ** (-0.5)
    stores = [(out_ph, phase_out), (out_en, energy_out), (out_sums, sums_out), (out_fld, field_out)]
    stores = [pltpu.make_async_copy(src, dst, lsem.at[7 + n]) for n, (src, dst) in enumerate(stores)]
    for copy in stores[:3]:
        copy.start()
    mark("w_fld")
    for w in range(11):
        j = (8 * c - 8 + w + SLOTS) % SLOTS
        pz, pb = chip_of(j)
        await_from(rfld.at[w], s_fld.at[0, 0], r_fld.at[w], pz * 2 + half, pb)
    mark("fout")
    for u in range(8):
        out_fld[:, u] = rfld[base + u]
    stores[3].start()

    mark("drain")
    for there, src, dst, ss, rs in sends:
        copy = remote(src, dst, ss, rs, c, b)
        if there is None:
            copy.wait_send()
        else:
            @pl.when(there)
            def _():
                copy.wait_send()
    for copy in stores:
        copy.wait()
    mark(None)


def hand_over(field, phase, energy, sums, field_out, phase_out, energy_out, bunching_out,
              a, p, e, q, out, sem):
    ins = [(field, a), (phase, p), (energy, e), (sums, q)]
    outs = [(a, field_out), (p, phase_out), (e, energy_out), (out, bunching_out)]
    ins = [pltpu.make_async_copy(src, dst, sem.at[n]) for n, (src, dst) in enumerate(ins)]
    outs = [pltpu.make_async_copy(src, dst, sem.at[4 + n]) for n, (src, dst) in enumerate(outs)]
    for copy in ins:
        copy.start()
    for n in (3, 1, 2, 0):
        ins[n].wait()
        if n == 3:
            for period in range(4):
                out[period] = q[2 * period:2 * period + 2]
        outs[n].start()
    for copy in outs:
        copy.wait()


def shards(field, row_prop, col_prop, phase, energy, cells, shifts):
    V = pltpu.VMEM
    D = pltpu.SemaphoreType.DMA
    blocks = (2, 8, 16, 256)
    square = (2, 256, 256)
    scratch = [
        V(blocks, F32), V(square, F32), V(square, F32),
        V((8, 512), F32), V((8, 512), F32), V((8, 512), jnp.int32),
        V((512, 512), BF16), V((512, 512), BF16), V(square, BF16), V(square, BF16),
        V((32, 128), jnp.int32), V((32, 128), F32), V((8, 128, 512), BF16),
        V(blocks, F32), V(blocks, F32), V((4, *blocks), F32), V((4, *blocks), F32),
        V((2, 32, 128), F32), V((4, 32, 128), F32), V((72, 128), F32), V((4, 32, 128), F32),
        pltpu.SMEM((4,), jnp.int32), V((8, 8), F32), V((8, 512), F32), V((8, 512), F32), V(blocks, F32),
        V((8, 3, 4, 128), F32), V((2, 8, 3, 4, 128), F32), V((3, 72, 128), F32),
        V((3, 2, 72, 128), F32), V((3, 2, 32, 128), F32), V((8, 128), F32), V((8, 128), F32),
        V((8, 9, 128), F32), V(blocks, F32), V((11, 2, 16, 256), F32), V((11, 9, 128), F32),
        D((11,)), D((8,)), D((8,)), D((2, 8)), D((2, 8)), D((4, 2)), D((4, 2)),
        D((3, 2)), D((3, 2)), D((3, 2)), D((3, 2)), D, D,
        D((2, 8)), D((11,)), D((2, 8)), D((11,)),
    ]
    hbm = pl.BlockSpec(memory_space=pl.ANY)
    results = (jax.ShapeDtypeStruct(blocks, F32), jax.ShapeDtypeStruct((8, 512), F32),
               jax.ShapeDtypeStruct((8, 512), F32))
    out = pl.pallas_call(
        kernel,
        out_shape=(*results, jax.ShapeDtypeStruct((8, 8), F32)),
        in_specs=[hbm] * 7,
        out_specs=[hbm] * 4,
        scratch_shapes=scratch,
        compiler_params=pltpu.CompilerParams(
            collective_id=0, has_side_effects=True, vmem_limit_bytes=VMEM_LIMIT),
    )(shifts, field, row_prop, col_prop, phase, energy, cells)
    return pl.pallas_call(
        hand_over,
        out_shape=(*results, jax.ShapeDtypeStruct((4, 2, 8), F32)),
        in_specs=[hbm] * 4,
        out_specs=[hbm] * 4,
        scratch_shapes=[V(blocks, F32), V((8, 512), F32), V((8, 512), F32), V((8, 8), F32),
                        V((4, 2, 8), F32), D((8,))],
        compiler_params=pltpu.CompilerParams(vmem_limit_bytes=VMEM_LIMIT),
    )(*out)


def solution(mesh):
    return jax.shard_map(
        shards,
        mesh=mesh,
        in_specs=(
            P(None, "cuts", "row", None),
            P(),
            P(),
            P("cuts", "row"),
            P("cuts", "row"),
            P("cuts", "row"),
            P(),
        ),
        out_specs=(
            P(None, "cuts", "row", None),
            P("cuts", "row"),
            P("cuts", "row"),
            P(None, None, "cuts"),
        ),
        check_vma=False,
    )
```

```python
import jax
import jax.numpy as jnp
from jax import lax
from jax.experimental import pallas as pl
from jax.experimental.pallas import tpu as pltpu
from jax.sharding import PartitionSpec as P

F32 = jnp.float32
BF16 = jnp.bfloat16
MESH = pl.DeviceIdType.MESH
ELEC = 8192
CUTS = 32
SLOTS = 256
VMEM_LIMIT = 67_000_000
kick_rate = 0.5
source_gain = 0.5


def split(x):
    high = x.astype(BF16)
    return high, (x - high.astype(F32)).astype(BF16)


PATH = (0, 1, 5, 6, 10, 11, 15, 12, 8, 4, 7, 3, 2, 14, 13, 9)


def lookup(table, i):
    low = sum(n << (3 * (q % 8)) for q, n in enumerate(t % 8 for t in table[:8]))
    high = sum(n << (3 * (q % 8)) for q, n in enumerate(t % 8 for t in table[8:]))
    tops = sum((t // 8) << q for q, t in enumerate(table))
    word = jnp.where(i < 8, low, high)
    return ((word >> (3 * (i % 8))) & 7) + 8 * ((tops >> i) & 1)


def chip_of(j):
    z, at = j // 16, lookup(PATH, j % 16)
    return z, (at % 4 + z) % 4 + 4 * ((at // 4 + 2 * z) % 4)


def slot_of(z, b):
    at = (b % 4 + 3 * z) % 4 + 4 * ((b // 4 + 2 * z) % 4)
    return z * 16 + lookup(tuple(PATH.index(q) for q in range(16)), at)


def kernel(shifts_in, field_in, row_in, col_in, phase_in, energy_in, cells_in,
           field_out, phase_out, energy_out, sums_out,
           own, rowp, colp, ph_in, en_in, ce_in, mh, ml, ah, al,
           key_i, col_i, onehot, fld, arr, gown, goth, samp, emit, state, cell_f,
           shifts, out_sums, out_ph, out_en, out_fld, xel, rxel, sst, rst, rce, psum, psum_in, efin, fin, rfld, rel,
           lsem, s_a2a, r_a2a, s_xel, r_xel, s_ex, r_ex, s_st, r_st, s_ce, r_ce,
           s_ps, r_ps, s_fld, r_fld, s_el, r_el):
    c = lax.axis_index("cuts")
    b = lax.axis_index("row")
    z = c // 2
    h = c % 2
    half = b // 8
    place = b % 8
    slot = slot_of(z, b)
    group = (slot // 8) % 2
    base_cut = slot // 8
    partner = c + 1 - 2 * h
    sends = []
    scope = []

    def mark(name):
        if scope:
            scope.pop().__exit__(None, None, None)
        if name:
            scope.append(jax.named_scope(name))
            scope[0].__enter__()

    def remote(src, dst, ss, rs, dc, db):
        return pltpu.make_async_remote_copy(
            src_ref=src, dst_ref=dst, send_sem=ss, recv_sem=rs,
            device_id=(dc, db), device_id_type=MESH)

    def send(src, dst, ss, rs, dc, db, extra=None):
        here = (dc == c) & (db == b)
        there = jnp.logical_not(here)
        if extra is not None:
            here = here & extra
            there = there & extra

        @pl.when(there)
        def _():
            remote(src, dst, ss, rs, dc, db).start()

        @pl.when(here)
        def _():
            dst[...] = src[...]

        sends.append((there, src, dst, ss, rs))

    def sure_send(src, dst, ss, rs, dc, db):
        remote(src, dst, ss, rs, dc, db).start()
        sends.append((None, src, dst, ss, rs))

    def await_from(dst, ss, rs, dc, db):
        @pl.when(jnp.logical_not((dc == c) & (db == b)))
        def _():
            remote(dst, dst, ss, rs, dc, db).wait_recv()

    def sure_await(dst, ss, rs):
        remote(dst, dst, ss, rs, c, b).wait_recv()

    mark("start")
    barrier = pltpu.get_barrier_semaphore()
    below = (base_cut + 1) % CUTS
    itself = (half == h) & ((base_cut == c) | ((below == c) & (slot % 8 >= 6)))
    def greet(dc, extra=None):
        for v in range(8):
            ok = jnp.logical_not((dc == c) & (8 * h + v == b))

            @pl.when(ok if extra is None else ok & extra)
            def _():
                pl.semaphore_signal(barrier, inc=1, device_id=(dc, 8 * h + v), device_id_type=MESH)

    greet(base_cut)
    greet(below, slot % 8 >= 6)
    for k in (1, 2):
        pz, pb = chip_of((slot + k) % SLOTS)
        pl.semaphore_signal(barrier, inc=1, device_id=(pz * 2 + h, pb), device_id_type=MESH)
    pl.semaphore_signal(barrier, inc=1, device_id=(partner, b), device_id_type=MESH)

    loads = [(phase_in, ph_in), (energy_in, en_in), (cells_in, ce_in), (field_in, own),
             (col_in, colp), (row_in, rowp), (shifts_in, shifts)]
    loads = [pltpu.make_async_copy(src, dst, lsem.at[n]) for n, (src, dst) in enumerate(loads)]
    for copy in loads:
        copy.start()

    mark("unpack")
    for n in (0, 1, 2):
        loads[n].wait()
    for u in range(8):
        for i in range(4):
            lanes = slice(128 * i, 128 * i + 128)
            xel[u, 0, i:i + 1, :] = ph_in[u:u + 1, lanes]
            xel[u, 1, i:i + 1, :] = en_in[u:u + 1, lanes]
            xel[u, 2, i:i + 1, :] = ce_in[u:u + 1, lanes].astype(F32)

    mark("w_barrier")
    loads[3].wait()
    pl.semaphore_wait(barrier, 13 - jnp.where(itself, 1, 0))

    mark("send0")
    for i in range(8):
        u = (place + i) % 8
        for k in (1, 2):
            pz, pb = chip_of((8 * c + u - k + SLOTS) % SLOTS)
            send(xel.at[u], rxel.at[k - 1, place], s_xel.at[k - 1, u], r_xel.at[k - 1, place], pz * 2 + half, pb)
    for i in range(8):
        u = (place + i) % 8
        _, db = chip_of(8 * c + u)
        send(own.at[:, u], arr.at[:, place], s_a2a.at[u], r_a2a.at[place], z * 2 + half, db)

    mark("prep")
    loads[4].wait()
    loads[5].wait()
    for part in range(2):
        hi, lo = split(jnp.transpose(colp[part]))
        places = ((0, 0, 1), (1, 1, 1)) if part == 0 else ((1, 0, -1), (0, 1, 1))
        for kk, nn, sign in places:
            at = (slice(256 * kk, 256 * kk + 256), slice(256 * nn, 256 * nn + 256))
            mh[at] = hi if sign > 0 else -hi
            ml[at] = lo if sign > 0 else -lo
    rows = pl.ds(pl.multiple_of(h * 128, 128), 128)
    for side in range(2):
        cols = pl.ds(pl.multiple_of((h + side - 2 * h * side) * 128, 128), 128)
        rr = split(rowp[0, rows, cols])
        ri = split(rowp[1, rows, cols])
        for n, ref in ((0, ah), (1, al)):
            ref[side, 0:128, 0:128] = rr[n]
            ref[side, 0:128, 128:256] = -ri[n]
            ref[side, 128:256, 0:128] = ri[n]
            ref[side, 128:256, 128:256] = rr[n]

    def build_onehot(period):
        if period < 3:
            relay(cell_f.at[period], rce, s_ce, r_ce, period)
        cell = cell_f[period].astype(jnp.int32)
        key_i[...] = ((cell >> 8) & 15) + ((cell >> 7) & 1) * 16
        col_i[...] = cell & 127
        iota = lax.broadcasted_iota(jnp.int32, (128, 128), 0)
        for u in range(8):
            for i in range(4):
                at = 4 * u + i
                hot = jnp.where(iota == col_i[at:at + 1, :], 1.0, 0.0)
                onehot[u, :, 128 * i:128 * i + 128] = hot.astype(BF16)

    def relay(src, dst, ss, rs, period):
        for k in (1, 2):
            pz, pb = chip_of((slot - k + SLOTS) % SLOTS)
            sure_send(src, dst.at[period, k - 1], ss.at[period, k - 1], rs.at[period, k - 1], pz * 2 + h, pb)

    def sample():
        iota = lax.broadcasted_iota(jnp.int32, (32, 128), 0)
        for u in range(8):
            fu = jnp.concatenate([fld[p, u, :, 128 * q:128 * q + 128] for p in range(2) for q in range(2)], axis=0)
            hi, lo = split(fu)
            got = jnp.dot(jnp.concatenate([hi, lo], axis=0), onehot[u], preferred_element_type=F32)
            got = got[0:64] + got[64:128]
            for i in range(4):
                at = 4 * u + i
                lanes = slice(128 * i, 128 * i + 128)
                mask = iota == key_i[at:at + 1, :]
                for part in range(2):
                    picked = jnp.where(mask, got[32 * part:32 * part + 32, lanes], 0.0)
                    samp[part, at:at + 1, :] = jnp.sum(picked, axis=0, keepdims=True)

    def deposit():
        iota = lax.broadcasted_iota(jnp.int32, (32, 128), 0)
        for u in range(8):
            pieces = []
            for i in range(4):
                at = 4 * u + i
                mask = iota == key_i[at:at + 1, :]
                pieces.append(jnp.concatenate(
                    [jnp.where(mask, emit[n, at:at + 1, :], 0.0).astype(BF16) for n in range(4)], axis=0))
            weights = jnp.concatenate(pieces, axis=1)
            add = lax.dot_general(weights, onehot[u], (((1,), (1,)), ((), ())), preferred_element_type=F32)
            add = add[0:64] + add[64:128]
            for p in range(2):
                for q in range(2):
                    lanes = slice(128 * q, 128 * q + 128)
                    rows = slice(32 * p + 16 * q, 32 * p + 16 * q + 16)
                    fld[p, u, :, lanes] = fld[p, u, :, lanes] + add[rows]

    def kick(period):
        cosine, sine = jnp.cos(state[0:32, :]), jnp.sin(state[0:32, :])
        energy = state[32:64, :] - kick_rate * (samp[0] * cosine - samp[1] * sine)
        phase = state[0:32, :] + energy
        cosine, sine = jnp.cos(phase), jnp.sin(phase)
        line = lax.broadcasted_iota(jnp.int32, (8, 128), 0)
        total = state[64:72, :]
        total = total + jnp.where(line == 2 * period, jnp.sum(cosine, axis=0, keepdims=True), 0.0)
        total = total + jnp.where(line == 2 * period + 1, -jnp.sum(sine, axis=0, keepdims=True), 0.0)
        for n, value in ((0, source_gain * cosine), (1, -source_gain * sine)):
            high = value.astype(BF16).astype(F32)
            emit[n] = high
            emit[2 + n] = value - high
        return phase, energy, total

    def sweep_cols(target):
        f = fld[...].reshape(2, 128, 256)
        parts = [split(f[0]), split(f[1])]
        lh = jnp.concatenate([parts[0][0], parts[1][0]], axis=1)
        ll = jnp.concatenate([parts[0][1], parts[1][1]], axis=1)
        for part in range(2):
            lanes = slice(256 * part, 256 * part + 256)
            g = jnp.dot(lh, mh[:, lanes], preferred_element_type=F32)
            g = g + jnp.dot(lh, ml[:, lanes], preferred_element_type=F32)
            g = g + jnp.dot(ll, mh[:, lanes], preferred_element_type=F32)
            target[part] = g.reshape(8, 16, 256)

    def rows_of(side, g):
        hi, lo = split(g)
        out = jnp.dot(ah[side], hi, preferred_element_type=F32)
        out = out + jnp.dot(al[side], hi, preferred_element_type=F32)
        return out + jnp.dot(ah[side], lo, preferred_element_type=F32)

    def to_rows(source, dst, ss, rs):
        c1, c2 = (slot + 5) // 8, (slot + 8) // 8
        for q in (2, 6, 3, 7, 1, 5, 0, 4):
            v = place ^ q
            for n, cc in ((0, c1), (1, c2)):
                extra = None if n == 0 else c1 != c2
                w = slot - 8 * cc + 8
                send(source(v), dst.at[w], ss.at[n, v], rs.at[w], cc % CUTS, 8 * h + v, extra)

    def cells_for(period):
        mark("w_ce")
        for k in (1, 2):
            sure_await(rce.at[period - 1, k - 1], s_ce.at[period - 1, k - 1], r_ce.at[period - 1, k - 1])
        mark("hot")
        cell_f[period] = jnp.where(shifts[period] == 1, rce[period - 1, 0], rce[period - 1, 1])
        build_onehot(period)

    mark("w_xel")
    for k in (1, 2):
        for v in range(8):
            await_from(rxel.at[k - 1, v], s_xel.at[k - 1, v], r_xel.at[k - 1, v],
                       ((slot + k) % SLOTS) // 8, 8 * h + v)
    loads[6].wait()
    mark("first")
    one = shifts[0] == 1
    for v in range(8):
        state[4 * v:4 * v + 4, :] = jnp.where(one, rxel[0, v, 0], rxel[1, v, 0])
        state[32 + 4 * v:36 + 4 * v, :] = jnp.where(one, rxel[0, v, 1], rxel[1, v, 1])
        cell_f[0, 4 * v:4 * v + 4, :] = jnp.where(one, rxel[0, v, 2], rxel[1, v, 2])
    state[64:72, :] = jnp.zeros((8, 128), F32)
    build_onehot(0)
    moved = shifts[0]
    mark("w_a2a")
    for v in range(8):
        await_from(arr.at[:, v], s_a2a.at[v], r_a2a.at[v], z * 2 + group, 8 * h + v)
    fld[...] = jnp.where(((slot + moved) & 255) < shifts[0], 0.0, arr[...])
    for period in range(4):
        mark("samp")
        sample()
        if period > 0:
            mark("w_st")
            for k in (1, 2):
                sure_await(rst.at[period - 1, k - 1], s_st.at[period - 1, k - 1], r_st.at[period - 1, k - 1])
            state[...] = jnp.where(shifts[period] == 1, rst[period - 1, 0], rst[period - 1, 1])
        mark("kick")
        phase, energy, total = kick(period)
        if period < 3:
            sst[period, 0:32, :] = phase
            sst[period, 32:64, :] = energy
            sst[period, 64:72, :] = total
            relay(sst.at[period], rst, s_st, r_st, period)
        else:
            state[0:32, :] = phase
            state[32:64, :] = energy
            psum[...] = total
            sure_send(psum, psum_in, s_ps, r_ps, partner, b)
        mark("dep")
        deposit()

        mark("col")
        sweep_cols(gown.at[period])
        for part in range(2):
            sure_send(gown.at[period, part], goth.at[period, part],
                      s_ex.at[period, part], r_ex.at[period, part], partner, b)
        mark("rowown")
        acc = rows_of(0, gown[period].reshape(256, 256))
        if period < 3:
            cells_for(period + 1)
        else:
            mark("elsend")
            sure_await(psum_in, s_ps, r_ps)
            diagonal = (lax.broadcasted_iota(jnp.int32, (8, 128), 0)
                        == lax.broadcasted_iota(jnp.int32, (8, 128), 1))
            total = jnp.sum(psum[...] + psum_in[...], axis=1, keepdims=True)
            total = jnp.sum(jnp.where(diagonal, total, 0.0), axis=0, keepdims=True)
            for v in range(8):
                efin[v, 0:4, :] = state[4 * v:4 * v + 4, :]
                efin[v, 4:8, :] = state[32 + 4 * v:36 + 4 * v, :]
                efin[v, 8:9, :] = total
            to_rows(lambda v: efin.at[v], rel, s_el, r_el)
        mark("w_ex")
        for part in range(2):
            sure_await(goth.at[period, part], s_ex.at[period, part], r_ex.at[period, part])
        mark("rowoth")
        acc = (acc + rows_of(1, goth[period].reshape(256, 256))).reshape(2, 8, 16, 256)
        if period < 3:
            moved = moved + shifts[period + 1]
            fld[...] = jnp.where(((slot + moved) & 255) < shifts[period + 1], 0.0, acc)

    mark("fsend")
    fin[...] = acc
    to_rows(lambda v: fin.at[:, v], rfld, s_fld, r_fld)

    mark("w_small")
    for w in range(11):
        j = (8 * c - 8 + w + SLOTS) % SLOTS
        pz, pb = chip_of(j)
        await_from(rel.at[w], s_el.at[0, 0], r_el.at[w], pz * 2 + half, pb)
    mark("smallout")
    base = jnp.clip(8 - moved, 0, 3)
    lane = lax.broadcasted_iota(jnp.int32, (8, 8), 1)
    sums = jnp.zeros((8, 8), F32)
    for u in range(8):
        tile = rel[base + u]
        for i in range(4):
            lanes = slice(128 * i, 128 * i + 128)
            out_ph[u:u + 1, lanes] = tile[i:i + 1]
            out_en[u:u + 1, lanes] = tile[4 + i:5 + i]
        total = jnp.sum(jnp.where(diagonal, tile[8:9], 0.0), axis=1, keepdims=True)
        sums = jnp.where(lane == u, total, sums)
    out_sums[...] = sums * ELEC ** (-0.5)
    stores = [(out_ph, phase_out), (out_en, energy_out), (out_sums, sums_out), (out_fld, field_out)]
    stores = [pltpu.make_async_copy(src, dst, lsem.at[7 + n]) for n, (src, dst) in enumerate(stores)]
    for copy in stores[:3]:
        copy.start()
    mark("w_fld")
    for w in range(11):
        j = (8 * c - 8 + w + SLOTS) % SLOTS
        pz, pb = chip_of(j)
        await_from(rfld.at[w], s_fld.at[0, 0], r_fld.at[w], pz * 2 + half, pb)
    mark("fout")
    for u in range(8):
        out_fld[:, u] = rfld[base + u]
    stores[3].start()

    mark("drain")
    for there, src, dst, ss, rs in sends:
        copy = remote(src, dst, ss, rs, c, b)
        if there is None:
            copy.wait_send()
        else:
            @pl.when(there)
            def _():
                copy.wait_send()
    for copy in stores:
        copy.wait()
    mark(None)


def hand_over(field, phase, energy, sums, field_out, phase_out, energy_out, bunching_out,
              a, p, e, q, out, sem):
    ins = [(field, a), (phase, p), (energy, e), (sums, q)]
    outs = [(a, field_out), (p, phase_out), (e, energy_out), (out, bunching_out)]
    ins = [pltpu.make_async_copy(src, dst, sem.at[n]) for n, (src, dst) in enumerate(ins)]
    outs = [pltpu.make_async_copy(src, dst, sem.at[4 + n]) for n, (src, dst) in enumerate(outs)]
    for copy in ins:
        copy.start()
    for n in (3, 1, 2, 0):
        ins[n].wait()
        if n == 3:
            for period in range(4):
                out[period] = q[2 * period:2 * period + 2]
        outs[n].start()
    for copy in outs:
        copy.wait()


def shards(field, row_prop, col_prop, phase, energy, cells, shifts):
    V = pltpu.VMEM
    D = pltpu.SemaphoreType.DMA
    blocks = (2, 8, 16, 256)
    square = (2, 256, 256)
    scratch = [
        V(blocks, F32), V(square, F32), V(square, F32),
        V((8, 512), F32), V((8, 512), F32), V((8, 512), jnp.int32),
        V((512, 512), BF16), V((512, 512), BF16), V(square, BF16), V(square, BF16),
        V((32, 128), jnp.int32), V((32, 128), jnp.int32), V((8, 128, 512), BF16),
        V(blocks, F32), V(blocks, F32), V((4, *blocks), F32), V((4, *blocks), F32),
        V((2, 32, 128), F32), V((4, 32, 128), F32), V((72, 128), F32), V((4, 32, 128), F32),
        pltpu.SMEM((4,), jnp.int32), V((8, 8), F32), V((8, 512), F32), V((8, 512), F32), V(blocks, F32),
        V((8, 3, 4, 128), F32), V((2, 8, 3, 4, 128), F32), V((3, 72, 128), F32),
        V((3, 2, 72, 128), F32), V((3, 2, 32, 128), F32), V((8, 128), F32), V((8, 128), F32),
        V((8, 9, 128), F32), V(blocks, F32), V((11, 2, 16, 256), F32), V((11, 9, 128), F32),
        D((11,)), D((8,)), D((8,)), D((2, 8)), D((2, 8)), D((4, 2)), D((4, 2)),
        D((3, 2)), D((3, 2)), D((3, 2)), D((3, 2)), D, D,
        D((2, 8)), D((11,)), D((2, 8)), D((11,)),
    ]
    hbm = pl.BlockSpec(memory_space=pl.ANY)
    results = (jax.ShapeDtypeStruct(blocks, F32), jax.ShapeDtypeStruct((8, 512), F32),
               jax.ShapeDtypeStruct((8, 512), F32))
    out = pl.pallas_call(
        kernel,
        out_shape=(*results, jax.ShapeDtypeStruct((8, 8), F32)),
        in_specs=[hbm] * 7,
        out_specs=[hbm] * 4,
        scratch_shapes=scratch,
        compiler_params=pltpu.CompilerParams(
            collective_id=0, has_side_effects=True, vmem_limit_bytes=VMEM_LIMIT),
    )(shifts, field, row_prop, col_prop, phase, energy, cells)
    return pl.pallas_call(
        hand_over,
        out_shape=(*results, jax.ShapeDtypeStruct((4, 2, 8), F32)),
        in_specs=[hbm] * 4,
        out_specs=[hbm] * 4,
        scratch_shapes=[V(blocks, F32), V((8, 512), F32), V((8, 512), F32), V((8, 8), F32),
                        V((4, 2, 8), F32), D((8,))],
        compiler_params=pltpu.CompilerParams(vmem_limit_bytes=VMEM_LIMIT),
    )(*out)


def solution(mesh):
    return jax.shard_map(
        shards,
        mesh=mesh,
        in_specs=(
            P(None, "cuts", "row", None),
            P(),
            P(),
            P("cuts", "row"),
            P("cuts", "row"),
            P("cuts", "row"),
            P(),
        ),
        out_specs=(
            P(None, "cuts", "row", None),
            P("cuts", "row"),
            P("cuts", "row"),
            P(None, None, "cuts"),
        ),
        check_vma=False,
    )
```

```python
import jax
import jax.numpy as jnp
from jax import lax
from jax.experimental import pallas as pl
from jax.experimental.pallas import tpu as pltpu
from jax.sharding import PartitionSpec as P

F32 = jnp.float32
BF16 = jnp.bfloat16
MESH = pl.DeviceIdType.MESH
ELEC = 8192
CUTS = 32
SLOTS = 256
VMEM_LIMIT = 67_000_000
kick_rate = 0.5
source_gain = 0.5


def split(x):
    high = x.astype(BF16)
    return high, (x - high.astype(F32)).astype(BF16)


PATH = (0, 1, 5, 6, 10, 11, 15, 12, 8, 4, 7, 3, 2, 14, 13, 9)


def lookup(table, i):
    low = sum(n << (3 * (q % 8)) for q, n in enumerate(t % 8 for t in table[:8]))
    high = sum(n << (3 * (q % 8)) for q, n in enumerate(t % 8 for t in table[8:]))
    tops = sum((t // 8) << q for q, t in enumerate(table))
    word = jnp.where(i < 8, low, high)
    return ((word >> (3 * (i % 8))) & 7) + 8 * ((tops >> i) & 1)


def chip_of(j):
    z, at = j // 16, lookup(PATH, j % 16)
    return z, (at % 4 + z) % 4 + 4 * ((at // 4 + 2 * z) % 4)


def slot_of(z, b):
    at = (b % 4 + 3 * z) % 4 + 4 * ((b // 4 + 2 * z) % 4)
    return z * 16 + lookup(tuple(PATH.index(q) for q in range(16)), at)


def kernel(shifts_in, field_in, row_in, col_in, phase_in, energy_in, cells_in,
           rfld, rel,
           own, rowp, colp, ph_in, en_in, ce_in, mh, ml, ah, al,
           key_i, col_i, onehot, fld, arr, gown, goth, samp, emit, state, cell_f,
           shifts, xel, rxel, sst, rst, rce, psum, psum_in, efin, fin,
           lsem, s_a2a, r_a2a, s_xel, r_xel, s_ex, r_ex, s_st, r_st, s_ce, r_ce,
           s_ps, r_ps, s_fld, r_fld, s_el, r_el):
    c = lax.axis_index("cuts")
    b = lax.axis_index("row")
    z = c // 2
    h = c % 2
    half = b // 8
    place = b % 8
    slot = slot_of(z, b)
    group = (slot // 8) % 2
    base_cut = slot // 8
    partner = c + 1 - 2 * h
    sends = []
    scope = []

    def mark(name):
        if scope:
            scope.pop().__exit__(None, None, None)
        if name:
            scope.append(jax.named_scope(name))
            scope[0].__enter__()

    def remote(src, dst, ss, rs, dc, db):
        return pltpu.make_async_remote_copy(
            src_ref=src, dst_ref=dst, send_sem=ss, recv_sem=rs,
            device_id=(dc, db), device_id_type=MESH)

    def send(src, dst, ss, rs, dc, db, extra=None, far=True):
        here = (dc == c) & (db == b)
        there = jnp.logical_not(here)
        if extra is not None:
            here = here & extra
            there = there & extra

        @pl.when(there)
        def _():
            remote(src, dst, ss, rs, dc, db).start()

        @pl.when(here)
        def _():
            if far:
                dst[...] = src[...]
            else:
                pltpu.make_async_copy(src, dst, rs).start()

        sends.append((there, src, dst, ss, rs))

    def sure_send(src, dst, ss, rs, dc, db):
        remote(src, dst, ss, rs, dc, db).start()
        sends.append((None, src, dst, ss, rs))

    def await_from(dst, ss, rs, dc, db):
        @pl.when(jnp.logical_not((dc == c) & (db == b)))
        def _():
            remote(dst, dst, ss, rs, dc, db).wait_recv()

    def sure_await(dst, ss, rs):
        remote(dst, dst, ss, rs, c, b).wait_recv()

    mark("start")
    barrier = pltpu.get_barrier_semaphore()
    below = (base_cut + 1) % CUTS
    itself = (half == h) & ((base_cut == c) | ((below == c) & (slot % 8 >= 6)))
    def greet(dc, extra=None):
        for v in range(8):
            ok = jnp.logical_not((dc == c) & (8 * h + v == b))

            @pl.when(ok if extra is None else ok & extra)
            def _():
                pl.semaphore_signal(barrier, inc=1, device_id=(dc, 8 * h + v), device_id_type=MESH)

    greet(base_cut)
    greet(below, slot % 8 >= 6)
    for k in (1, 2):
        pz, pb = chip_of((slot + k) % SLOTS)
        pl.semaphore_signal(barrier, inc=1, device_id=(pz * 2 + h, pb), device_id_type=MESH)
    pl.semaphore_signal(barrier, inc=1, device_id=(partner, b), device_id_type=MESH)

    loads = [(phase_in, ph_in), (energy_in, en_in), (cells_in, ce_in), (field_in, own),
             (col_in, colp), (row_in, rowp), (shifts_in, shifts)]
    loads = [pltpu.make_async_copy(src, dst, lsem.at[n]) for n, (src, dst) in enumerate(loads)]
    for copy in loads:
        copy.start()

    mark("unpack")
    for n in (0, 1, 2):
        loads[n].wait()
    for u in range(8):
        for i in range(4):
            lanes = slice(128 * i, 128 * i + 128)
            xel[u, 0, i:i + 1, :] = ph_in[u:u + 1, lanes]
            xel[u, 1, i:i + 1, :] = en_in[u:u + 1, lanes]
            xel[u, 2, i:i + 1, :] = ce_in[u:u + 1, lanes].astype(F32)

    mark("w_barrier")
    loads[3].wait()
    pl.semaphore_wait(barrier, 13 - jnp.where(itself, 1, 0))

    mark("send0")
    for i in range(8):
        u = (place + i) % 8
        for k in (1, 2):
            pz, pb = chip_of((8 * c + u - k + SLOTS) % SLOTS)
            send(xel.at[u], rxel.at[k - 1, place], s_xel.at[k - 1, u], r_xel.at[k - 1, place], pz * 2 + half, pb)
    for i in range(8):
        u = (place + i) % 8
        _, db = chip_of(8 * c + u)
        send(own.at[:, u], arr.at[:, place], s_a2a.at[u], r_a2a.at[place], z * 2 + half, db)

    mark("prep")
    loads[4].wait()
    loads[5].wait()
    for part in range(2):
        hi, lo = split(jnp.transpose(colp[part]))
        places = ((0, 0, 1), (1, 1, 1)) if part == 0 else ((1, 0, -1), (0, 1, 1))
        for kk, nn, sign in places:
            at = (slice(256 * kk, 256 * kk + 256), slice(256 * nn, 256 * nn + 256))
            mh[at] = hi if sign > 0 else -hi
            ml[at] = lo if sign > 0 else -lo
    rows = pl.ds(pl.multiple_of(h * 128, 128), 128)
    for side in range(2):
        cols = pl.ds(pl.multiple_of((h + side - 2 * h * side) * 128, 128), 128)
        rr = split(rowp[0, rows, cols])
        ri = split(rowp[1, rows, cols])
        for n, ref in ((0, ah), (1, al)):
            ref[side, 0:128, 0:128] = rr[n]
            ref[side, 0:128, 128:256] = -ri[n]
            ref[side, 128:256, 0:128] = ri[n]
            ref[side, 128:256, 128:256] = rr[n]

    def build_onehot(period):
        if period < 3:
            relay(cell_f.at[period], rce, s_ce, r_ce, period)
        cell = cell_f[period].astype(jnp.int32)
        key_i[...] = ((cell >> 8) & 15) + ((cell >> 7) & 1) * 16
        col_i[...] = cell & 127
        iota = lax.broadcasted_iota(jnp.int32, (128, 128), 0)
        for u in range(8):
            for i in range(4):
                at = 4 * u + i
                hot = jnp.where(iota == col_i[at:at + 1, :], 1.0, 0.0)
                onehot[u, :, 128 * i:128 * i + 128] = hot.astype(BF16)

    def relay(src, dst, ss, rs, period):
        for k in (1, 2):
            pz, pb = chip_of((slot - k + SLOTS) % SLOTS)
            sure_send(src, dst.at[period, k - 1], ss.at[period, k - 1], rs.at[period, k - 1], pz * 2 + h, pb)

    def sample():
        iota = lax.broadcasted_iota(jnp.int32, (32, 128), 0)
        for u in range(8):
            fu = jnp.concatenate([fld[p, u, :, 128 * q:128 * q + 128] for p in range(2) for q in range(2)], axis=0)
            hi, lo = split(fu)
            got = jnp.dot(jnp.concatenate([hi, lo], axis=0), onehot[u], preferred_element_type=F32)
            got = got[0:64] + got[64:128]
            for i in range(4):
                at = 4 * u + i
                lanes = slice(128 * i, 128 * i + 128)
                mask = iota == key_i[at:at + 1, :]
                for part in range(2):
                    picked = jnp.where(mask, got[32 * part:32 * part + 32, lanes], 0.0)
                    samp[part, at:at + 1, :] = jnp.sum(picked, axis=0, keepdims=True)

    def deposit():
        iota = lax.broadcasted_iota(jnp.int32, (32, 128), 0)
        for u in range(8):
            pieces = []
            for i in range(4):
                at = 4 * u + i
                mask = iota == key_i[at:at + 1, :]
                pieces.append(jnp.concatenate(
                    [jnp.where(mask, emit[n, at:at + 1, :], 0.0).astype(BF16) for n in range(4)], axis=0))
            weights = jnp.concatenate(pieces, axis=1)
            add = lax.dot_general(weights, onehot[u], (((1,), (1,)), ((), ())), preferred_element_type=F32)
            add = add[0:64] + add[64:128]
            for p in range(2):
                for q in range(2):
                    lanes = slice(128 * q, 128 * q + 128)
                    rows = slice(32 * p + 16 * q, 32 * p + 16 * q + 16)
                    fld[p, u, :, lanes] = fld[p, u, :, lanes] + add[rows]

    def kick(period):
        cosine, sine = jnp.cos(state[0:32, :]), jnp.sin(state[0:32, :])
        energy = state[32:64, :] - kick_rate * (samp[0] * cosine - samp[1] * sine)
        phase = state[0:32, :] + energy
        cosine, sine = jnp.cos(phase), jnp.sin(phase)
        line = lax.broadcasted_iota(jnp.int32, (8, 128), 0)
        total = state[64:72, :]
        total = total + jnp.where(line == 2 * period, jnp.sum(cosine, axis=0, keepdims=True), 0.0)
        total = total + jnp.where(line == 2 * period + 1, -jnp.sum(sine, axis=0, keepdims=True), 0.0)
        for n, value in ((0, source_gain * cosine), (1, -source_gain * sine)):
            high = value.astype(BF16).astype(F32)
            emit[n] = high
            emit[2 + n] = value - high
        return phase, energy, total

    def sweep_cols(target):
        f = fld[...].reshape(2, 128, 256)
        parts = [split(f[0]), split(f[1])]
        lh = jnp.concatenate([parts[0][0], parts[1][0]], axis=1)
        ll = jnp.concatenate([parts[0][1], parts[1][1]], axis=1)
        for part in range(2):
            lanes = slice(256 * part, 256 * part + 256)
            g = jnp.dot(lh, mh[:, lanes], preferred_element_type=F32)
            g = g + jnp.dot(lh, ml[:, lanes], preferred_element_type=F32)
            g = g + jnp.dot(ll, mh[:, lanes], preferred_element_type=F32)
            target[part] = g.reshape(8, 16, 256)

    def rows_of(side, g):
        hi, lo = split(g)
        out = jnp.dot(ah[side], hi, preferred_element_type=F32)
        out = out + jnp.dot(al[side], hi, preferred_element_type=F32)
        return out + jnp.dot(ah[side], lo, preferred_element_type=F32)

    def to_rows(source, dst, ss, rs):
        c1, c2 = (slot + 5) // 8, (slot + 8) // 8
        for q in (2, 6, 3, 7, 1, 5, 0, 4):
            v = place ^ q
            for n, cc in ((0, c1), (1, c2)):
                extra = None if n == 0 else c1 != c2
                w = slot - 8 * cc + 8
                send(source(v), dst.at[w], ss.at[n, v], rs.at[w], cc % CUTS, 8 * h + v, extra, False)

    def cells_for(period):
        mark("w_ce")
        for k in (1, 2):
            sure_await(rce.at[period - 1, k - 1], s_ce.at[period - 1, k - 1], r_ce.at[period - 1, k - 1])
        mark("hot")
        cell_f[period] = jnp.where(shifts[period] == 1, rce[period - 1, 0], rce[period - 1, 1])
        build_onehot(period)

    mark("w_xel")
    for k in (1, 2):
        for v in range(8):
            await_from(rxel.at[k - 1, v], s_xel.at[k - 1, v], r_xel.at[k - 1, v],
                       ((slot + k) % SLOTS) // 8, 8 * h + v)
    loads[6].wait()
    mark("first")
    one = shifts[0] == 1
    for v in range(8):
        state[4 * v:4 * v + 4, :] = jnp.where(one, rxel[0, v, 0], rxel[1, v, 0])
        state[32 + 4 * v:36 + 4 * v, :] = jnp.where(one, rxel[0, v, 1], rxel[1, v, 1])
        cell_f[0, 4 * v:4 * v + 4, :] = jnp.where(one, rxel[0, v, 2], rxel[1, v, 2])
    state[64:72, :] = jnp.zeros((8, 128), F32)
    build_onehot(0)
    moved = shifts[0]
    mark("w_a2a")
    for v in range(8):
        await_from(arr.at[:, v], s_a2a.at[v], r_a2a.at[v], z * 2 + group, 8 * h + v)
    fld[...] = jnp.where(((slot + moved) & 255) < shifts[0], 0.0, arr[...])
    for period in range(4):
        mark("samp")
        sample()
        if period > 0:
            mark("w_st")
            for k in (1, 2):
                sure_await(rst.at[period - 1, k - 1], s_st.at[period - 1, k - 1], r_st.at[period - 1, k - 1])
            state[...] = jnp.where(shifts[period] == 1, rst[period - 1, 0], rst[period - 1, 1])
        mark("kick")
        phase, energy, total = kick(period)
        if period < 3:
            sst[period, 0:32, :] = phase
            sst[period, 32:64, :] = energy
            sst[period, 64:72, :] = total
            relay(sst.at[period], rst, s_st, r_st, period)
        else:
            state[0:32, :] = phase
            state[32:64, :] = energy
            psum[...] = total
            sure_send(psum, psum_in, s_ps, r_ps, partner, b)
        mark("dep")
        deposit()

        mark("col")
        sweep_cols(gown.at[period])
        for part in range(2):
            sure_send(gown.at[period, part], goth.at[period, part],
                      s_ex.at[period, part], r_ex.at[period, part], partner, b)
        mark("rowown")
        acc = rows_of(0, gown[period].reshape(256, 256))
        if period < 3:
            cells_for(period + 1)
        else:
            mark("elsend")
            sure_await(psum_in, s_ps, r_ps)
            diagonal = (lax.broadcasted_iota(jnp.int32, (8, 128), 0)
                        == lax.broadcasted_iota(jnp.int32, (8, 128), 1))
            total = jnp.sum(psum[...] + psum_in[...], axis=1, keepdims=True)
            total = jnp.sum(jnp.where(diagonal, total, 0.0), axis=0, keepdims=True)
            for v in range(8):
                efin[v, 0:4, :] = state[4 * v:4 * v + 4, :]
                efin[v, 4:8, :] = state[32 + 4 * v:36 + 4 * v, :]
                efin[v, 8:9, :] = total
            to_rows(lambda v: efin.at[v], rel, s_el, r_el)
        mark("w_ex")
        for part in range(2):
            sure_await(goth.at[period, part], s_ex.at[period, part], r_ex.at[period, part])
        mark("rowoth")
        acc = (acc + rows_of(1, goth[period].reshape(256, 256))).reshape(2, 8, 16, 256)
        if period < 3:
            moved = moved + shifts[period + 1]
            fld[...] = jnp.where(((slot + moved) & 255) < shifts[period + 1], 0.0, acc)

    mark("fsend")
    fin[...] = acc
    to_rows(lambda v: fin.at[:, v], rfld, s_fld, r_fld)

    mark("w_small")
    for w in range(11):
        sure_await(rel.at[w], s_el.at[0, 0], r_el.at[w])
    mark("w_fld")
    for w in range(11):
        sure_await(rfld.at[w], s_fld.at[0, 0], r_fld.at[w])

    mark("drain")
    for there, src, dst, ss, rs in sends:
        copy = remote(src, dst, ss, rs, c, b)
        if there is None:
            copy.wait_send()
        else:
            @pl.when(there)
            def _():
                copy.wait_send()
    mark(None)


def hand_over(shifts_in, fields, electrons, field_out, phase_out, energy_out, bunching_out,
              shifts, rfld, rel, out_fld, out_ph, out_en, out_sums, bunching, sem):
    ins = [(shifts_in, shifts), (electrons, rel), (fields, rfld)]
    outs = [(out_ph, phase_out), (out_en, energy_out), (bunching, bunching_out), (out_fld, field_out)]
    ins = [pltpu.make_async_copy(src, dst, sem.at[n]) for n, (src, dst) in enumerate(ins)]
    outs = [pltpu.make_async_copy(src, dst, sem.at[3 + n]) for n, (src, dst) in enumerate(outs)]
    for copy in ins:
        copy.start()
    for copy in ins:
        copy.wait()
    base = jnp.clip(8 - (shifts[0] + shifts[1] + shifts[2] + shifts[3]), 0, 3)
    for u in range(8):
        out_fld[:, u] = rfld[base + u]
    outs[3].start()
    lane = lax.broadcasted_iota(jnp.int32, (8, 8), 1)
    diagonal = (lax.broadcasted_iota(jnp.int32, (8, 128), 0)
                == lax.broadcasted_iota(jnp.int32, (8, 128), 1))
    sums = jnp.zeros((8, 8), F32)
    for u in range(8):
        tile = rel[base + u]
        for i in range(4):
            lanes = slice(128 * i, 128 * i + 128)
            out_ph[u:u + 1, lanes] = tile[i:i + 1]
            out_en[u:u + 1, lanes] = tile[4 + i:5 + i]
        total = jnp.sum(jnp.where(diagonal, tile[8:9], 0.0), axis=1, keepdims=True)
        sums = jnp.where(lane == u, total, sums)
    out_sums[...] = sums * ELEC ** (-0.5)
    for period in range(4):
        bunching[period] = out_sums[2 * period:2 * period + 2]
    for copy in outs[:3]:
        copy.start()
    for copy in outs:
        copy.wait()


def shards(field, row_prop, col_prop, phase, energy, cells, shifts):
    V = pltpu.VMEM
    D = pltpu.SemaphoreType.DMA
    blocks = (2, 8, 16, 256)
    square = (2, 256, 256)
    scratch = [
        V(blocks, F32), V(square, F32), V(square, F32),
        V((8, 512), F32), V((8, 512), F32), V((8, 512), jnp.int32),
        V((512, 512), BF16), V((512, 512), BF16), V(square, BF16), V(square, BF16),
        V((32, 128), jnp.int32), V((32, 128), jnp.int32), V((8, 128, 512), BF16),
        V(blocks, F32), V(blocks, F32), V((4, *blocks), F32), V((4, *blocks), F32),
        V((2, 32, 128), F32), V((4, 32, 128), F32), V((72, 128), F32), V((4, 32, 128), F32),
        pltpu.SMEM((4,), jnp.int32),
        V((8, 3, 4, 128), F32), V((2, 8, 3, 4, 128), F32), V((3, 72, 128), F32),
        V((3, 2, 72, 128), F32), V((3, 2, 32, 128), F32), V((8, 128), F32), V((8, 128), F32),
        V((8, 9, 128), F32), V(blocks, F32),
        D((11,)), D((8,)), D((8,)), D((2, 8)), D((2, 8)), D((4, 2)), D((4, 2)),
        D((3, 2)), D((3, 2)), D((3, 2)), D((3, 2)), D, D,
        D((2, 8)), D((11,)), D((2, 8)), D((11,)),
    ]
    hbm = pl.BlockSpec(memory_space=pl.ANY)
    results = (jax.ShapeDtypeStruct(blocks, F32), jax.ShapeDtypeStruct((8, 512), F32),
               jax.ShapeDtypeStruct((8, 512), F32))
    out = pl.pallas_call(
        kernel,
        out_shape=(jax.ShapeDtypeStruct((11, 2, 16, 256), F32), jax.ShapeDtypeStruct((11, 9, 128), F32)),
        in_specs=[hbm] * 7,
        out_specs=[hbm] * 2,
        scratch_shapes=scratch,
        compiler_params=pltpu.CompilerParams(
            collective_id=0, has_side_effects=True, vmem_limit_bytes=VMEM_LIMIT),
    )(shifts, field, row_prop, col_prop, phase, energy, cells)
    return pl.pallas_call(
        hand_over,
        out_shape=(*results, jax.ShapeDtypeStruct((4, 2, 8), F32)),
        in_specs=[hbm] * 3,
        out_specs=[hbm] * 4,
        scratch_shapes=[pltpu.SMEM((4,), jnp.int32), V((11, 2, 16, 256), F32), V((11, 9, 128), F32),
                        V(blocks, F32), V((8, 512), F32), V((8, 512), F32), V((8, 8), F32),
                        V((4, 2, 8), F32), D((7,))],
        compiler_params=pltpu.CompilerParams(vmem_limit_bytes=VMEM_LIMIT),
    )(shifts, *out)


def solution(mesh):
    return jax.shard_map(
        shards,
        mesh=mesh,
        in_specs=(
            P(None, "cuts", "row", None),
            P(),
            P(),
            P("cuts", "row"),
            P("cuts", "row"),
            P("cuts", "row"),
            P(),
        ),
        out_specs=(
            P(None, "cuts", "row", None),
            P("cuts", "row"),
            P("cuts", "row"),
            P(None, None, "cuts"),
        ),
        check_vma=False,
    )
```

```python
import jax
import jax.numpy as jnp
from jax import lax
from jax.experimental import pallas as pl
from jax.experimental.pallas import tpu as pltpu
from jax.sharding import PartitionSpec as P

F32 = jnp.float32
BF16 = jnp.bfloat16
MESH = pl.DeviceIdType.MESH
ELEC = 8192
CUTS = 32
SLOTS = 256
VMEM_LIMIT = 67_000_000
kick_rate = 0.5
source_gain = 0.5


def split(x):
    high = x.astype(BF16)
    return high, (x - high.astype(F32)).astype(BF16)


PATH = (0, 1, 5, 6, 10, 11, 15, 12, 8, 4, 7, 3, 2, 14, 13, 9)


def lookup(table, i):
    low = sum(n << (3 * (q % 8)) for q, n in enumerate(t % 8 for t in table[:8]))
    high = sum(n << (3 * (q % 8)) for q, n in enumerate(t % 8 for t in table[8:]))
    tops = sum((t // 8) << q for q, t in enumerate(table))
    word = jnp.where(i < 8, low, high)
    return ((word >> (3 * (i % 8))) & 7) + 8 * ((tops >> i) & 1)


def chip_of(j):
    z, at = j // 16, lookup(PATH, j % 16)
    return z, (at % 4 + z) % 4 + 4 * ((at // 4 + 2 * z) % 4)


def slot_of(z, b):
    at = (b % 4 + 3 * z) % 4 + 4 * ((b // 4 + 2 * z) % 4)
    return z * 16 + lookup(tuple(PATH.index(q) for q in range(16)), at)


def kernel(shifts_in, field_in, row_in, col_in, phase_in, energy_in, cells_in,
           rfld, rel,
           own, rowp, colp, ph_in, en_in, ce_in, mh, ml, ah, al,
           key_i, col_i, onehot, fld, arr, gown, goth, samp, emit, state, cell_f,
           shifts, xel, rxel, sst, rst, rce, psum, psum_in, efin, fin,
           lsem, s_a2a, r_a2a, s_xel, r_xel, s_ex, r_ex, s_st, r_st, s_ce, r_ce,
           s_ps, r_ps, s_fld, r_fld, s_el, r_el):
    c = lax.axis_index("cuts")
    b = lax.axis_index("row")
    z = c // 2
    h = c % 2
    half = b // 8
    place = b % 8
    slot = slot_of(z, b)
    group = (slot // 8) % 2
    base_cut = slot // 8
    partner = c + 1 - 2 * h
    sends = []
    scope = []

    def mark(name):
        if scope:
            scope.pop().__exit__(None, None, None)
        if name:
            scope.append(jax.named_scope(name))
            scope[0].__enter__()

    def remote(src, dst, ss, rs, dc, db):
        return pltpu.make_async_remote_copy(
            src_ref=src, dst_ref=dst, send_sem=ss, recv_sem=rs,
            device_id=(dc, db), device_id_type=MESH)

    def send(src, dst, ss, rs, dc, db, extra=None, far=True):
        here = (dc == c) & (db == b)
        there = jnp.logical_not(here)
        if extra is not None:
            here = here & extra
            there = there & extra

        @pl.when(there)
        def _():
            remote(src, dst, ss, rs, dc, db).start()

        @pl.when(here)
        def _():
            if far:
                dst[...] = src[...]
            else:
                pltpu.make_async_copy(src, dst, rs).start()

        sends.append((there, src, dst, ss, rs))

    def sure_send(src, dst, ss, rs, dc, db):
        remote(src, dst, ss, rs, dc, db).start()
        sends.append((None, src, dst, ss, rs))

    def await_from(dst, ss, rs, dc, db):
        @pl.when(jnp.logical_not((dc == c) & (db == b)))
        def _():
            remote(dst, dst, ss, rs, dc, db).wait_recv()

    def sure_await(dst, ss, rs):
        remote(dst, dst, ss, rs, c, b).wait_recv()

    mark("start")
    barrier = pltpu.get_barrier_semaphore()
    below = (base_cut + 1) % CUTS
    itself = (half == h) & ((base_cut == c) | ((below == c) & (slot % 8 >= 6)))
    def greet(dc, extra=None):
        for v in range(8):
            ok = jnp.logical_not((dc == c) & (8 * h + v == b))

            @pl.when(ok if extra is None else ok & extra)
            def _():
                pl.semaphore_signal(barrier, inc=1, device_id=(dc, 8 * h + v), device_id_type=MESH)

    greet(base_cut)
    greet(below, slot % 8 >= 6)
    for k in (1, 2):
        pz, pb = chip_of((slot + k) % SLOTS)
        pl.semaphore_signal(barrier, inc=1, device_id=(pz * 2 + h, pb), device_id_type=MESH)
    pl.semaphore_signal(barrier, inc=1, device_id=(partner, b), device_id_type=MESH)

    loads = [(phase_in, ph_in), (energy_in, en_in), (cells_in, ce_in), (field_in, own),
             (col_in, colp), (row_in, rowp), (shifts_in, shifts)]
    loads = [pltpu.make_async_copy(src, dst, lsem.at[n]) for n, (src, dst) in enumerate(loads)]
    for copy in loads:
        copy.start()

    mark("unpack")
    for n in (0, 1, 2):
        loads[n].wait()
    for u in range(8):
        for i in range(4):
            lanes = slice(128 * i, 128 * i + 128)
            xel[u, 0, i:i + 1, :] = ph_in[u:u + 1, lanes]
            xel[u, 1, i:i + 1, :] = en_in[u:u + 1, lanes]
            xel[u, 2, i:i + 1, :] = ce_in[u:u + 1, lanes].astype(F32)

    mark("w_barrier")
    loads[3].wait()
    pl.semaphore_wait(barrier, 13 - jnp.where(itself, 1, 0))

    mark("send0")
    for i in range(8):
        u = (place + i) % 8
        for k in (1, 2):
            pz, pb = chip_of((8 * c + u - k + SLOTS) % SLOTS)
            send(xel.at[u], rxel.at[k - 1, place], s_xel.at[k - 1, u], r_xel.at[k - 1, place], pz * 2 + half, pb)
    for i in range(8):
        u = (place + i) % 8
        _, db = chip_of(8 * c + u)
        send(own.at[:, u], arr.at[:, place], s_a2a.at[u], r_a2a.at[place], z * 2 + half, db)

    mark("prep")
    loads[4].wait()
    loads[5].wait()
    for part in range(2):
        hi, lo = split(jnp.transpose(colp[part]))
        places = ((0, 0, 1), (1, 1, 1)) if part == 0 else ((1, 0, -1), (0, 1, 1))
        for kk, nn, sign in places:
            at = (slice(256 * kk, 256 * kk + 256), slice(256 * nn, 256 * nn + 256))
            mh[at] = hi if sign > 0 else -hi
            ml[at] = lo if sign > 0 else -lo
    rows = pl.ds(pl.multiple_of(h * 128, 128), 128)
    for side in range(2):
        cols = pl.ds(pl.multiple_of((h + side - 2 * h * side) * 128, 128), 128)
        rr = split(rowp[0, rows, cols])
        ri = split(rowp[1, rows, cols])
        for n, ref in ((0, ah), (1, al)):
            ref[side, 0:128, 0:128] = rr[n]
            ref[side, 0:128, 128:256] = -ri[n]
            ref[side, 128:256, 0:128] = ri[n]
            ref[side, 128:256, 128:256] = rr[n]

    def build_onehot(period):
        if period < 3:
            relay(cell_f.at[period], rce, s_ce, r_ce, period)
        cell = cell_f[period].astype(jnp.int32)
        key_i[...] = ((cell >> 8) & 15) + ((cell >> 7) & 1) * 16
        col_i[...] = cell & 127
        iota = lax.broadcasted_iota(jnp.int32, (128, 128), 0)
        for u in range(8):
            for i in range(4):
                at = 4 * u + i
                hot = jnp.where(iota == col_i[at:at + 1, :], 1.0, 0.0)
                onehot[u, :, 128 * i:128 * i + 128] = hot.astype(BF16)

    def relay(src, dst, ss, rs, period):
        for k in (2, 1):
            pz, pb = chip_of((slot - k + SLOTS) % SLOTS)
            sure_send(src, dst.at[period, k - 1], ss.at[period, k - 1], rs.at[period, k - 1], pz * 2 + h, pb)

    def sample():
        iota = lax.broadcasted_iota(jnp.int32, (32, 128), 0)
        for u in range(8):
            fu = jnp.concatenate([fld[p, u, :, 128 * q:128 * q + 128] for p in range(2) for q in range(2)], axis=0)
            hi, lo = split(fu)
            got = jnp.dot(jnp.concatenate([hi, lo], axis=0), onehot[u], preferred_element_type=F32)
            got = got[0:64] + got[64:128]
            for i in range(4):
                at = 4 * u + i
                lanes = slice(128 * i, 128 * i + 128)
                mask = iota == key_i[at:at + 1, :]
                for part in range(2):
                    picked = jnp.where(mask, got[32 * part:32 * part + 32, lanes], 0.0)
                    samp[part, at:at + 1, :] = jnp.sum(picked, axis=0, keepdims=True)

    def deposit():
        iota = lax.broadcasted_iota(jnp.int32, (32, 128), 0)
        for u in range(8):
            pieces = []
            for i in range(4):
                at = 4 * u + i
                mask = iota == key_i[at:at + 1, :]
                pieces.append(jnp.concatenate(
                    [jnp.where(mask, emit[n, at:at + 1, :], 0.0).astype(BF16) for n in range(4)], axis=0))
            weights = jnp.concatenate(pieces, axis=1)
            add = lax.dot_general(weights, onehot[u], (((1,), (1,)), ((), ())), preferred_element_type=F32)
            add = add[0:64] + add[64:128]
            for p in range(2):
                for q in range(2):
                    lanes = slice(128 * q, 128 * q + 128)
                    rows = slice(32 * p + 16 * q, 32 * p + 16 * q + 16)
                    fld[p, u, :, lanes] = fld[p, u, :, lanes] + add[rows]

    def kick(period):
        cosine, sine = jnp.cos(state[0:32, :]), jnp.sin(state[0:32, :])
        energy = state[32:64, :] - kick_rate * (samp[0] * cosine - samp[1] * sine)
        phase = state[0:32, :] + energy
        cosine, sine = jnp.cos(phase), jnp.sin(phase)
        line = lax.broadcasted_iota(jnp.int32, (8, 128), 0)
        total = state[64:72, :]
        total = total + jnp.where(line == 2 * period, jnp.sum(cosine, axis=0, keepdims=True), 0.0)
        total = total + jnp.where(line == 2 * period + 1, -jnp.sum(sine, axis=0, keepdims=True), 0.0)
        for n, value in ((0, source_gain * cosine), (1, -source_gain * sine)):
            high = value.astype(BF16).astype(F32)
            emit[n] = high
            emit[2 + n] = value - high
        return phase, energy, total

    def sweep_cols(target):
        f = fld[...].reshape(2, 128, 256)
        parts = [split(f[0]), split(f[1])]
        lh = jnp.concatenate([parts[0][0], parts[1][0]], axis=1)
        ll = jnp.concatenate([parts[0][1], parts[1][1]], axis=1)
        for part in range(2):
            lanes = slice(256 * part, 256 * part + 256)
            g = jnp.dot(lh, mh[:, lanes], preferred_element_type=F32)
            g = g + jnp.dot(lh, ml[:, lanes], preferred_element_type=F32)
            g = g + jnp.dot(ll, mh[:, lanes], preferred_element_type=F32)
            target[part] = g.reshape(8, 16, 256)

    def rows_of(side, g):
        hi, lo = split(g)
        out = jnp.dot(ah[side], hi, preferred_element_type=F32)
        out = out + jnp.dot(al[side], hi, preferred_element_type=F32)
        return out + jnp.dot(ah[side], lo, preferred_element_type=F32)

    def to_rows(source, dst, ss, rs):
        c1, c2 = (slot + 5) // 8, (slot + 8) // 8
        for q in (2, 6, 3, 7, 1, 5, 0, 4):
            v = place ^ q
            for n, cc in ((1, c2), (0, c1)):
                extra = None if n == 0 else c1 != c2
                w = slot - 8 * cc + 8
                send(source(v), dst.at[w], ss.at[n, v], rs.at[w], cc % CUTS, 8 * h + v, extra, False)

    def cells_for(period):
        mark("w_ce")
        for k in (1, 2):
            sure_await(rce.at[period - 1, k - 1], s_ce.at[period - 1, k - 1], r_ce.at[period - 1, k - 1])
        mark("hot")
        cell_f[period] = jnp.where(shifts[period] == 1, rce[period - 1, 0], rce[period - 1, 1])
        build_onehot(period)

    mark("w_xel")
    for k in (1, 2):
        for v in range(8):
            await_from(rxel.at[k - 1, v], s_xel.at[k - 1, v], r_xel.at[k - 1, v],
                       ((slot + k) % SLOTS) // 8, 8 * h + v)
    loads[6].wait()
    mark("first")
    one = shifts[0] == 1
    for v in range(8):
        state[4 * v:4 * v + 4, :] = jnp.where(one, rxel[0, v, 0], rxel[1, v, 0])
        state[32 + 4 * v:36 + 4 * v, :] = jnp.where(one, rxel[0, v, 1], rxel[1, v, 1])
        cell_f[0, 4 * v:4 * v + 4, :] = jnp.where(one, rxel[0, v, 2], rxel[1, v, 2])
    state[64:72, :] = jnp.zeros((8, 128), F32)
    build_onehot(0)
    moved = shifts[0]
    mark("w_a2a")
    for v in range(8):
        await_from(arr.at[:, v], s_a2a.at[v], r_a2a.at[v], z * 2 + group, 8 * h + v)
    fld[...] = jnp.where(((slot + moved) & 255) < shifts[0], 0.0, arr[...])
    for period in range(4):
        mark("samp")
        sample()
        if period > 0:
            mark("w_st")
            for k in (1, 2):
                sure_await(rst.at[period - 1, k - 1], s_st.at[period - 1, k - 1], r_st.at[period - 1, k - 1])
            state[...] = jnp.where(shifts[period] == 1, rst[period - 1, 0], rst[period - 1, 1])
        mark("kick")
        phase, energy, total = kick(period)
        if period < 3:
            sst[period, 0:32, :] = phase
            sst[period, 32:64, :] = energy
            sst[period, 64:72, :] = total
            relay(sst.at[period], rst, s_st, r_st, period)
        else:
            state[0:32, :] = phase
            state[32:64, :] = energy
            psum[...] = total
            sure_send(psum, psum_in, s_ps, r_ps, partner, b)
        mark("dep")
        deposit()

        mark("col")
        sweep_cols(gown.at[period])
        for part in range(2):
            sure_send(gown.at[period, part], goth.at[period, part],
                      s_ex.at[period, part], r_ex.at[period, part], partner, b)
        mark("rowown")
        acc = rows_of(0, gown[period].reshape(256, 256))
        if period < 3:
            cells_for(period + 1)
        else:
            mark("elsend")
            sure_await(psum_in, s_ps, r_ps)
            diagonal = (lax.broadcasted_iota(jnp.int32, (8, 128), 0)
                        == lax.broadcasted_iota(jnp.int32, (8, 128), 1))
            total = jnp.sum(psum[...] + psum_in[...], axis=1, keepdims=True)
            total = jnp.sum(jnp.where(diagonal, total, 0.0), axis=0, keepdims=True)
            for v in range(8):
                efin[v, 0:4, :] = state[4 * v:4 * v + 4, :]
                efin[v, 4:8, :] = state[32 + 4 * v:36 + 4 * v, :]
                efin[v, 8:9, :] = total
            to_rows(lambda v: efin.at[v], rel, s_el, r_el)
        mark("w_ex")
        for part in range(2):
            sure_await(goth.at[period, part], s_ex.at[period, part], r_ex.at[period, part])
        mark("rowoth")
        acc = (acc + rows_of(1, goth[period].reshape(256, 256))).reshape(2, 8, 16, 256)
        if period < 3:
            moved = moved + shifts[period + 1]
            fld[...] = jnp.where(((slot + moved) & 255) < shifts[period + 1], 0.0, acc)

    mark("fsend")
    fin[...] = acc
    to_rows(lambda v: fin.at[:, v], rfld, s_fld, r_fld)

    mark("w_small")
    for w in range(11):
        sure_await(rel.at[w], s_el.at[0, 0], r_el.at[w])
    mark("w_fld")
    for w in range(11):
        sure_await(rfld.at[w], s_fld.at[0, 0], r_fld.at[w])

    mark("drain")
    for there, src, dst, ss, rs in sends:
        copy = remote(src, dst, ss, rs, c, b)
        if there is None:
            copy.wait_send()
        else:
            @pl.when(there)
            def _():
                copy.wait_send()
    mark(None)


def hand_over(shifts_in, fields, electrons, field_out, phase_out, energy_out, bunching_out,
              shifts, rfld, rel, out_fld, out_ph, out_en, out_sums, bunching, sem):
    ins = [(shifts_in, shifts), (electrons, rel), (fields, rfld)]
    outs = [(out_ph, phase_out), (out_en, energy_out), (bunching, bunching_out), (out_fld, field_out)]
    ins = [pltpu.make_async_copy(src, dst, sem.at[n]) for n, (src, dst) in enumerate(ins)]
    outs = [pltpu.make_async_copy(src, dst, sem.at[3 + n]) for n, (src, dst) in enumerate(outs)]
    for copy in ins:
        copy.start()
    ins[0].wait()
    ins[1].wait()
    base = jnp.clip(8 - (shifts[0] + shifts[1] + shifts[2] + shifts[3]), 0, 3)
    lane = lax.broadcasted_iota(jnp.int32, (8, 8), 1)
    diagonal = (lax.broadcasted_iota(jnp.int32, (8, 128), 0)
                == lax.broadcasted_iota(jnp.int32, (8, 128), 1))
    sums = jnp.zeros((8, 8), F32)
    for u in range(8):
        tile = rel[base + u]
        for i in range(4):
            lanes = slice(128 * i, 128 * i + 128)
            out_ph[u:u + 1, lanes] = tile[i:i + 1]
            out_en[u:u + 1, lanes] = tile[4 + i:5 + i]
        total = jnp.sum(jnp.where(diagonal, tile[8:9], 0.0), axis=1, keepdims=True)
        sums = jnp.where(lane == u, total, sums)
    out_sums[...] = sums * ELEC ** (-0.5)
    for period in range(4):
        bunching[period] = out_sums[2 * period:2 * period + 2]
    for copy in outs[:3]:
        copy.start()
    ins[2].wait()
    for u in range(8):
        out_fld[:, u] = rfld[base + u]
    outs[3].start()
    for copy in outs:
        copy.wait()


def shards(field, row_prop, col_prop, phase, energy, cells, shifts):
    V = pltpu.VMEM
    D = pltpu.SemaphoreType.DMA
    blocks = (2, 8, 16, 256)
    square = (2, 256, 256)
    scratch = [
        V(blocks, F32), V(square, F32), V(square, F32),
        V((8, 512), F32), V((8, 512), F32), V((8, 512), jnp.int32),
        V((512, 512), BF16), V((512, 512), BF16), V(square, BF16), V(square, BF16),
        V((32, 128), jnp.int32), V((32, 128), jnp.int32), V((8, 128, 512), BF16),
        V(blocks, F32), V(blocks, F32), V((4, *blocks), F32), V((4, *blocks), F32),
        V((2, 32, 128), F32), V((4, 32, 128), F32), V((72, 128), F32), V((4, 32, 128), F32),
        pltpu.SMEM((4,), jnp.int32),
        V((8, 3, 4, 128), F32), V((2, 8, 3, 4, 128), F32), V((3, 72, 128), F32),
        V((3, 2, 72, 128), F32), V((3, 2, 32, 128), F32), V((8, 128), F32), V((8, 128), F32),
        V((8, 9, 128), F32), V(blocks, F32),
        D((11,)), D((8,)), D((8,)), D((2, 8)), D((2, 8)), D((4, 2)), D((4, 2)),
        D((3, 2)), D((3, 2)), D((3, 2)), D((3, 2)), D, D,
        D((2, 8)), D((11,)), D((2, 8)), D((11,)),
    ]
    hbm = pl.BlockSpec(memory_space=pl.ANY)
    results = (jax.ShapeDtypeStruct(blocks, F32), jax.ShapeDtypeStruct((8, 512), F32),
               jax.ShapeDtypeStruct((8, 512), F32))
    out = pl.pallas_call(
        kernel,
        out_shape=(jax.ShapeDtypeStruct((11, 2, 16, 256), F32), jax.ShapeDtypeStruct((11, 9, 128), F32)),
        in_specs=[hbm] * 7,
        out_specs=[hbm] * 2,
        scratch_shapes=scratch,
        compiler_params=pltpu.CompilerParams(
            collective_id=0, has_side_effects=True, vmem_limit_bytes=VMEM_LIMIT),
    )(shifts, field, row_prop, col_prop, phase, energy, cells)
    return pl.pallas_call(
        hand_over,
        out_shape=(*results, jax.ShapeDtypeStruct((4, 2, 8), F32)),
        in_specs=[hbm] * 3,
        out_specs=[hbm] * 4,
        scratch_shapes=[pltpu.SMEM((4,), jnp.int32), V((11, 2, 16, 256), F32), V((11, 9, 128), F32),
                        V(blocks, F32), V((8, 512), F32), V((8, 512), F32), V((8, 8), F32),
                        V((4, 2, 8), F32), D((7,))],
        compiler_params=pltpu.CompilerParams(vmem_limit_bytes=VMEM_LIMIT),
    )(shifts, *out)


def solution(mesh):
    return jax.shard_map(
        shards,
        mesh=mesh,
        in_specs=(
            P(None, "cuts", "row", None),
            P(),
            P(),
            P("cuts", "row"),
            P("cuts", "row"),
            P("cuts", "row"),
            P(),
        ),
        out_specs=(
            P(None, "cuts", "row", None),
            P("cuts", "row"),
            P("cuts", "row"),
            P(None, None, "cuts"),
        ),
        check_vma=False,
    )
```

```python
import jax
import jax.numpy as jnp
from jax import lax
from jax.experimental import pallas as pl
from jax.experimental.pallas import tpu as pltpu
from jax.sharding import PartitionSpec as P

F32 = jnp.float32
BF16 = jnp.bfloat16
MESH = pl.DeviceIdType.MESH
ELEC = 8192
CUTS = 32
SLOTS = 256
VMEM_LIMIT = 67_000_000
kick_rate = 0.5
source_gain = 0.5


def split(x):
    high = x.astype(BF16)
    return high, (x - high.astype(F32)).astype(BF16)


PATH = (0, 1, 5, 6, 10, 11, 15, 12, 8, 4, 7, 3, 2, 14, 13, 9)


def lookup(table, i):
    low = sum(n << (3 * (q % 8)) for q, n in enumerate(t % 8 for t in table[:8]))
    high = sum(n << (3 * (q % 8)) for q, n in enumerate(t % 8 for t in table[8:]))
    tops = sum((t // 8) << q for q, t in enumerate(table))
    word = jnp.where(i < 8, low, high)
    return ((word >> (3 * (i % 8))) & 7) + 8 * ((tops >> i) & 1)


def chip_of(j):
    z, at = j // 16, lookup(PATH, j % 16)
    return z, (at % 4 + z) % 4 + 4 * ((at // 4 + 2 * z) % 4)


def slot_of(z, b):
    at = (b % 4 + 3 * z) % 4 + 4 * ((b // 4 + 2 * z) % 4)
    return z * 16 + lookup(tuple(PATH.index(q) for q in range(16)), at)


def kernel(shifts_in, field_in, row_in, col_in, phase_in, energy_in, cells_in,
           rfld, rel,
           own, rowp, colp, ph_in, en_in, ce_in, mh, ml, ah, al,
           key_i, col_i, onehot, fld, arr, gown, goth, samp, emit, state, cell_f,
           shifts, xel, rxel, sst, rst, rce, psum, psum_in, efin, fin,
           lsem, s_a2a, r_a2a, s_xel, r_xel, s_ex, r_ex, s_st, r_st, s_ce, r_ce,
           s_ps, r_ps, s_fld, r_fld, s_el, r_el):
    c = lax.axis_index("cuts")
    b = lax.axis_index("row")
    z = c // 2
    h = c % 2
    half = b // 8
    place = b % 8
    slot = slot_of(z, b)
    group = (slot // 8) % 2
    base_cut = slot // 8
    partner = c + 1 - 2 * h
    sends = []
    scope = []

    def mark(name):
        if scope:
            scope.pop().__exit__(None, None, None)
        if name:
            scope.append(jax.named_scope(name))
            scope[0].__enter__()

    def remote(src, dst, ss, rs, dc, db):
        return pltpu.make_async_remote_copy(
            src_ref=src, dst_ref=dst, send_sem=ss, recv_sem=rs,
            device_id=(dc, db), device_id_type=MESH)

    def send(src, dst, ss, rs, dc, db, extra=None, far=True):
        here = (dc == c) & (db == b)
        there = jnp.logical_not(here)
        if extra is not None:
            here = here & extra
            there = there & extra

        @pl.when(there)
        def _():
            remote(src, dst, ss, rs, dc, db).start()

        @pl.when(here)
        def _():
            if far:
                dst[...] = src[...]
            else:
                pltpu.make_async_copy(src, dst, rs).start()

        sends.append((there, src, dst, ss, rs))

    def sure_send(src, dst, ss, rs, dc, db):
        remote(src, dst, ss, rs, dc, db).start()
        sends.append((None, src, dst, ss, rs))

    def await_from(dst, ss, rs, dc, db):
        @pl.when(jnp.logical_not((dc == c) & (db == b)))
        def _():
            remote(dst, dst, ss, rs, dc, db).wait_recv()

    def sure_await(dst, ss, rs):
        remote(dst, dst, ss, rs, c, b).wait_recv()

    mark("start")
    barrier = pltpu.get_barrier_semaphore()
    below = (base_cut + 1) % CUTS
    itself = (half == h) & ((base_cut == c) | ((below == c) & (slot % 8 >= 6)))
    def greet(dc, extra=None):
        for v in range(8):
            ok = jnp.logical_not((dc == c) & (8 * h + v == b))

            @pl.when(ok if extra is None else ok & extra)
            def _():
                pl.semaphore_signal(barrier, inc=1, device_id=(dc, 8 * h + v), device_id_type=MESH)

    greet(below, slot % 8 >= 6)
    greet(base_cut)
    for k in (1, 2):
        pz, pb = chip_of((slot + k) % SLOTS)
        pl.semaphore_signal(barrier, inc=1, device_id=(pz * 2 + h, pb), device_id_type=MESH)
    pl.semaphore_signal(barrier, inc=1, device_id=(partner, b), device_id_type=MESH)

    loads = [(phase_in, ph_in), (energy_in, en_in), (cells_in, ce_in), (field_in, own),
             (col_in, colp), (row_in, rowp), (shifts_in, shifts)]
    loads = [pltpu.make_async_copy(src, dst, lsem.at[n]) for n, (src, dst) in enumerate(loads)]
    for copy in loads:
        copy.start()

    mark("unpack")
    for n in (0, 1, 2):
        loads[n].wait()
    for u in range(8):
        for i in range(4):
            lanes = slice(128 * i, 128 * i + 128)
            xel[u, 0, i:i + 1, :] = ph_in[u:u + 1, lanes]
            xel[u, 1, i:i + 1, :] = en_in[u:u + 1, lanes]
            xel[u, 2, i:i + 1, :] = ce_in[u:u + 1, lanes].astype(F32)

    mark("w_barrier")
    loads[3].wait()
    pl.semaphore_wait(barrier, 13 - jnp.where(itself, 1, 0))

    mark("send0")
    for i in range(8):
        u = (place + i) % 8
        for k in (2, 1):
            pz, pb = chip_of((8 * c + u - k + SLOTS) % SLOTS)
            send(xel.at[u], rxel.at[k - 1, place], s_xel.at[k - 1, u], r_xel.at[k - 1, place], pz * 2 + half, pb)
    for i in range(8):
        u = (place + i) % 8
        _, db = chip_of(8 * c + u)
        send(own.at[:, u], arr.at[:, place], s_a2a.at[u], r_a2a.at[place], z * 2 + half, db)

    mark("prep")
    loads[4].wait()
    loads[5].wait()
    for part in range(2):
        hi, lo = split(jnp.transpose(colp[part]))
        places = ((0, 0, 1), (1, 1, 1)) if part == 0 else ((1, 0, -1), (0, 1, 1))
        for kk, nn, sign in places:
            at = (slice(256 * kk, 256 * kk + 256), slice(256 * nn, 256 * nn + 256))
            mh[at] = hi if sign > 0 else -hi
            ml[at] = lo if sign > 0 else -lo
    rows = pl.ds(pl.multiple_of(h * 128, 128), 128)
    for side in range(2):
        cols = pl.ds(pl.multiple_of((h + side - 2 * h * side) * 128, 128), 128)
        rr = split(rowp[0, rows, cols])
        ri = split(rowp[1, rows, cols])
        for n, ref in ((0, ah), (1, al)):
            ref[side, 0:128, 0:128] = rr[n]
            ref[side, 0:128, 128:256] = -ri[n]
            ref[side, 128:256, 0:128] = ri[n]
            ref[side, 128:256, 128:256] = rr[n]

    def build_onehot(period):
        if period < 3:
            relay(cell_f.at[period], rce, s_ce, r_ce, period)
        cell = cell_f[period].astype(jnp.int32)
        key_i[...] = ((cell >> 8) & 15) + ((cell >> 7) & 1) * 16
        col_i[...] = cell & 127
        iota = lax.broadcasted_iota(jnp.int32, (128, 128), 0)
        for u in range(8):
            for i in range(4):
                at = 4 * u + i
                hot = jnp.where(iota == col_i[at:at + 1, :], 1.0, 0.0)
                onehot[u, :, 128 * i:128 * i + 128] = hot.astype(BF16)

    def relay(src, dst, ss, rs, period):
        for k in (2, 1):
            pz, pb = chip_of((slot - k + SLOTS) % SLOTS)
            sure_send(src, dst.at[period, k - 1], ss.at[period, k - 1], rs.at[period, k - 1], pz * 2 + h, pb)

    def sample():
        iota = lax.broadcasted_iota(jnp.int32, (32, 128), 0)
        for u in range(8):
            fu = jnp.concatenate([fld[p, u, :, 128 * q:128 * q + 128] for p in range(2) for q in range(2)], axis=0)
            hi, lo = split(fu)
            got = jnp.dot(jnp.concatenate([hi, lo], axis=0), onehot[u], preferred_element_type=F32)
            got = got[0:64] + got[64:128]
            for i in range(4):
                at = 4 * u + i
                lanes = slice(128 * i, 128 * i + 128)
                mask = iota == key_i[at:at + 1, :]
                for part in range(2):
                    picked = jnp.where(mask, got[32 * part:32 * part + 32, lanes], 0.0)
                    samp[part, at:at + 1, :] = jnp.sum(picked, axis=0, keepdims=True)

    def deposit():
        iota = lax.broadcasted_iota(jnp.int32, (32, 128), 0)
        for u in range(8):
            pieces = []
            for i in range(4):
                at = 4 * u + i
                mask = iota == key_i[at:at + 1, :]
                pieces.append(jnp.concatenate(
                    [jnp.where(mask, emit[n, at:at + 1, :], 0.0).astype(BF16) for n in range(4)], axis=0))
            weights = jnp.concatenate(pieces, axis=1)
            add = lax.dot_general(weights, onehot[u], (((1,), (1,)), ((), ())), preferred_element_type=F32)
            add = add[0:64] + add[64:128]
            for p in range(2):
                for q in range(2):
                    lanes = slice(128 * q, 128 * q + 128)
                    rows = slice(32 * p + 16 * q, 32 * p + 16 * q + 16)
                    fld[p, u, :, lanes] = fld[p, u, :, lanes] + add[rows]

    def kick(period):
        cosine, sine = jnp.cos(state[0:32, :]), jnp.sin(state[0:32, :])
        energy = state[32:64, :] - kick_rate * (samp[0] * cosine - samp[1] * sine)
        phase = state[0:32, :] + energy
        cosine, sine = jnp.cos(phase), jnp.sin(phase)
        line = lax.broadcasted_iota(jnp.int32, (8, 128), 0)
        total = state[64:72, :]
        total = total + jnp.where(line == 2 * period, jnp.sum(cosine, axis=0, keepdims=True), 0.0)
        total = total + jnp.where(line == 2 * period + 1, -jnp.sum(sine, axis=0, keepdims=True), 0.0)
        for n, value in ((0, source_gain * cosine), (1, -source_gain * sine)):
            high = value.astype(BF16).astype(F32)
            emit[n] = high
            emit[2 + n] = value - high
        return phase, energy, total

    def sweep_cols(target):
        f = fld[...].reshape(2, 128, 256)
        parts = [split(f[0]), split(f[1])]
        lh = jnp.concatenate([parts[0][0], parts[1][0]], axis=1)
        ll = jnp.concatenate([parts[0][1], parts[1][1]], axis=1)
        for part in range(2):
            lanes = slice(256 * part, 256 * part + 256)
            g = jnp.dot(lh, mh[:, lanes], preferred_element_type=F32)
            g = g + jnp.dot(lh, ml[:, lanes], preferred_element_type=F32)
            g = g + jnp.dot(ll, mh[:, lanes], preferred_element_type=F32)
            target[part] = g.reshape(8, 16, 256)

    def rows_of(side, g):
        hi, lo = split(g)
        out = jnp.dot(ah[side], hi, preferred_element_type=F32)
        out = out + jnp.dot(al[side], hi, preferred_element_type=F32)
        return out + jnp.dot(ah[side], lo, preferred_element_type=F32)

    def to_rows(source, dst, ss, rs):
        c1, c2 = (slot + 5) // 8, (slot + 8) // 8
        for q in (2, 6, 3, 7, 1, 5, 0, 4):
            v = place ^ q
            for n, cc in ((1, c2), (0, c1)):
                extra = None if n == 0 else c1 != c2
                w = slot - 8 * cc + 8
                send(source(v), dst.at[w], ss.at[n, v], rs.at[w], cc % CUTS, 8 * h + v, extra, False)

    def cells_for(period):
        mark("w_ce")
        for k in (1, 2):
            sure_await(rce.at[period - 1, k - 1], s_ce.at[period - 1, k - 1], r_ce.at[period - 1, k - 1])
        mark("hot")
        cell_f[period] = jnp.where(shifts[period] == 1, rce[period - 1, 0], rce[period - 1, 1])
        build_onehot(period)

    mark("w_xel")
    for k in (1, 2):
        for v in range(8):
            await_from(rxel.at[k - 1, v], s_xel.at[k - 1, v], r_xel.at[k - 1, v],
                       ((slot + k) % SLOTS) // 8, 8 * h + v)
    loads[6].wait()
    mark("first")
    one = shifts[0] == 1
    for v in range(8):
        state[4 * v:4 * v + 4, :] = jnp.where(one, rxel[0, v, 0], rxel[1, v, 0])
        state[32 + 4 * v:36 + 4 * v, :] = jnp.where(one, rxel[0, v, 1], rxel[1, v, 1])
        cell_f[0, 4 * v:4 * v + 4, :] = jnp.where(one, rxel[0, v, 2], rxel[1, v, 2])
    state[64:72, :] = jnp.zeros((8, 128), F32)
    build_onehot(0)
    moved = shifts[0]
    mark("w_a2a")
    for v in range(8):
        await_from(arr.at[:, v], s_a2a.at[v], r_a2a.at[v], z * 2 + group, 8 * h + v)
    fld[...] = jnp.where(((slot + moved) & 255) < shifts[0], 0.0, arr[...])
    for period in range(4):
        mark("samp")
        sample()
        if period > 0:
            mark("w_st")
            for k in (1, 2):
                sure_await(rst.at[period - 1, k - 1], s_st.at[period - 1, k - 1], r_st.at[period - 1, k - 1])
            state[...] = jnp.where(shifts[period] == 1, rst[period - 1, 0], rst[period - 1, 1])
        mark("kick")
        phase, energy, total = kick(period)
        if period < 3:
            sst[period, 0:32, :] = phase
            sst[period, 32:64, :] = energy
            sst[period, 64:72, :] = total
            relay(sst.at[period], rst, s_st, r_st, period)
        else:
            state[0:32, :] = phase
            state[32:64, :] = energy
            psum[...] = total
            sure_send(psum, psum_in, s_ps, r_ps, partner, b)
        mark("dep")
        deposit()

        mark("col")
        sweep_cols(gown.at[period])
        for part in range(2):
            sure_send(gown.at[period, part], goth.at[period, part],
                      s_ex.at[period, part], r_ex.at[period, part], partner, b)
        mark("rowown")
        acc = rows_of(0, gown[period].reshape(256, 256))
        if period < 3:
            cells_for(period + 1)
        else:
            mark("elsend")
            sure_await(psum_in, s_ps, r_ps)
            diagonal = (lax.broadcasted_iota(jnp.int32, (8, 128), 0)
                        == lax.broadcasted_iota(jnp.int32, (8, 128), 1))
            total = jnp.sum(psum[...] + psum_in[...], axis=1, keepdims=True)
            total = jnp.sum(jnp.where(diagonal, total, 0.0), axis=0, keepdims=True)
            for v in range(8):
                efin[v, 0:4, :] = state[4 * v:4 * v + 4, :]
                efin[v, 4:8, :] = state[32 + 4 * v:36 + 4 * v, :]
                efin[v, 8:9, :] = total
            to_rows(lambda v: efin.at[v], rel, s_el, r_el)
        mark("w_ex")
        for part in range(2):
            sure_await(goth.at[period, part], s_ex.at[period, part], r_ex.at[period, part])
        mark("rowoth")
        acc = (acc + rows_of(1, goth[period].reshape(256, 256))).reshape(2, 8, 16, 256)
        if period < 3:
            moved = moved + shifts[period + 1]
            fld[...] = jnp.where(((slot + moved) & 255) < shifts[period + 1], 0.0, acc)

    mark("fsend")
    fin[...] = acc
    to_rows(lambda v: fin.at[:, v], rfld, s_fld, r_fld)

    mark("w_small")
    for w in range(11):
        sure_await(rel.at[w], s_el.at[0, 0], r_el.at[w])
    mark("w_fld")
    for w in range(11):
        sure_await(rfld.at[w], s_fld.at[0, 0], r_fld.at[w])

    mark("drain")
    for there, src, dst, ss, rs in sends:
        copy = remote(src, dst, ss, rs, c, b)
        if there is None:
            copy.wait_send()
        else:
            @pl.when(there)
            def _():
                copy.wait_send()
    mark(None)


def hand_over(shifts_in, fields, electrons, field_out, phase_out, energy_out, bunching_out,
              shifts, rfld, rel, out_fld, out_ph, out_en, out_sums, bunching, sem):
    ins = [(shifts_in, shifts), (electrons, rel), (fields, rfld)]
    outs = [(out_ph, phase_out), (out_en, energy_out), (bunching, bunching_out), (out_fld, field_out)]
    ins = [pltpu.make_async_copy(src, dst, sem.at[n]) for n, (src, dst) in enumerate(ins)]
    outs = [pltpu.make_async_copy(src, dst, sem.at[3 + n]) for n, (src, dst) in enumerate(outs)]
    for copy in ins:
        copy.start()
    ins[0].wait()
    ins[1].wait()
    base = jnp.clip(8 - (shifts[0] + shifts[1] + shifts[2] + shifts[3]), 0, 3)
    lane = lax.broadcasted_iota(jnp.int32, (8, 8), 1)
    diagonal = (lax.broadcasted_iota(jnp.int32, (8, 128), 0)
                == lax.broadcasted_iota(jnp.int32, (8, 128), 1))
    sums = jnp.zeros((8, 8), F32)
    for u in range(8):
        tile = rel[base + u]
        for i in range(4):
            lanes = slice(128 * i, 128 * i + 128)
            out_ph[u:u + 1, lanes] = tile[i:i + 1]
            out_en[u:u + 1, lanes] = tile[4 + i:5 + i]
        total = jnp.sum(jnp.where(diagonal, tile[8:9], 0.0), axis=1, keepdims=True)
        sums = jnp.where(lane == u, total, sums)
    out_sums[...] = sums * ELEC ** (-0.5)
    for period in range(4):
        bunching[period] = out_sums[2 * period:2 * period + 2]
    for copy in outs[:3]:
        copy.start()
    ins[2].wait()
    for u in range(8):
        out_fld[:, u] = rfld[base + u]
    outs[3].start()
    for copy in outs:
        copy.wait()


def shards(field, row_prop, col_prop, phase, energy, cells, shifts):
    V = pltpu.VMEM
    D = pltpu.SemaphoreType.DMA
    blocks = (2, 8, 16, 256)
    square = (2, 256, 256)
    scratch = [
        V(blocks, F32), V(square, F32), V(square, F32),
        V((8, 512), F32), V((8, 512), F32), V((8, 512), jnp.int32),
        V((512, 512), BF16), V((512, 512), BF16), V(square, BF16), V(square, BF16),
        V((32, 128), jnp.int32), V((32, 128), jnp.int32), V((8, 128, 512), BF16),
        V(blocks, F32), V(blocks, F32), V((4, *blocks), F32), V((4, *blocks), F32),
        V((2, 32, 128), F32), V((4, 32, 128), F32), V((72, 128), F32), V((4, 32, 128), F32),
        pltpu.SMEM((4,), jnp.int32),
        V((8, 3, 4, 128), F32), V((2, 8, 3, 4, 128), F32), V((3, 72, 128), F32),
        V((3, 2, 72, 128), F32), V((3, 2, 32, 128), F32), V((8, 128), F32), V((8, 128), F32),
        V((8, 9, 128), F32), V(blocks, F32),
        D((11,)), D((8,)), D((8,)), D((2, 8)), D((2, 8)), D((4, 2)), D((4, 2)),
        D((3, 2)), D((3, 2)), D((3, 2)), D((3, 2)), D, D,
        D((2, 8)), D((11,)), D((2, 8)), D((11,)),
    ]
    hbm = pl.BlockSpec(memory_space=pl.ANY)
    results = (jax.ShapeDtypeStruct(blocks, F32), jax.ShapeDtypeStruct((8, 512), F32),
               jax.ShapeDtypeStruct((8, 512), F32))
    out = pl.pallas_call(
        kernel,
        out_shape=(jax.ShapeDtypeStruct((11, 2, 16, 256), F32), jax.ShapeDtypeStruct((11, 9, 128), F32)),
        in_specs=[hbm] * 7,
        out_specs=[hbm] * 2,
        scratch_shapes=scratch,
        compiler_params=pltpu.CompilerParams(
            collective_id=0, has_side_effects=True, vmem_limit_bytes=VMEM_LIMIT),
    )(shifts, field, row_prop, col_prop, phase, energy, cells)
    return pl.pallas_call(
        hand_over,
        out_shape=(*results, jax.ShapeDtypeStruct((4, 2, 8), F32)),
        in_specs=[hbm] * 3,
        out_specs=[hbm] * 4,
        scratch_shapes=[pltpu.SMEM((4,), jnp.int32), V((11, 2, 16, 256), F32), V((11, 9, 128), F32),
                        V(blocks, F32), V((8, 512), F32), V((8, 512), F32), V((8, 8), F32),
                        V((4, 2, 8), F32), D((7,))],
        compiler_params=pltpu.CompilerParams(vmem_limit_bytes=VMEM_LIMIT),
    )(shifts, *out)


def solution(mesh):
    return jax.shard_map(
        shards,
        mesh=mesh,
        in_specs=(
            P(None, "cuts", "row", None),
            P(),
            P(),
            P("cuts", "row"),
            P("cuts", "row"),
            P("cuts", "row"),
            P(),
        ),
        out_specs=(
            P(None, "cuts", "row", None),
            P("cuts", "row"),
            P("cuts", "row"),
            P(None, None, "cuts"),
        ),
        check_vma=False,
    )
```
